16 devices in a mesh: fsdp: 16 (over z, y, x, core).
Axes of the slice: x: 2, y: 2, z: 2, core: 2. Of those that a mesh axis runs over, the one named last changes fastest.
Arguments:
- tokens_x: bfloat16 [96, 256, 640], P('fsdp')
- context: bfloat16 [96, 77, 2048], P('fsdp')
- cot_out: bfloat16 [96, 256, 640], P('fsdp')
- w_qkv: bfloat16 [2, 1228800], P(None, 'fsdp')
- w_out: bfloat16 [2, 409600], P(None, 'fsdp')
- w_q2: bfloat16 [2, 409600], P(None, 'fsdp')
- w_kv2: bfloat16 [2, 2621440], P(None, 'fsdp')
- w_out2: bfloat16 [2, 409600], P(None, 'fsdp')
- w_ff1: bfloat16 [2, 3276800], P(None, 'fsdp')
- w_ff2: bfloat16 [2, 1638400], P(None, 'fsdp')
- w_vecs: bfloat16 [2, 10880], P(None, 'fsdp')
Outputs:
- output 1: bfloat16 [96, 256, 640], P('fsdp')
- output 2: bfloat16 [96, 256, 640], P('fsdp')
- output 3: float32 [2, 1228800], P(None, 'fsdp')
- output 4: float32 [2, 409600], P(None, 'fsdp')
- output 5: float32 [2, 409600], P(None, 'fsdp')
- output 6: float32 [2, 2621440], P(None, 'fsdp')
- output 7: float32 [2, 409600], P(None, 'fsdp')
- output 8: float32 [2, 3276800], P(None, 'fsdp')
- output 9: float32 [2, 1638400], P(None, 'fsdp')
- output 10: float32 [2, 10880], P(None, 'fsdp')
All inputs are finite; a program needn't handle non-finite values.
Results may differ from the reference program's by a relative error of at most 0.0199622.
Values are sent between devices in bfloat16 or wider.
A program may use at most 1 GiB of HBM per device.

```python
import math
import jax
import jax.numpy as jnp
from jax import lax

FSDP = 16
BATCH_DEV = 6
TOKENS = 256
D = 640
CTX_D = 2048
CTX_LEN = 77
HEAD = 64
BLOCKS = 2

BATCH = FSDP * BATCH_DEV
HEADS = D // HEAD
FF = 4 * D
SHAPES = ((D, 3 * D), (D, D), (D, D), (CTX_D, 2 * D), (D, D), (D, 2 * FF), (FF, D), (9 * D + 2 * FF,))
NAMES = ('w_qkv', 'w_out', 'w_q2', 'w_kv2', 'w_out2', 'w_ff1', 'w_ff2', 'w_vecs')


def padded_len(shape):
    return ((math.prod(shape) + FSDP - 1) // FSDP) * FSDP


def setup_inputs(seed: int = 0) -> dict:
    draws = jax.random.split(jax.random.key(seed), 11)
    tokens_x = jax.random.normal(draws[0], (BATCH, TOKENS, D), jnp.float32)
    context = jax.random.normal(draws[1], (BATCH, CTX_LEN, CTX_D), jnp.float32)
    cot_out = jax.random.normal(draws[2], (BATCH, TOKENS, D), jnp.float32)
    result = {'tokens_x': tokens_x.astype(jnp.bfloat16), 'context': context.astype(jnp.bfloat16), 'cot_out': cot_out.astype(jnp.bfloat16)}
    for index in range(7):
        shape = SHAPES[index]
        drawn = jax.random.normal(draws[3 + index], (BLOCKS, padded_len(shape)), jnp.float32) * shape[0] ** -0.5
        result[NAMES[index]] = drawn.astype(jnp.bfloat16)
    length = padded_len(SHAPES[7])
    position = jnp.arange(length)
    gain_mask = ((position < 6 * D) & ((position // D) % 2 == 0)).astype(jnp.float32)
    drawn = 0.3 * jax.random.normal(draws[10], (BLOCKS, length), jnp.float32) + gain_mask
    result['w_vecs'] = drawn.astype(jnp.bfloat16)
    return result


def matmul(lhs, rhs):
    return jnp.dot(lhs, rhs, preferred_element_type=jnp.float32)


def layer_norm(residual, gain, shift):
    average = jnp.mean(residual, axis=-1, keepdims=True)
    centered = residual - average
    variance = jnp.mean(centered * centered, axis=-1, keepdims=True)
    return centered * lax.rsqrt(variance + 1e-5) * gain + shift


def attend(query, keys, values):
    scores = jnp.einsum('qhe,khe->hqk', query.astype(jnp.float32), keys.astype(jnp.float32)) * HEAD ** -0.5
    probabilities = jax.nn.softmax(scores, axis=-1).astype(jnp.bfloat16)
    mixed = jnp.einsum('hqk,khe->qhe', probabilities.astype(jnp.float32), values.astype(jnp.float32))
    return mixed.astype(jnp.bfloat16)


def batched_attend(query, keys, values):
    return lax.map(lambda trio: attend(trio[0], trio[1], trio[2]), (query, keys, values))


def block_forward(residual, ctx_rows, flats):
    matrices = [flat[:math.prod(shape)].reshape(shape).astype(jnp.bfloat16) for flat, shape in zip(flats[:7], SHAPES[:7])]
    w_qkv, w_out, w_q2, w_kv2, w_out2, w_ff1, w_ff2 = matrices
    rows = flats[7][:9 * D].reshape(9, D)
    bias_ff1 = flats[7][9 * D:9 * D + 2 * FF]
    norm1 = layer_norm(residual, rows[0], rows[1]).astype(jnp.bfloat16)
    qkv_heads = matmul(norm1, w_qkv).astype(jnp.bfloat16).reshape(BATCH, TOKENS, 3, HEADS, HEAD)
    self_out = batched_attend(qkv_heads[:, :, 0], qkv_heads[:, :, 1], qkv_heads[:, :, 2]).reshape(BATCH * TOKENS, D)
    residual = residual + matmul(self_out, w_out) + rows[6]
    norm2 = layer_norm(residual, rows[2], rows[3]).astype(jnp.bfloat16)
    query = matmul(norm2, w_q2).astype(jnp.bfloat16).reshape(BATCH, TOKENS, HEADS, HEAD)
    kv_heads = matmul(ctx_rows, w_kv2).astype(jnp.bfloat16).reshape(BATCH, CTX_LEN, 2, HEADS, HEAD)
    cross_out = batched_attend(query, kv_heads[:, :, 0], kv_heads[:, :, 1]).reshape(BATCH * TOKENS, D)
    residual = residual + matmul(cross_out, w_out2) + rows[7]
    norm3 = layer_norm(residual, rows[4], rows[5]).astype(jnp.bfloat16)
    hidden = matmul(norm3, w_ff1) + bias_ff1
    gated = (hidden[:, :FF] * jax.nn.gelu(hidden[:, FF:], approximate=False)).astype(jnp.bfloat16)
    return residual + matmul(gated, w_ff2) + rows[8]


def forward(tokens_x, context, flats):
    residual = tokens_x.reshape(BATCH * TOKENS, D).astype(jnp.float32)
    ctx_rows = context.reshape(BATCH * CTX_LEN, CTX_D)

    def step(carry, block_flats):
        return block_forward(carry, ctx_rows, block_flats), None

    residual, unused = lax.scan(step, residual, flats)
    return residual.astype(jnp.bfloat16).reshape(BATCH, TOKENS, D)


def reference(tokens_x, context, cot_out, w_qkv, w_out, w_q2, w_kv2, w_out2, w_ff1, w_ff2, w_vecs):
    flats = tuple(param.astype(jnp.float32) for param in (w_qkv, w_out, w_q2, w_kv2, w_out2, w_ff1, w_ff2, w_vecs))
    out_tokens, pullback = jax.vjp(lambda tok_in, param_set: forward(tok_in, context, param_set), tokens_x, flats)
    grad_x, grads = pullback(cot_out)
    scaled = [grad_item / BATCH for grad_item in grads]
    return (out_tokens, grad_x, scaled[0], scaled[1], scaled[2], scaled[3], scaled[4], scaled[5], scaled[6], scaled[7])
```

```python
import math
import jax
import jax.numpy as jnp
from jax import lax
from jax.sharding import PartitionSpec as P

HEAD = 64
AXIS = 'fsdp'


def weight_shapes(width, ctx_width):
    return ((width, 3 * width), (width, width), (width, width), (ctx_width, 2 * width),
            (width, width), (width, 8 * width), (4 * width, width), (17 * width,))


def layer_norm(residual, gain, shift):
    average = jnp.mean(residual, axis=-1, keepdims=True)
    centered = residual - average
    variance = jnp.mean(centered * centered, axis=-1, keepdims=True)
    return centered * lax.rsqrt(variance + 1e-5) * gain + shift


def attend(query, keys, values):
    scores = jnp.einsum('bqhe,bkhe->bhqk', query, keys, preferred_element_type=jnp.float32) * HEAD ** -0.5
    probabilities = jax.nn.softmax(scores, axis=-1).astype(jnp.bfloat16)
    mixed = jnp.einsum('bhqk,bkhe->bqhe', probabilities, values, preferred_element_type=jnp.float32)
    return mixed.astype(jnp.bfloat16)


def self_attend(qkv_heads):
    return attend(qkv_heads[:, :, 0], qkv_heads[:, :, 1], qkv_heads[:, :, 2])


def cross_attend(query, kv_heads):
    return attend(query, kv_heads[:, :, 0], kv_heads[:, :, 1])


def geglu(hidden):
    half = hidden.shape[-1] // 2
    return (hidden[..., :half] * jax.nn.gelu(hidden[..., half:], approximate=False)).astype(jnp.bfloat16)


def project(inputs, weight):
    return jnp.einsum('btd,de->bte', inputs, weight, preferred_element_type=jnp.float32)


def project_back(grads, weight):
    return jnp.einsum('bte,de->btd', grads, weight, preferred_element_type=jnp.float32)


def weight_grad(inputs, grads):
    return jnp.einsum('btd,bte->de', inputs, grads, preferred_element_type=jnp.float32)


def gather_block(shards, width):
    shapes = weight_shapes(width, shards[3].shape[0] * lax.axis_size(AXIS) // (2 * width))
    n_dev = lax.axis_size(AXIS)
    local = [shard.reshape(shape[0] // n_dev, shape[1]) for shard, shape in zip(shards[:7], shapes[:7])]
    small = jnp.concatenate([local[1], local[2], local[4]], axis=1)
    first = lax.all_gather(local[0], AXIS, axis=0, tiled=True)
    small = lax.all_gather(small, AXIS, axis=0, tiled=True)
    kv2 = lax.all_gather(local[3], AXIS, axis=0, tiled=True)
    ff1 = lax.all_gather(local[5], AXIS, axis=0, tiled=True)
    ff2 = lax.all_gather(local[6], AXIS, axis=0, tiled=True)
    return dict(w_qkv=first, w_out=small[:, :width], w_q2=small[:, width:2 * width], w_kv2=kv2,
                w_out2=small[:, 2 * width:], w_ff1=ff1, w_ff2=ff2)


def block_forward(residual, context, weights):
    batch, tokens, width = residual.shape
    heads = width // HEAD
    rows = weights['rows']
    norm1, ln1_back = jax.vjp(layer_norm, residual, rows[0], rows[1])
    norm1 = norm1.astype(jnp.bfloat16)
    qkv_heads = project(norm1, weights['w_qkv']).astype(jnp.bfloat16).reshape(batch, tokens, 3, heads, HEAD)
    self_out, self_back = jax.vjp(self_attend, qkv_heads)
    self_out = self_out.reshape(batch, tokens, width)
    residual = residual + project(self_out, weights['w_out']) + rows[6]
    norm2, ln2_back = jax.vjp(layer_norm, residual, rows[2], rows[3])
    norm2 = norm2.astype(jnp.bfloat16)
    query = project(norm2, weights['w_q2']).astype(jnp.bfloat16).reshape(batch, tokens, heads, HEAD)
    kv_heads = project(context, weights['w_kv2']).astype(jnp.bfloat16).reshape(batch, context.shape[1], 2, heads, HEAD)
    cross_out, cross_back = jax.vjp(cross_attend, query, kv_heads)
    cross_out = cross_out.reshape(batch, tokens, width)
    residual = residual + project(cross_out, weights['w_out2']) + rows[7]
    norm3, ln3_back = jax.vjp(layer_norm, residual, rows[4], rows[5])
    norm3 = norm3.astype(jnp.bfloat16)
    gated, geglu_back = jax.vjp(geglu, project(norm3, weights['w_ff1']) + weights['bias_ff1'])
    residual = residual + project(gated, weights['w_ff2']) + rows[8]
    saved = dict(ln1_back=ln1_back, norm1=norm1, self_back=self_back, self_out=self_out,
                 ln2_back=ln2_back, norm2=norm2, cross_back=cross_back, cross_out=cross_out,
                 ln3_back=ln3_back, norm3=norm3, geglu_back=geglu_back, gated=gated)
    return residual, saved


def block_backward(grad, context, weights, saved):
    batch, tokens, width = grad.shape
    heads = width // HEAD
    grad_bf = grad.astype(jnp.bfloat16)
    g_bias_ff2 = jnp.sum(grad, axis=(0, 1))
    g_ff2 = weight_grad(saved['gated'], grad_bf)
    d_gated = project_back(grad_bf, weights['w_ff2']).astype(jnp.bfloat16)
    (d_hidden,) = saved['geglu_back'](d_gated)
    g_bias_ff1 = jnp.sum(d_hidden, axis=(0, 1))
    d_hidden = d_hidden.astype(jnp.bfloat16)
    g_ff1 = weight_grad(saved['norm3'], d_hidden)
    d_res, g_ln3_gain, g_ln3_shift = saved['ln3_back'](project_back(d_hidden, weights['w_ff1']))
    grad = grad + d_res
    grad_bf = grad.astype(jnp.bfloat16)
    g_bias_out2 = jnp.sum(grad, axis=(0, 1))
    g_out2 = weight_grad(saved['cross_out'], grad_bf)
    d_cross = project_back(grad_bf, weights['w_out2']).astype(jnp.bfloat16).reshape(batch, tokens, heads, HEAD)
    d_query, d_kv = saved['cross_back'](d_cross)
    d_query = d_query.reshape(batch, tokens, width)
    g_q2 = weight_grad(saved['norm2'], d_query)
    g_kv2 = weight_grad(context, d_kv.reshape(batch, context.shape[1], 2 * width))
    d_res, g_ln2_gain, g_ln2_shift = saved['ln2_back'](project_back(d_query, weights['w_q2']))
    grad = grad + d_res
    grad_bf = grad.astype(jnp.bfloat16)
    g_bias_out = jnp.sum(grad, axis=(0, 1))
    g_out = weight_grad(saved['self_out'], grad_bf)
    d_self = project_back(grad_bf, weights['w_out']).astype(jnp.bfloat16).reshape(batch, tokens, heads, HEAD)
    (d_qkv,) = saved['self_back'](d_self)
    d_qkv = d_qkv.reshape(batch, tokens, 3 * width)
    g_qkv = weight_grad(saved['norm1'], d_qkv)
    d_res, g_ln1_gain, g_ln1_shift = saved['ln1_back'](project_back(d_qkv, weights['w_qkv']))
    grad = grad + d_res
    g_vecs = jnp.concatenate([g_ln1_gain, g_ln1_shift, g_ln2_gain, g_ln2_shift, g_ln3_gain, g_ln3_shift,
                              g_bias_out, g_bias_out2, g_bias_ff2, g_bias_ff1])
    return grad, [g_qkv, g_out, g_q2, g_kv2, g_out2, g_ff1, g_ff2, g_vecs]


def scatter_grads(grads, n_dev, total):
    result = []
    for grad_full in grads[:7]:
        shard = lax.psum_scatter(grad_full, AXIS, scatter_dimension=0, tiled=True)
        result.append(shard.reshape(-1) / total)
    return result


def solution(mesh):
    n_dev = mesh.shape[AXIS]

    def local(tokens_x, context, cot_out, *shards):
        batch, tokens, width = tokens_x.shape
        blocks = shards[0].shape[0]
        total = batch * n_dev
        residual = tokens_x.astype(jnp.float32)
        saved_list = []
        all_weights = []
        vecs = lax.all_gather(shards[7].reshape(1, blocks, -1), AXIS, axis=0, tiled=True)
        vecs = jnp.swapaxes(vecs, 0, 1).reshape(blocks, -1)
        for layer in range(blocks):
            weights = gather_block([shard[layer] for shard in shards[:7]], width)
            weights['rows'] = vecs[layer, :9 * width].reshape(9, width).astype(jnp.float32)
            weights['bias_ff1'] = vecs[layer, 9 * width:17 * width].astype(jnp.float32)
            residual, saved = block_forward(residual, context, weights)
            saved_list.append(saved)
            all_weights.append(weights)
        grad = cot_out.astype(jnp.float32)
        grad_shards = []
        vec_grads = []
        for layer in reversed(range(blocks)):
            grad, block_grads = block_backward(grad, context, all_weights[layer], saved_list[layer])
            grad_shards.insert(0, scatter_grads(block_grads, n_dev, total))
            vec_grads.insert(0, block_grads[7])
        vec = jnp.stack(vec_grads)
        length = shards[7].shape[1]
        vec = lax.psum_scatter(vec.reshape(blocks, n_dev, length), AXIS, scatter_dimension=1, tiled=False) / total
        stacked = [jnp.stack([per_layer[index] for per_layer in grad_shards]) for index in range(7)]
        return tuple([residual.astype(jnp.bfloat16), grad.astype(jnp.bfloat16)] + stacked + [vec])

    param_spec = P(None, AXIS)
    in_specs = (P(AXIS), P(AXIS), P(AXIS)) + (param_spec,) * 8
    out_specs = (P(AXIS), P(AXIS)) + (param_spec,) * 8
    return jax.shard_map(local, mesh=mesh, in_specs=in_specs, out_specs=out_specs, check_vma=False)
```

```python
import math
import jax
import jax.numpy as jnp
from jax import lax
from jax.experimental import pallas as pl
from jax.experimental.pallas import tpu as pltpu
from jax.sharding import PartitionSpec as P

AXIS = 'fsdp'
HEAD = 64
EPS = 1e-5
F32 = jnp.float32
BF16 = jnp.bfloat16
LANES = 128
SLOT = 128
PAIR_ROWS = 512
FF_COLS = 256

TAIL_P = 0.265
TAIL = (0.10574158579953814, 0.10524628753634038, 0.10270369607548423, 0.0603023517537824, 0.13797880111692826,
        -0.11640058407079061, 0.2178489286936914, -0.1442454807654402, 0.03082441619112092)


def weight_shapes(width, ctx_width):
    return ((width, 3 * width), (width, width), (width, width), (ctx_width, 2 * width),
            (width, width), (width, 8 * width), (4 * width, width), (17 * width,))


def mm(lhs, rhs):
    return jnp.dot(lhs, rhs, preferred_element_type=F32)


def mm_nt(lhs, rhs):
    return lax.dot_general(lhs, rhs, (((1,), (1,)), ((), ())), preferred_element_type=F32)


def mm_tn(lhs, rhs):
    return lax.dot_general(lhs, rhs, (((0,), (0,)), ((), ())), preferred_element_type=F32)


def normalize(x):
    centered = x - jnp.mean(x, axis=-1, keepdims=True)
    scale = lax.rsqrt(jnp.mean(centered * centered, axis=-1, keepdims=True) + EPS)
    return centered * scale, scale


def norm_back(x, d_norm, gain):
    hat, scale = normalize(x)
    d_hat = d_norm * gain
    pulled = d_hat - jnp.mean(d_hat, axis=-1, keepdims=True) - hat * jnp.mean(d_hat * hat, axis=-1, keepdims=True)
    return pulled * scale, jnp.sum(d_norm * hat, axis=0, keepdims=True), jnp.sum(d_norm, axis=0, keepdims=True)


def low_half(rows):
    return lax.broadcasted_iota(jnp.int32, (rows, LANES), 1) < HEAD


def head_stack(pair, low):
    zero = jnp.zeros_like(pair)
    return jnp.concatenate([jnp.where(low, pair, zero), jnp.where(low, zero, pair)], axis=0)


def head_unstack(stacked, low):
    half = stacked.shape[0] // 2
    return jnp.where(low, stacked[:half], stacked[half:])


def softmax_halves(scores, valid):
    half = scores.shape[1] // 2
    parts = []
    for index in range(2):
        part = scores[:, index * half:(index + 1) * half]
        if valid < half:
            part = jnp.where(lax.broadcasted_iota(jnp.int32, part.shape, 1) < valid, part, -jnp.inf)
        part = jnp.exp(part - jnp.max(part, axis=-1, keepdims=True))
        parts.append(part * (1.0 / jnp.sum(part, axis=-1, keepdims=True)))
    return parts


def pair_forward(query, keys, values, valid):
    low = low_half(keys.shape[0])
    scores = mm_nt(query * BF16(HEAD ** -0.5), head_stack(keys, low))
    probs = jnp.concatenate([part.astype(BF16) for part in softmax_halves(scores, valid)], axis=1)
    return mm(probs, head_stack(values, low)).astype(BF16)


def pair_backward(query, keys, values, d_out, valid):
    low = low_half(keys.shape[0])
    half = keys.shape[0]
    query = query * BF16(HEAD ** -0.5)
    key_stack = head_stack(keys, low)
    value_stack = head_stack(values, low)
    parts = softmax_halves(mm_nt(query, key_stack), valid)
    probs = jnp.concatenate([part.astype(BF16) for part in parts], axis=1)
    d_values = head_unstack(mm_tn(probs, d_out), low).astype(BF16)
    d_probs = mm_nt(d_out, value_stack)
    d_scores = []
    for index in range(2):
        part, d_part = parts[index], d_probs[:, index * half:(index + 1) * half]
        d_scores.append((part * (d_part - jnp.sum(part * d_part, axis=-1, keepdims=True))).astype(BF16))
    d_scores = jnp.concatenate(d_scores, axis=1)
    d_query = (mm(d_scores, key_stack) * HEAD ** -0.5).astype(BF16)
    d_keys = head_unstack(mm_tn(d_scores, query), low).astype(BF16)
    return d_query, d_keys, d_values


def self_forward_kernel(heads, tokens, h_ref, w_qkv_ref, w_out_ref, rows_ref, h1_ref, qkv_ref, out_ref):
    width = heads * HEAD
    hat, unused = normalize(h_ref[...].astype(F32))
    norm1 = (hat * rows_ref[0:1] + rows_ref[1:2]).astype(BF16)
    qkv_ref[...] = mm(norm1, w_qkv_ref[...]).astype(BF16)

    def sample(index, carry):
        rows = pl.ds(pl.multiple_of(index * tokens, tokens), tokens)
        for pair in range(heads // 2):
            cols = pair * LANES
            out_ref[rows, cols:cols + LANES] = pair_forward(
                qkv_ref[rows, cols:cols + LANES], qkv_ref[rows, width + cols:width + cols + LANES],
                qkv_ref[rows, 2 * width + cols:2 * width + cols + LANES], tokens)
        return carry

    lax.fori_loop(0, h_ref.shape[0] // tokens, sample, 0)
    h1_ref[...] = h_ref[...].astype(F32) + mm(out_ref[...], w_out_ref[...]) + rows_ref[6:7]


def cross_forward_kernel(heads, tokens, ctx_len, h1_ref, context_ref, w_q_ref, w_kv_ref, w_out_ref, rows_ref,
                         h2_ref, q_ref, kv_ref, out_ref):
    width = heads * HEAD
    samples = kv_ref.shape[0] // SLOT
    pad = context_ref.shape[0] // samples
    step = pl.program_id(0)

    @pl.when(step == 0)
    def _():
        kv = mm(context_ref[...], w_kv_ref[...]).astype(BF16)
        for index in range(samples):
            kv_ref[index * SLOT:index * SLOT + pad] = kv[index * pad:(index + 1) * pad]
            kv_ref[index * SLOT + pad:(index + 1) * SLOT] = jnp.zeros((SLOT - pad, 2 * width), BF16)

    hat, unused = normalize(h1_ref[...])
    norm2 = (hat * rows_ref[2:3] + rows_ref[3:4]).astype(BF16)
    q_ref[...] = mm(norm2, w_q_ref[...]).astype(BF16)
    per_step = h1_ref.shape[0] // tokens

    def sample(index, carry):
        rows = pl.ds(pl.multiple_of(index * tokens, tokens), tokens)
        kv_rows = pl.ds(pl.multiple_of((step * per_step + index) * SLOT, SLOT), SLOT)
        for pair in range(heads // 2):
            cols = pair * LANES
            out_ref[rows, cols:cols + LANES] = pair_forward(
                q_ref[rows, cols:cols + LANES], kv_ref[kv_rows, cols:cols + LANES],
                kv_ref[kv_rows, width + cols:width + cols + LANES], ctx_len)
        return carry

    lax.fori_loop(0, per_step, sample, 0)
    h2_ref[...] = h1_ref[...] + mm(out_ref[...], w_out_ref[...]) + rows_ref[7:8]


def normal_cdf(u):
    t = 1.0 / (1.0 + TAIL_P * jnp.abs(u))
    poly = TAIL[-1]
    for coef in TAIL[-2::-1]:
        poly = poly * t + coef
    bell = jnp.exp(u * u * -0.5)
    tail = bell * (t * poly)
    return jnp.where(u >= 0, 1.0 - tail, tail), bell


def ff_forward_kernel(chunk, h2_ref, w1a_ref, w1g_ref, w2_ref, b1a_ref, b1g_ref, rows_ref,
                      h3_ref, fa_ref, fg_ref, z_ref, norm_ref, acc_ref):
    step = pl.program_id(0)
    chunks = h2_ref.shape[0] // chunk

    @pl.when(step == 0)
    def _():
        def start(index, carry):
            rows = pl.ds(pl.multiple_of(index * chunk, chunk), chunk)
            hat, unused = normalize(h2_ref[rows])
            norm_ref[rows] = (hat * rows_ref[4:5] + rows_ref[5:6]).astype(BF16)
            acc_ref[rows] = jnp.zeros((chunk, h2_ref.shape[1]), F32)
            return carry

        lax.fori_loop(0, chunks, start, 0)

    def body(index, carry):
        rows = pl.ds(pl.multiple_of(index * chunk, chunk), chunk)
        norm3 = norm_ref[rows]
        gate = mm(norm3, w1g_ref[...]) + b1g_ref[...]
        cdf, bell = normal_cdf(gate)
        factor = gate * cdf
        value = mm(norm3, w1a_ref[...]) + b1a_ref[...]
        z = (value * factor).astype(BF16)
        z_ref[0, rows] = z
        fa_ref[0, rows] = factor
        fg_ref[0, rows] = value * (cdf + gate * bell * (2 * math.pi) ** -0.5)
        acc_ref[rows] += mm(z, w2_ref[...])
        return carry

    lax.fori_loop(0, chunks, body, 0)

    @pl.when(step == pl.num_programs(0) - 1)
    def _():
        h3_ref[...] = h2_ref[...] + acc_ref[...] + rows_ref[8:9]


def ff_backward_kernel(chunk, grad_ref, h2_ref, w1a_ref, w1g_ref, w2_ref, fa_ref, fg_ref, z_ref, rows_ref,
                       out_ref, d_w1a_ref, d_w1g_ref, d_w2_ref, d_b1_ref, d_rows_ref,
                       norm_t_ref, grad_bf_ref, du_ref, w1_ref, acc_ref):
    step = pl.program_id(0)
    chunks = h2_ref.shape[0] // chunk
    cols = fa_ref.shape[2]

    @pl.when(step == 0)
    def _():
        d_rows_ref[...] = jnp.zeros_like(d_rows_ref)

        def start(index, carry):
            rows = pl.ds(pl.multiple_of(index * chunk, chunk), chunk)
            hat, unused = normalize(h2_ref[rows])
            norm_t_ref[:, rows] = (hat * rows_ref[4:5] + rows_ref[5:6]).astype(BF16).T
            grad_bf_ref[rows] = grad_ref[rows].astype(BF16)
            d_rows_ref[8:9] += jnp.sum(grad_ref[rows], axis=0, keepdims=True)
            acc_ref[rows] = jnp.zeros((chunk, h2_ref.shape[1]), F32)
            return carry

        lax.fori_loop(0, chunks, start, 0)

    w1_ref[:, :cols] = w1a_ref[...]
    w1_ref[:, cols:] = w1g_ref[...]

    def body(index, sums):
        rows = pl.ds(pl.multiple_of(index * chunk, chunk), chunk)
        dz = mm_nt(grad_bf_ref[rows], w2_ref[...]).astype(BF16).astype(F32)
        du_a = dz * fa_ref[0, rows]
        du_g = dz * fg_ref[0, rows]
        du_ref[rows, :cols] = du_a.astype(BF16)
        du_ref[rows, cols:] = du_g.astype(BF16)
        acc_ref[rows] += mm_nt(du_ref[rows], w1_ref[...])
        return (sums[0] + jnp.sum(du_a, axis=0, keepdims=True), sums[1] + jnp.sum(du_g, axis=0, keepdims=True))

    zero = jnp.zeros((1, cols), F32)
    sum_a, sum_g = lax.fori_loop(0, chunks, body, (zero, zero))
    d_b1_ref[0, 0:1] = sum_a
    d_b1_ref[0, 1:2] = sum_g
    d_w1a_ref[...] = mm(norm_t_ref[...], du_ref[:, :cols])
    d_w1g_ref[...] = mm(norm_t_ref[...], du_ref[:, cols:])
    d_w2_ref[...] = mm_tn(z_ref[0], grad_bf_ref[...])

    @pl.when(step == pl.num_programs(0) - 1)
    def _():
        def finish(index, carry):
            rows = pl.ds(pl.multiple_of(index * chunk, chunk), chunk)
            d_res, d_gain, d_shift = norm_back(h2_ref[rows], acc_ref[rows], rows_ref[4:5])
            out_ref[rows] = grad_ref[rows] + d_res
            d_rows_ref[4:5] += d_gain
            d_rows_ref[5:6] += d_shift
            return carry

        lax.fori_loop(0, chunks, finish, 0)


def cross_backward_kernel(heads, tokens, ctx_len, row_steps, grad_ref, h1_ref, q_ref, out2_ref, kv_ref, context_ref,
                          w_q_ref, w_out_ref, rows_ref, out_ref, d_wq_ref, d_wout_ref, d_wkv_ref, d_rows_ref,
                          d_mix_ref, d_q_ref, d_kv_ref):
    width = heads * HEAD
    step = pl.program_id(0)
    pad = context_ref.shape[0] // (kv_ref.shape[0] // SLOT)
    per_step = h1_ref.shape[0] // tokens

    @pl.when(step == 0)
    def _():
        d_rows_ref[...] = jnp.zeros_like(d_rows_ref)
        d_wq_ref[...] = jnp.zeros_like(d_wq_ref)
        d_wout_ref[...] = jnp.zeros_like(d_wout_ref)

    @pl.when(step < row_steps)
    def _():
        grad = grad_ref[...]
        grad_bf = grad.astype(BF16)
        d_rows_ref[7:8] += jnp.sum(grad, axis=0, keepdims=True)
        d_wout_ref[...] += mm_tn(out2_ref[...], grad_bf)
        d_mix_ref[...] = mm_nt(grad_bf, w_out_ref[...]).astype(BF16)

        def sample(index, carry):
            rows = pl.ds(pl.multiple_of(index * tokens, tokens), tokens)
            kv_rows = pl.ds(pl.multiple_of((step * per_step + index) * SLOT, SLOT), SLOT)
            d_kv_rows = pl.ds(pl.multiple_of((step * per_step + index) * pad, pad), pad)
            for pair in range(heads // 2):
                cols = pair * LANES
                d_query, d_keys, d_values = pair_backward(
                    q_ref[rows, cols:cols + LANES], kv_ref[kv_rows, cols:cols + LANES],
                    kv_ref[kv_rows, width + cols:width + cols + LANES], d_mix_ref[rows, cols:cols + LANES], ctx_len)
                d_q_ref[rows, cols:cols + LANES] = d_query
                d_kv_ref[d_kv_rows, cols:cols + LANES] = d_keys[:pad]
                d_kv_ref[d_kv_rows, width + cols:width + cols + LANES] = d_values[:pad]
            return carry

        lax.fori_loop(0, per_step, sample, 0)
        h1 = h1_ref[...]
        hat, unused = normalize(h1)
        norm2 = (hat * rows_ref[2:3] + rows_ref[3:4]).astype(BF16)
        d_wq_ref[...] += mm_tn(norm2, d_q_ref[...])
        d_res, d_gain, d_shift = norm_back(h1, mm_nt(d_q_ref[...], w_q_ref[...]), rows_ref[2:3])
        out_ref[...] = grad + d_res
        d_rows_ref[2:3] += d_gain
        d_rows_ref[3:4] += d_shift

    @pl.when(step >= row_steps)
    def _():
        cols = d_wkv_ref.shape[1]
        start = pl.multiple_of((step - row_steps) * cols, cols)
        d_wkv_ref[...] = mm_tn(context_ref[...], d_kv_ref[:, pl.ds(start, cols)])


def self_backward_kernel(heads, tokens, row_steps, grad_ref, h_ref, qkv_ref, out1_ref, w_qkv_ref, w_out_ref, rows_ref,
                         out_ref, d_wqkv_ref, d_wout_ref, d_rows_ref, d_mix_ref, d_qkv_ref, norm_t_ref):
    width = heads * HEAD
    step = pl.program_id(0)
    block = h_ref.shape[0]

    @pl.when(step == 0)
    def _():
        d_rows_ref[...] = jnp.zeros_like(d_rows_ref)
        d_wout_ref[...] = jnp.zeros_like(d_wout_ref)

    @pl.when(step < row_steps)
    def _():
        grad = grad_ref[...]
        grad_bf = grad.astype(BF16)
        d_rows_ref[6:7] += jnp.sum(grad, axis=0, keepdims=True)
        d_wout_ref[...] += mm_tn(out1_ref[...], grad_bf)
        d_mix_ref[...] = mm_nt(grad_bf, w_out_ref[...]).astype(BF16)
        base = pl.multiple_of(step * block, block)

        def sample(index, carry):
            rows = pl.ds(pl.multiple_of(index * tokens, tokens), tokens)
            d_rows = pl.ds(pl.multiple_of(base + index * tokens, tokens), tokens)
            for pair in range(heads // 2):
                cols = pair * LANES
                d_query, d_keys, d_values = pair_backward(
                    qkv_ref[rows, cols:cols + LANES], qkv_ref[rows, width + cols:width + cols + LANES],
                    qkv_ref[rows, 2 * width + cols:2 * width + cols + LANES], d_mix_ref[rows, cols:cols + LANES], tokens)
                d_qkv_ref[d_rows, cols:cols + LANES] = d_query
                d_qkv_ref[d_rows, width + cols:width + cols + LANES] = d_keys
                d_qkv_ref[d_rows, 2 * width + cols:2 * width + cols + LANES] = d_values
            return carry

        lax.fori_loop(0, block // tokens, sample, 0)
        h = h_ref[...].astype(F32)
        hat, unused = normalize(h)
        norm_t_ref[:, pl.ds(base, block)] = (hat * rows_ref[0:1] + rows_ref[1:2]).astype(BF16).T
        d_norm = mm_nt(d_qkv_ref[pl.ds(base, block)], w_qkv_ref[...])
        d_res, d_gain, d_shift = norm_back(h, d_norm, rows_ref[0:1])
        out_ref[...] = (grad + d_res).astype(out_ref.dtype)
        d_rows_ref[0:1] += d_gain
        d_rows_ref[1:2] += d_shift

    @pl.when(step >= row_steps)
    def _():
        cols = d_wqkv_ref.shape[1]
        start = pl.multiple_of((step - row_steps) * cols, cols)
        d_wqkv_ref[...] = mm(norm_t_ref[...], d_qkv_ref[:, pl.ds(start, cols)])


def whole(shape):
    return pl.BlockSpec(shape, lambda step: (0,) * len(shape))


def params(**extra):
    return pltpu.CompilerParams(dimension_semantics=('arbitrary',), vmem_limit_bytes=62 * 1024 * 1024, **extra)


def cost(flops, moved):
    return pl.CostEstimate(flops=int(flops), bytes_accessed=int(moved), transcendentals=0)


def self_forward(h, w_qkv, w_out, rows, tokens):
    total, width = h.shape
    heads = width // HEAD
    row = lambda cols: pl.BlockSpec((PAIR_ROWS, cols), lambda step: (step, 0))
    return pl.pallas_call(
        lambda *refs: self_forward_kernel(heads, tokens, *refs),
        grid=(total // PAIR_ROWS,),
        in_specs=[row(width), whole(w_qkv.shape), whole(w_out.shape), whole(rows.shape)],
        out_specs=[row(width), row(3 * width), row(width)],
        out_shape=[jax.ShapeDtypeStruct((total, width), F32), jax.ShapeDtypeStruct((total, 3 * width), BF16),
                   jax.ShapeDtypeStruct((total, width), BF16)],
        compiler_params=params(), cost_estimate=cost(total * width * width * 10, 20e6), name='self_forward',
    )(h, w_qkv, w_out, rows)


def cross_forward(h1, context, w_q, w_kv, w_out, rows, tokens, ctx_len, samples):
    total, width = h1.shape
    heads = width // HEAD
    row = lambda cols: pl.BlockSpec((PAIR_ROWS, cols), lambda step: (step, 0))
    return pl.pallas_call(
        lambda *refs: cross_forward_kernel(heads, tokens, ctx_len, *refs),
        grid=(total // PAIR_ROWS,),
        in_specs=[row(width), whole(context.shape), whole(w_q.shape), whole(w_kv.shape), whole(w_out.shape),
                  whole(rows.shape)],
        out_specs=[row(width), row(width), whole((samples * SLOT, 2 * width)), row(width)],
        out_shape=[jax.ShapeDtypeStruct((total, width), F32), jax.ShapeDtypeStruct((total, width), BF16),
                   jax.ShapeDtypeStruct((samples * SLOT, 2 * width), BF16), jax.ShapeDtypeStruct((total, width), BF16)],
        compiler_params=params(), cost_estimate=cost(total * width * width * 8, 20e6), name='cross_forward',
    )(h1, context, w_q, w_kv, w_out, rows)


def ff_forward(h2, w1, w2, b1, rows, chunk):
    total, width = h2.shape
    inner = w2.shape[0]
    steps = inner // FF_COLS
    saved = pl.BlockSpec((1, total, FF_COLS), lambda step: (step, 0, 0))
    return pl.pallas_call(
        lambda *refs: ff_forward_kernel(chunk, *refs),
        grid=(steps,),
        in_specs=[whole(h2.shape), pl.BlockSpec((width, FF_COLS), lambda step: (0, step)),
                  pl.BlockSpec((width, FF_COLS), lambda step: (0, step + steps)),
                  pl.BlockSpec((FF_COLS, width), lambda step: (step, 0)),
                  pl.BlockSpec((1, FF_COLS), lambda step: (0, step)),
                  pl.BlockSpec((1, FF_COLS), lambda step: (0, step + steps)), whole(rows.shape)],
        out_specs=[whole(h2.shape), saved, saved, saved],
        out_shape=[jax.ShapeDtypeStruct((total, width), F32), jax.ShapeDtypeStruct((steps, total, FF_COLS), F32),
                   jax.ShapeDtypeStruct((steps, total, FF_COLS), F32), jax.ShapeDtypeStruct((steps, total, FF_COLS), BF16)],
        scratch_shapes=[pltpu.VMEM((total, width), BF16), pltpu.VMEM((total, width), F32)],
        compiler_params=params(), cost_estimate=cost(total * width * inner * 6, 60e6), name='ff_forward',
    )(h2, w1, w1, w2, b1, b1, rows)


def ff_backward(grad, h2, w1, w2, fa, fg, z, rows, chunk):
    total, width = h2.shape
    inner = w2.shape[0]
    steps = inner // FF_COLS
    saved = pl.BlockSpec((1, total, FF_COLS), lambda step: (step, 0, 0))
    column = pl.BlockSpec((width, FF_COLS), lambda step: (0, step))
    once = lambda shape: pl.BlockSpec(shape, lambda step: (0,) * len(shape), pipeline_mode=pl.Buffered(1))
    return pl.pallas_call(
        lambda *refs: ff_backward_kernel(chunk, *refs),
        grid=(steps,),
        in_specs=[once(grad.shape), once(h2.shape), column,
                  pl.BlockSpec((width, FF_COLS), lambda step: (0, step + steps)),
                  pl.BlockSpec((FF_COLS, width), lambda step: (step, 0)), saved, saved, saved, whole(rows.shape)],
        out_specs=[whole(h2.shape), column, column, pl.BlockSpec((FF_COLS, width), lambda step: (step, 0)),
                   pl.BlockSpec((1, 8, FF_COLS), lambda step: (step, 0, 0)), whole(rows.shape)],
        out_shape=[jax.ShapeDtypeStruct((total, width), F32), jax.ShapeDtypeStruct((width, inner), F32),
                   jax.ShapeDtypeStruct((width, inner), F32), jax.ShapeDtypeStruct((inner, width), F32),
                   jax.ShapeDtypeStruct((steps, 8, FF_COLS), F32), jax.ShapeDtypeStruct(rows.shape, F32)],
        scratch_shapes=[pltpu.VMEM((width, total), BF16), pltpu.VMEM((total, width), BF16),
                        pltpu.VMEM((total, 2 * FF_COLS), BF16), pltpu.VMEM((width, 2 * FF_COLS), BF16),
                        pltpu.VMEM((total, width), F32)],
        compiler_params=params(), cost_estimate=cost(total * width * inner * 12, 80e6), name='ff_backward',
    )(grad, h2, w1, w1, w2, fa, fg, z, rows)


def cross_backward(grad, h1, q, out2, kv, context, w_q, w_out, rows, tokens, ctx_len):
    total, width = h1.shape
    heads = width // HEAD
    row_steps = total // PAIR_ROWS
    kv_cols = 256
    extra = 2 * width // kv_cols
    row = lambda cols: pl.BlockSpec((PAIR_ROWS, cols), lambda step: (jnp.minimum(step, row_steps - 1), 0))
    return pl.pallas_call(
        lambda *refs: cross_backward_kernel(heads, tokens, ctx_len, row_steps, *refs),
        grid=(row_steps + extra,),
        in_specs=[row(width), row(width), row(width), row(width), whole(kv.shape), whole(context.shape),
                  whole(w_q.shape), whole(w_out.shape), whole(rows.shape)],
        out_specs=[row(width), whole(w_q.shape), whole(w_out.shape),
                   pl.BlockSpec((context.shape[1], kv_cols), lambda step: (0, jnp.maximum(step - row_steps, 0))),
                   whole(rows.shape)],
        out_shape=[jax.ShapeDtypeStruct((total, width), F32), jax.ShapeDtypeStruct(w_q.shape, F32),
                   jax.ShapeDtypeStruct(w_out.shape, F32), jax.ShapeDtypeStruct((context.shape[1], 2 * width), F32),
                   jax.ShapeDtypeStruct(rows.shape, F32)],
        scratch_shapes=[pltpu.VMEM((PAIR_ROWS, width), BF16), pltpu.VMEM((PAIR_ROWS, width), BF16),
                        pltpu.VMEM((context.shape[0], 2 * width), BF16)],
        compiler_params=params(), cost_estimate=cost(total * width * width * 16, 40e6), name='cross_backward',
    )(grad, h1, q, out2, kv, context, w_q, w_out, rows)


def self_backward(grad, h, qkv, out1, w_qkv, w_out, rows, tokens, out_dtype):
    total, width = h.shape
    heads = width // HEAD
    row_steps = total // PAIR_ROWS
    cols = 384
    extra = 3 * width // cols
    row = lambda cols: pl.BlockSpec((PAIR_ROWS, cols), lambda step: (jnp.minimum(step, row_steps - 1), 0))
    return pl.pallas_call(
        lambda *refs: self_backward_kernel(heads, tokens, row_steps, *refs),
        grid=(row_steps + extra,),
        in_specs=[row(width), row(width), row(3 * width), row(width), whole(w_qkv.shape), whole(w_out.shape),
                  whole(rows.shape)],
        out_specs=[row(width), pl.BlockSpec((width, cols), lambda step: (0, jnp.maximum(step - row_steps, 0))),
                   whole(w_out.shape), whole(rows.shape)],
        out_shape=[jax.ShapeDtypeStruct((total, width), out_dtype), jax.ShapeDtypeStruct(w_qkv.shape, F32),
                   jax.ShapeDtypeStruct(w_out.shape, F32), jax.ShapeDtypeStruct(rows.shape, F32)],
        scratch_shapes=[pltpu.VMEM((PAIR_ROWS, width), BF16), pltpu.VMEM((total, 3 * width), BF16),
                        pltpu.VMEM((width, total), BF16)],
        compiler_params=params(), cost_estimate=cost(total * width * width * 24, 40e6), name='self_backward',
    )(grad, h, qkv, out1, w_qkv, w_out, rows)


def gather(local):
    return lax.all_gather(local, AXIS, axis=0, tiled=True)


def scatter(grad, total):
    return lax.psum_scatter(grad, AXIS, scatter_dimension=0, tiled=True) / total


def solution(mesh):
    n_dev = mesh.shape[AXIS]

    def local(tokens_x, context, cot_out, *shards):
        samples, tokens, width = tokens_x.shape
        ctx_len, ctx_width = context.shape[1:]
        blocks = shards[0].shape[0]
        total = samples * n_dev
        chunk = PAIR_ROWS
        shapes = weight_shapes(width, ctx_width)
        pieces = [[shard[layer].reshape(shape[0] // n_dev, shape[1]) for shard, shape in zip(shards[:7], shapes[:7])]
                  for layer in range(blocks)]
        vecs = lax.all_gather(shards[7].reshape(1, blocks, -1), AXIS, axis=0, tiled=True)
        vecs = jnp.swapaxes(vecs, 0, 1).reshape(blocks, -1).astype(F32)
        pad = -(-ctx_len // 16) * 16
        ctx_rows = jnp.pad(context, ((0, 0), (0, pad - ctx_len), (0, 0))).reshape(samples * pad, ctx_width)
        h = tokens_x.reshape(samples * tokens, width)
        saved = []
        for layer in range(blocks):
            w_qkv, w_out, w_q2, w_kv2, w_out2, w_ff1, w_ff2 = pieces[layer]
            w_qkv = gather(w_qkv)
            small = gather(jnp.concatenate([w_out, w_q2, w_out2], axis=1))
            w_out, w_q2, w_out2 = (small[:, index * width:(index + 1) * width] for index in range(3))
            w_kv2, w_ff1, w_ff2 = gather(w_kv2), gather(w_ff1), gather(w_ff2)
            rows = jnp.pad(vecs[layer, :9 * width].reshape(9, width), ((0, 7), (0, 0)))
            b1 = vecs[layer, 9 * width:17 * width].reshape(1, 8 * width)
            h1, qkv, out1 = self_forward(h, w_qkv, w_out, rows, tokens)
            h2, q, kv, out2 = cross_forward(h1, ctx_rows, w_q2, w_kv2, w_out2, rows, tokens, ctx_len, samples)
            h3, fa, fg, z = ff_forward(h2, w_ff1, w_ff2, b1, rows, chunk)
            saved.append((h, h1, h2, qkv, out1, q, kv, out2, fa, fg, z, w_qkv, w_out, w_q2, w_out2, w_ff1, w_ff2, rows))
            h = h3
        out_tokens = h.astype(BF16).reshape(tokens_x.shape)
        grad = cot_out.reshape(samples * tokens, width).astype(F32)
        results, vec_grads = [None] * blocks, [None] * blocks
        for layer in reversed(range(blocks)):
            h, h1, h2, qkv, out1, q, kv, out2, fa, fg, z, w_qkv, w_out, w_q2, w_out2, w_ff1, w_ff2, rows = saved[layer]
            grad, d_w1a, d_w1g, d_w2, d_b1, d_rows3 = ff_backward(grad, h2, w_ff1, w_ff2, fa, fg, z, rows, chunk)
            g_ff1 = jnp.concatenate([scatter(d_w1a, total), scatter(d_w1g, total)], axis=1)
            g_ff2 = scatter(d_w2, total)
            grad, d_wq, d_wout2, d_wkv, d_rows2 = cross_backward(grad, h1, q, out2, kv, ctx_rows, w_q2, w_out2, rows,
                                                                 tokens, ctx_len)
            g_q2, g_out2, g_kv2 = scatter(d_wq, total), scatter(d_wout2, total), scatter(d_wkv, total)
            grad, d_wqkv, d_wout, d_rows1 = self_backward(grad, h, qkv, out1, w_qkv, w_out, rows, tokens,
                                                          BF16 if layer == 0 else F32)
            g_qkv, g_out = scatter(d_wqkv, total), scatter(d_wout, total)
            d_rows = (d_rows1 + d_rows2 + d_rows3)[:9].reshape(-1)
            d_b1 = jnp.swapaxes(d_b1[:, :2], 0, 1).reshape(-1)
            vec_grads[layer] = jnp.concatenate([d_rows, d_b1])
            results[layer] = [g_qkv, g_out, g_q2, g_kv2, g_out2, g_ff1, g_ff2]
        vec = jnp.stack(vec_grads).reshape(blocks, n_dev, -1)
        vec = lax.psum_scatter(vec, AXIS, scatter_dimension=1, tiled=False) / total
        stacked = [jnp.stack([result[index].reshape(-1) for result in results]) for index in range(7)]
        return tuple([out_tokens, grad.reshape(tokens_x.shape)] + stacked + [vec])

    param_spec = P(None, AXIS)
    in_specs = (P(AXIS), P(AXIS), P(AXIS)) + (param_spec,) * 8
    out_specs = (P(AXIS), P(AXIS)) + (param_spec,) * 8
    return jax.shard_map(local, mesh=mesh, in_specs=in_specs, out_specs=out_specs, check_vma=False)
```

```python
import functools
import math
from typing import Any, NamedTuple
import jax
import jax.numpy as jnp
from jax import lax
from jax.experimental import pallas as pl
from jax.experimental.pallas import tpu as pltpu
from jax.sharding import PartitionSpec as P

AXIS = 'fsdp'
HEAD = 64
EPS = 1e-5
F32 = jnp.float32
BF16 = jnp.bfloat16
LANES = 128
SLOT = 128
PAIR_ROWS = 512
FF_COLS = 256

TAIL_P = 0.265
TAIL = (0.10574158579953814, 0.10524628753634038, 0.10270369607548423, 0.0603023517537824, 0.13797880111692826,
        -0.11640058407079061, 0.2178489286936914, -0.1442454807654402, 0.03082441619112092)


def weight_shapes(width, ctx_width):
    return ((width, 3 * width), (width, width), (width, width), (ctx_width, 2 * width),
            (width, width), (width, 8 * width), (4 * width, width), (17 * width,))


def mm(lhs, rhs):
    return jnp.dot(lhs, rhs, preferred_element_type=F32)


def mm_nt(lhs, rhs):
    return lax.dot_general(lhs, rhs, (((1,), (1,)), ((), ())), preferred_element_type=F32)


def mm_tn(lhs, rhs):
    return lax.dot_general(lhs, rhs, (((0,), (0,)), ((), ())), preferred_element_type=F32)


def normalize(x):
    centered = x - jnp.mean(x, axis=-1, keepdims=True)
    scale = lax.rsqrt(jnp.mean(centered * centered, axis=-1, keepdims=True) + EPS)
    return centered * scale, scale


def norm_back(x, d_norm, gain):
    hat, scale = normalize(x)
    d_hat = d_norm * gain
    pulled = d_hat - jnp.mean(d_hat, axis=-1, keepdims=True) - hat * jnp.mean(d_hat * hat, axis=-1, keepdims=True)
    return pulled * scale, jnp.sum(d_norm * hat, axis=0, keepdims=True), jnp.sum(d_norm, axis=0, keepdims=True)


def low_half(rows):
    return lax.broadcasted_iota(jnp.int32, (rows, LANES), 1) < HEAD


def head_stack(pair, low):
    zero = jnp.zeros_like(pair)
    return jnp.concatenate([jnp.where(low, pair, zero), jnp.where(low, zero, pair)], axis=0)


def head_unstack(stacked, low):
    half = stacked.shape[0] // 2
    return jnp.where(low, stacked[:half], stacked[half:])


def softmax_halves(scores, valid):
    half = scores.shape[1] // 2
    parts = []
    for index in range(2):
        part = scores[:, index * half:(index + 1) * half]
        if valid < half:
            part = jnp.where(lax.broadcasted_iota(jnp.int32, part.shape, 1) < valid, part, -jnp.inf)
        part = jnp.exp(part - jnp.max(part, axis=-1, keepdims=True))
        parts.append(part * (1.0 / jnp.sum(part, axis=-1, keepdims=True)))
    return parts


def pair_forward(query, keys, values, valid):
    low = low_half(keys.shape[0])
    scores = mm_nt(query * BF16(HEAD ** -0.5), head_stack(keys, low))
    probs = jnp.concatenate([part.astype(BF16) for part in softmax_halves(scores, valid)], axis=1)
    return mm(probs, head_stack(values, low)).astype(BF16)


def pair_backward(query, keys, values, d_out, valid):
    low = low_half(keys.shape[0])
    half = keys.shape[0]
    query = query * BF16(HEAD ** -0.5)
    key_stack = head_stack(keys, low)
    value_stack = head_stack(values, low)
    parts = softmax_halves(mm_nt(query, key_stack), valid)
    probs = jnp.concatenate([part.astype(BF16) for part in parts], axis=1)
    d_values = head_unstack(mm_tn(probs, d_out), low).astype(BF16)
    d_probs = mm_nt(d_out, value_stack)
    d_scores = []
    for index in range(2):
        part, d_part = parts[index], d_probs[:, index * half:(index + 1) * half]
        d_scores.append((part * (d_part - jnp.sum(part * d_part, axis=-1, keepdims=True))).astype(BF16))
    d_scores = jnp.concatenate(d_scores, axis=1)
    d_query = (mm(d_scores, key_stack) * HEAD ** -0.5).astype(BF16)
    d_keys = head_unstack(mm_tn(d_scores, query), low).astype(BF16)
    return d_query, d_keys, d_values


def self_forward_kernel(heads, tokens, h_ref, w_qkv_ref, w_out_ref, rows_ref, h1_ref, qkv_ref, out_ref):
    width = heads * HEAD
    hat, unused = normalize(h_ref[...].astype(F32))
    norm1 = (hat * rows_ref[0:1] + rows_ref[1:2]).astype(BF16)
    qkv_ref[...] = mm(norm1, w_qkv_ref[...]).astype(BF16)

    def sample(index, carry):
        rows = pl.ds(pl.multiple_of(index * tokens, tokens), tokens)
        for pair in range(heads // 2):
            cols = pair * LANES
            out_ref[rows, cols:cols + LANES] = pair_forward(
                qkv_ref[rows, cols:cols + LANES], qkv_ref[rows, width + cols:width + cols + LANES],
                qkv_ref[rows, 2 * width + cols:2 * width + cols + LANES], tokens)
        return carry

    lax.fori_loop(0, h_ref.shape[0] // tokens, sample, 0)
    h1_ref[...] = h_ref[...].astype(F32) + mm(out_ref[...], w_out_ref[...]) + rows_ref[6:7]


def cross_forward_kernel(heads, tokens, ctx_len, h1_ref, context_ref, w_q_ref, w_kv_ref, w_out_ref, rows_ref,
                         h2_ref, q_ref, kv_ref, out_ref):
    width = heads * HEAD
    samples = kv_ref.shape[0] // SLOT
    pad = context_ref.shape[0] // samples
    step = pl.program_id(0)

    @pl.when(step == 0)
    def _():
        kv = mm(context_ref[...], w_kv_ref[...]).astype(BF16)
        for index in range(samples):
            kv_ref[index * SLOT:index * SLOT + pad] = kv[index * pad:(index + 1) * pad]
            kv_ref[index * SLOT + pad:(index + 1) * SLOT] = jnp.zeros((SLOT - pad, 2 * width), BF16)

    hat, unused = normalize(h1_ref[...])
    norm2 = (hat * rows_ref[2:3] + rows_ref[3:4]).astype(BF16)
    q_ref[...] = mm(norm2, w_q_ref[...]).astype(BF16)
    per_step = h1_ref.shape[0] // tokens

    def sample(index, carry):
        rows = pl.ds(pl.multiple_of(index * tokens, tokens), tokens)
        kv_rows = pl.ds(pl.multiple_of((step * per_step + index) * SLOT, SLOT), SLOT)
        for pair in range(heads // 2):
            cols = pair * LANES
            out_ref[rows, cols:cols + LANES] = pair_forward(
                q_ref[rows, cols:cols + LANES], kv_ref[kv_rows, cols:cols + LANES],
                kv_ref[kv_rows, width + cols:width + cols + LANES], ctx_len)
        return carry

    lax.fori_loop(0, per_step, sample, 0)
    h2_ref[...] = h1_ref[...] + mm(out_ref[...], w_out_ref[...]) + rows_ref[7:8]


def normal_cdf(u):
    t = 1.0 / (1.0 + TAIL_P * jnp.abs(u))
    poly = TAIL[-1]
    for coef in TAIL[-2::-1]:
        poly = poly * t + coef
    bell = jnp.exp(u * u * -0.5)
    tail = bell * (t * poly)
    return jnp.where(u >= 0, 1.0 - tail, tail), bell


def ff_forward_kernel(chunk, h2_ref, w1a_ref, w1g_ref, w2_ref, b1a_ref, b1g_ref, rows_ref,
                      h3_ref, fa_ref, fg_ref, z_ref, norm_ref, acc_ref):
    step = pl.program_id(0)
    chunks = h2_ref.shape[0] // chunk

    @pl.when(step == 0)
    def _():
        def start(index, carry):
            rows = pl.ds(pl.multiple_of(index * chunk, chunk), chunk)
            hat, unused = normalize(h2_ref[rows])
            norm_ref[rows] = (hat * rows_ref[4:5] + rows_ref[5:6]).astype(BF16)
            acc_ref[rows] = jnp.zeros((chunk, h2_ref.shape[1]), F32)
            return carry

        lax.fori_loop(0, chunks, start, 0)

    def body(index, carry):
        rows = pl.ds(pl.multiple_of(index * chunk, chunk), chunk)
        norm3 = norm_ref[rows]
        gate = mm(norm3, w1g_ref[...]) + b1g_ref[...]
        cdf, bell = normal_cdf(gate)
        factor = gate * cdf
        value = mm(norm3, w1a_ref[...]) + b1a_ref[...]
        z = (value * factor).astype(BF16)
        z_ref[0, rows] = z
        fa_ref[0, rows] = factor
        fg_ref[0, rows] = value * (cdf + gate * bell * (2 * math.pi) ** -0.5)
        acc_ref[rows] += mm(z, w2_ref[...])
        return carry

    lax.fori_loop(0, chunks, body, 0)

    @pl.when(step == pl.num_programs(0) - 1)
    def _():
        h3_ref[...] = h2_ref[...] + acc_ref[...] + rows_ref[8:9]


def whole(shape):
    return pl.BlockSpec(shape, lambda step: (0,) * len(shape))


def params(**extra):
    return pltpu.CompilerParams(dimension_semantics=('arbitrary',), vmem_limit_bytes=62 * 1024 * 1024, **extra)


def cost(flops, moved):
    return pl.CostEstimate(flops=int(flops), bytes_accessed=int(moved), transcendentals=0)


def self_forward(h, w_qkv, w_out, rows, tokens):
    total, width = h.shape
    heads = width // HEAD
    row = lambda cols: pl.BlockSpec((PAIR_ROWS, cols), lambda step: (step, 0))
    return pl.pallas_call(
        lambda *refs: self_forward_kernel(heads, tokens, *refs),
        grid=(total // PAIR_ROWS,),
        in_specs=[row(width), whole(w_qkv.shape), whole(w_out.shape), whole(rows.shape)],
        out_specs=[row(width), row(3 * width), row(width)],
        out_shape=[jax.ShapeDtypeStruct((total, width), F32), jax.ShapeDtypeStruct((total, 3 * width), BF16),
                   jax.ShapeDtypeStruct((total, width), BF16)],
        compiler_params=params(), cost_estimate=cost(total * width * width * 10, 20e6), name='self_forward',
    )(h, w_qkv, w_out, rows)


def cross_forward(h1, context, w_q, w_kv, w_out, rows, tokens, ctx_len, samples):
    total, width = h1.shape
    heads = width // HEAD
    row = lambda cols: pl.BlockSpec((PAIR_ROWS, cols), lambda step: (step, 0))
    return pl.pallas_call(
        lambda *refs: cross_forward_kernel(heads, tokens, ctx_len, *refs),
        grid=(total // PAIR_ROWS,),
        in_specs=[row(width), whole(context.shape), whole(w_q.shape), whole(w_kv.shape), whole(w_out.shape),
                  whole(rows.shape)],
        out_specs=[row(width), row(width), whole((samples * SLOT, 2 * width)), row(width)],
        out_shape=[jax.ShapeDtypeStruct((total, width), F32), jax.ShapeDtypeStruct((total, width), BF16),
                   jax.ShapeDtypeStruct((samples * SLOT, 2 * width), BF16), jax.ShapeDtypeStruct((total, width), BF16)],
        compiler_params=params(), cost_estimate=cost(total * width * width * 8, 20e6), name='cross_forward',
    )(h1, context, w_q, w_kv, w_out, rows)


def ff_forward(h2, w1, w2, b1, rows, chunk):
    total, width = h2.shape
    inner = w2.shape[0]
    steps = inner // FF_COLS
    saved = pl.BlockSpec((1, total, FF_COLS), lambda step: (step, 0, 0))
    return pl.pallas_call(
        lambda *refs: ff_forward_kernel(chunk, *refs),
        grid=(steps,),
        in_specs=[whole(h2.shape), pl.BlockSpec((width, FF_COLS), lambda step: (0, step)),
                  pl.BlockSpec((width, FF_COLS), lambda step: (0, step + steps)),
                  pl.BlockSpec((FF_COLS, width), lambda step: (step, 0)),
                  pl.BlockSpec((1, FF_COLS), lambda step: (0, step)),
                  pl.BlockSpec((1, FF_COLS), lambda step: (0, step + steps)), whole(rows.shape)],
        out_specs=[whole(h2.shape), saved, saved, saved],
        out_shape=[jax.ShapeDtypeStruct((total, width), F32), jax.ShapeDtypeStruct((steps, total, FF_COLS), F32),
                   jax.ShapeDtypeStruct((steps, total, FF_COLS), F32), jax.ShapeDtypeStruct((steps, total, FF_COLS), BF16)],
        scratch_shapes=[pltpu.VMEM((total, width), BF16), pltpu.VMEM((total, width), F32)],
        compiler_params=params(), cost_estimate=cost(total * width * inner * 6, 60e6), name='ff_forward',
    )(h2, w1, w1, w2, b1, b1, rows)


UNIT = 80
MACRO = 3 * UNIT
SLOTS = 3
STREAMS = 2
STAGES = 4
ORDERS = ((2, 1, 0), (1, 0, 2), (0, 2, 1))
MESH = pl.DeviceIdType.MESH


class Place:
    def __init__(self):
        me = lax.axis_index(AXIS)
        self.bits = [lax.rem(lax.div(me, weight), 2) for weight in (8, 4, 2, 1)]
        self.others = [1 - bit for bit in self.bits]
        self.devices = [(me + (1 - 2 * bit) * weight,) for bit, weight in zip(self.bits, (8, 4, 2, 1))]

    def entry_barrier(self):
        barrier = pltpu.get_barrier_semaphore()
        for device in self.devices:
            pl.semaphore_signal(barrier, inc=1, device_id=device, device_id_type=MESH)
        pl.semaphore_wait(barrier, 4)


def pick(ref, lead, dim, value):
    return ref.at[(lead,) + (slice(None),) * dim + (value,)]


class At(NamedTuple):
    stream: Any
    index: Any
    row: Any


class Reducer:
    def __init__(self, place, macros, scale, grads, out, refs):
        self.place, self.macros, self.scale, self.grads, self.out = place, macros, scale, grads, out
        self.own, self.held = refs[0], refs[1:1 + STAGES]
        self.result, self.send, self.recv, self.load, self.store = refs[1 + STAGES:]

    @staticmethod
    def scratch():
        held = [pltpu.VMEM((STREAMS * SLOTS * 3,) + (2,) * (3 - stage) + (UNIT, LANES), F32) for stage in range(STAGES)]
        sems = [pltpu.SemaphoreType.DMA((STREAMS, 3, STAGES)), pltpu.SemaphoreType.DMA((STREAMS * SLOTS * 3, STAGES)),
                pltpu.SemaphoreType.DMA((STREAMS, 3)), pltpu.SemaphoreType.DMA((STREAMS,))]
        return [pltpu.VMEM((STREAMS * 3, 2, 2, 2, UNIT, LANES), F32)] + held + [
            pltpu.VMEM((STREAMS, MACRO, LANES), F32)] + sems

    def axis(self, color, stage):
        return 3 if stage == 0 else ORDERS[color][stage - 1]

    def dim(self, color, stage):
        gone = ORDERS[color][:stage - 1]
        return sum(1 for axis in range(ORDERS[color][stage - 1]) if axis not in gone)

    def copy(self, at, color, stage):
        axis = self.axis(color, stage)
        other = self.place.others[axis]
        index = at.index + color
        if stage == 0:
            source = self.grads.at[:, :, :, other, pl.ds(at.row + color * UNIT, UNIT)]
        else:
            source = pick(self.held[stage - 1], index, self.dim(color, stage), other)
        return pltpu.make_async_remote_copy(
            src_ref=source, dst_ref=self.held[stage].at[index], send_sem=self.send.at[at.stream, color, stage],
            recv_sem=self.recv.at[index, stage], device_id=self.place.devices[axis], device_id_type=MESH)

    def own_copy(self, at, color):
        return pltpu.make_async_copy(self.grads.at[:, :, :, self.place.bits[3], pl.ds(at.row + color * UNIT, UNIT)],
                                     self.own.at[at.stream * 3 + color], self.load.at[at.stream, color])

    def out_copy(self, stream, row):
        return pltpu.make_async_copy(self.result.at[stream], self.out.at[pl.ds(row, MACRO)], self.store.at[stream])

    def add(self, at, color, stage):
        index = at.index + color
        if stage == 0:
            self.held[0][index] += self.own[at.stream * 3 + color]
            return
        mine = self.held[stage - 1][(index,) + (slice(None),) * self.dim(color, stage)
                                    + (self.place.bits[self.axis(color, stage)],)]
        if stage < STAGES - 1:
            self.held[stage][index] += mine
        else:
            self.result[at.stream, color * UNIT:(color + 1) * UNIT] = (self.held[stage][index] + mine) * self.scale

    def step(self, t):
        stream, tau = lax.rem(t, STREAMS), lax.div(t, STREAMS)

        def when_live(local, body):
            @pl.when((local >= 0) & (local * STREAMS + stream < self.macros))
            def _():
                body(At(stream, (stream * SLOTS + lax.rem(local, SLOTS)) * 3,
                        pl.multiple_of((local * STREAMS + stream) * MACRO, 8)))

        def take(stage, at):
            for color in range(3):
                copy = self.copy(at, color, stage)
                copy.wait_send()
                copy.wait_recv()
                if stage == 0:
                    self.own_copy(at, color).wait()
            if stage == STAGES - 1:
                @pl.when(tau > STAGES)
                def _():
                    self.out_copy(stream, pl.multiple_of(at.row - STREAMS * MACRO, 8)).wait()
            for color in range(3):
                self.add(at, color, stage)
            if stage == STAGES - 1:
                self.out_copy(stream, at.row).start()

        def give(stage, at):
            for color in range(3):
                self.copy(at, color, stage).start()
                if stage == 0:
                    self.own_copy(at, color).start()

        for stage in reversed(range(STAGES)):
            when_live(tau - 1 - stage, functools.partial(take, stage))
        for stage in range(STAGES):
            when_live(tau - stage, functools.partial(give, stage))

    def run(self, start, count):
        lax.fori_loop(0, count, lambda index, carry: (self.step(start + index), carry)[1], 0)

    def finish(self, start):
        self.run(start, self.macros + STREAMS * STAGES - start)
        for stream in range(STREAMS):
            last = (self.macros - 1 - stream) // STREAMS * STREAMS + stream
            self.out_copy(stream, last * MACRO).wait()


def view(values, *lead):
    return values.reshape((2, 2, 2, 2) + lead + (LANES,))


def put_tiles(stage, values, first=0):
    rows = values.shape[0] // 16
    for tile in range(values.shape[1] // LANES):
        at = first + tile * rows
        stage[:, :, :, :, at:at + rows] = view(values[:, tile * LANES:(tile + 1) * LANES], rows)


class Layout:
    def __init__(self, width, ctx_width, blocks):
        unit = width // 16 * (width // LANES)
        self.ff1, self.ff2 = 0, 8 * unit
        self.kv2 = 12 * unit
        self.q2 = self.kv2 + ctx_width // 16 * (2 * width // LANES)
        self.out2 = self.q2 + unit
        self.qkv = self.out2 + unit
        self.out = self.qkv + 3 * unit
        self.block = self.out + unit
        self.vec = blocks * self.block
        self.vec_rows = -(-17 * width // 16 // LANES // 8) * 8
        used = self.vec + blocks * self.vec_rows
        self.macros = -(-used // MACRO)
        self.pad = self.macros * MACRO - used
        self.rows = self.macros * MACRO


NAMES = ('h', 'h1', 'h2', 'qkv', 'out1', 'q', 'kv', 'out2', 'fa', 'fg', 'z', 'w_qkv', 'w_out', 'w_q2', 'w_out2', 'w_ff1',
         'w_ff2', 'rows')


def backward_kernel(cfg, *refs):
    tokens, ctx_len, width, blocks, layout, total, plan = cfg
    heads = width // HEAD
    cot_ref, context_ref = refs[:2]
    saved = [dict(zip(NAMES, refs[2 + layer * len(NAMES):])) for layer in range(blocks)]
    refs = refs[2 + blocks * len(NAMES):]
    gx_ref, grads_ref, out_ref = refs[:3]
    grad_ref, hidden_ref, rows_ref, d_rows_ref, vec_ref, in_sems = refs[3:9]
    place = Place()
    reducer = Reducer(place, layout.macros, 1.0 / total, grads_ref, out_ref, refs[9:])
    count = grad_ref.shape[0]
    chunk = PAIR_ROWS
    chunks = count // chunk
    phases = [(layer, kind) for layer in reversed(range(blocks)) for kind in ('h2', 'h1', 'h')]

    def hidden_copy(index):
        layer, kind = phases[index]
        return pltpu.make_async_copy(saved[layer][kind], hidden_ref.at[index % 2], in_sems.at[index % 2])

    def rows_copy(layer):
        return pltpu.make_async_copy(saved[layer]['rows'], rows_ref.at[layer], in_sems.at[2 + layer])

    def base(layer):
        return (blocks - 1 - layer) * layout.block

    def region(row, size):
        return grads_ref.at[:, :, :, :, pl.ds(pl.multiple_of(row, 8), size)]

    def each_chunk(body):
        def one(index, carry):
            body(pl.ds(pl.multiple_of(index * chunk, chunk), chunk))
            return carry
        lax.fori_loop(0, chunks, one, 0)

    def ff_phase(layer, index, first):
        hidden = hidden_ref.at[index % 2]
        rows = rows_ref.at[layer]
        d_rows = d_rows_ref.at[layer]
        vec = vec_ref.at[layer]
        src = saved[layer]
        inner = src['w_ff2'].shape[0]
        steps = inner // FF_COLS
        start, lag, limit = first

        def scoped(norm_t, grad_bf, du, w1, acc, stage1, stage2, sem1, sem2):
            def begin(at):
                hat, unused = normalize(hidden[at])
                norm_t[:, at] = (hat * rows[4:5] + rows[5:6]).astype(BF16).T
                grad_bf[at] = grad_ref[at].astype(BF16)
                d_rows[8:9] += jnp.sum(grad_ref[at], axis=0, keepdims=True)
                acc[at] = jnp.zeros((chunk, width), F32)

            each_chunk(begin)

            def copy1(step):
                return pltpu.make_async_copy(stage1, region(base(layer) + layout.ff1 + step * 160, 160), sem1)

            def copy2(step, part):
                block = step * 8 + part
                shard = lax.div(block, 5)
                row = pl.multiple_of(base(layer) + layout.ff2 + lax.rem(block, 5) * 160, 8)
                bits = [lax.rem(lax.div(shard, weight), 2) for weight in (8, 4, 2, 1)]
                return pltpu.make_async_copy(stage2.at[part], grads_ref.at[(*bits, pl.ds(row, 160))], sem2.at[part])

            def wait(step):
                copy1(step).wait()
                for part in range(8):
                    copy2(step, part).wait()

            def body(idx, w1a, w1g, w2, fa, fg, z):
                step = idx.index[0]
                w1[:, :FF_COLS] = w1a[...]
                w1[:, FF_COLS:] = w1g[...]

                def part(number, sums):
                    at = pl.ds(pl.multiple_of(number * chunk, chunk), chunk)
                    dz = mm_nt(grad_bf[at], w2[...]).astype(BF16).astype(F32)
                    du_a = dz * fa[0, at]
                    du_g = dz * fg[0, at]
                    du[at, :FF_COLS] = du_a.astype(BF16)
                    du[at, FF_COLS:] = du_g.astype(BF16)
                    acc[at] += mm_nt(du[at], w1[...])
                    return (sums[0] + jnp.sum(du_a, axis=0, keepdims=True), sums[1] + jnp.sum(du_g, axis=0, keepdims=True))

                zero = jnp.zeros((1, FF_COLS), F32)
                sums = lax.fori_loop(0, chunks, part, (zero, zero))
                for half in range(2):
                    for tile in range(2):
                        row = 9 * width // LANES + half * (inner // LANES) + 2 * step + tile
                        vec[pl.ds(row, 1)] = sums[half][:, tile * LANES:(tile + 1) * LANES]

                @pl.when(step > 0)
                def _():
                    wait(step - 1)

                if limit > 0:
                    @pl.when((step >= lag) & (step < lag + limit))
                    def _():
                        reducer.step(start + step - lag)

                put_tiles(stage1, mm(norm_t[...], du[:, :FF_COLS]))
                put_tiles(stage1, mm(norm_t[...], du[:, FF_COLS:]), 80)
                d_w2 = mm_tn(z[0], grad_bf[...])
                for tile in range(width // LANES):
                    stage2[:, tile * 32:(tile + 1) * 32] = d_w2[:, tile * LANES:(tile + 1) * LANES].reshape(8, 32, LANES)
                copy1(step).start()
                for number in range(8):
                    copy2(step, number).start()

            column = pl.BlockSpec((width, FF_COLS), lambda step: (0, step))
            kept = pl.BlockSpec((1, count, FF_COLS), lambda step: (step, 0, 0))
            pltpu.emit_pipeline(
                body, grid=(steps,),
                in_specs=[column, pl.BlockSpec((width, FF_COLS), lambda step: (0, step + steps)),
                          pl.BlockSpec((FF_COLS, width), lambda step: (step, 0)), kept, kept, kept],
                _explicit_indices=True,
            )(src['w_ff1'], src['w_ff1'], src['w_ff2'], src['fa'], src['fg'], src['z'])

            def finish(at):
                d_res, d_gain, d_shift = norm_back(hidden[at], acc[at], rows[4:5])
                grad_ref[at] += d_res
                d_rows[4:5] += d_gain
                d_rows[5:6] += d_shift

            each_chunk(finish)
            wait(steps - 1)

        pl.run_scoped(scoped, pltpu.VMEM((width, count), BF16), pltpu.VMEM((count, width), BF16),
                      pltpu.VMEM((count, 2 * FF_COLS), BF16), pltpu.VMEM((width, 2 * FF_COLS), BF16),
                      pltpu.VMEM((count, width), F32), pltpu.VMEM((2, 2, 2, 2, 160, LANES), F32),
                      pltpu.VMEM((8, 160, LANES), F32), pltpu.SemaphoreType.DMA, pltpu.SemaphoreType.DMA((8,)))

    def attention_phase(layer, index, first, cross):
        hidden = hidden_ref.at[index % 2]
        rows = rows_ref.at[layer]
        d_rows = d_rows_ref.at[layer]
        src = saved[layer]
        steps = count // PAIR_ROWS
        per_step = PAIR_ROWS // tokens
        start, in_samples, in_tails = first
        gain, shift, bias = (2, 3, 7) if cross else (0, 1, 6)
        samples = count // tokens
        pad = context_ref.shape[0] // samples
        kv_rows_all = context_ref.shape[0] if cross else count

        def scoped(d_mix, d_q, d_kv, norm_t, d_wq, d_wout, stage, stage_out, sem, sem_out, context, kv, ctx_sems):
            if cross:
                loads = [pltpu.make_async_copy(context_ref, context, ctx_sems.at[0]),
                         pltpu.make_async_copy(src['kv'], kv, ctx_sems.at[1])]
                for copy in loads:
                    copy.start()
                d_wq[...] = jnp.zeros_like(d_wq)
                for copy in loads:
                    copy.wait()
            d_wout[...] = jnp.zeros_like(d_wout)

            def body(idx, qkv, mixed, w_in, w_out):
                step = idx.index[0]
                at_rows = pl.ds(pl.multiple_of(step * PAIR_ROWS, PAIR_ROWS), PAIR_ROWS)
                grad_bf = grad_ref[at_rows].astype(BF16)
                d_rows[bias:bias + 1] += jnp.sum(grad_ref[at_rows], axis=0, keepdims=True)
                d_wout[...] += mm_tn(mixed[...], grad_bf)
                d_mix[...] = mm_nt(grad_bf, w_out[...]).astype(BF16)

                def sample(number, carry):
                    at = pl.ds(pl.multiple_of(number * tokens, tokens), tokens)
                    sample_index = step * per_step + number
                    if cross:
                        kv_at = pl.ds(pl.multiple_of(sample_index * SLOT, SLOT), SLOT)
                        d_kv_at = pl.ds(pl.multiple_of(sample_index * pad, pad), pad)
                        d_q_at = at
                    else:
                        d_q_at = pl.ds(pl.multiple_of(sample_index * tokens, tokens), tokens)
                    for pair in range(heads // 2):
                        cols = slice(pair * LANES, (pair + 1) * LANES)
                        k_cols = slice(width + pair * LANES, width + (pair + 1) * LANES)
                        v_cols = slice(2 * width + pair * LANES, 2 * width + (pair + 1) * LANES)
                        if cross:
                            d_query, d_keys, d_values = pair_backward(qkv[at, cols], kv[kv_at, cols], kv[kv_at, k_cols],
                                                                      d_mix[at, cols], ctx_len)
                            d_kv[d_kv_at, cols] = d_keys[:pad]
                            d_kv[d_kv_at, k_cols] = d_values[:pad]
                        else:
                            d_query, d_keys, d_values = pair_backward(qkv[at, cols], qkv[at, k_cols], qkv[at, v_cols],
                                                                      d_mix[at, cols], tokens)
                            d_q[d_q_at, k_cols] = d_keys
                            d_q[d_q_at, v_cols] = d_values
                        d_q[d_q_at, cols] = d_query
                    @pl.when(sample_index < in_samples)
                    def _():
                        reducer.step(start + sample_index)

                    return carry

                lax.fori_loop(0, per_step, sample, 0)
                hat, unused = normalize(hidden[at_rows])
                norm = (hat * rows[gain:gain + 1] + rows[shift:shift + 1]).astype(BF16)
                if cross:
                    d_wq[...] += mm_tn(norm, d_q[...])
                    d_norm = mm_nt(d_q[...], w_in[...])
                else:
                    norm_t[:, at_rows] = norm.T
                    d_norm = mm_nt(d_q[at_rows], w_in[...])
                d_res, d_gain, d_shift = norm_back(hidden[at_rows], d_norm, rows[gain:gain + 1])
                grad_ref[at_rows] += d_res
                d_rows[gain:gain + 1] += d_gain
                d_rows[shift:shift + 1] += d_shift

            w_in, w_out = ('w_q2', 'w_out2') if cross else ('w_qkv', 'w_out')
            block = lambda ref: pl.BlockSpec((PAIR_ROWS, ref.shape[1]), lambda step: (step, 0))
            full = lambda ref: pl.BlockSpec(ref.shape, lambda step: (0, 0))
            operands = [src['q' if cross else 'qkv'], src['out2' if cross else 'out1'], src[w_in], src[w_out]]
            pltpu.emit_pipeline(
                body, grid=(steps,), in_specs=[block(operands[0]), block(operands[1]), full(operands[2]), full(operands[3])],
                _explicit_indices=True,
            )(*operands)
            where = base(layer) + (layout.out2 if cross else layout.out)
            size = width // 16 * (width // LANES)
            if cross:
                put_tiles(stage_out, d_wq[...])
                put_tiles(stage_out, d_wout[...], size)
                copy_out = pltpu.make_async_copy(stage_out, region(base(layer) + layout.q2, 2 * size), sem_out)
            else:
                put_tiles(stage_out, d_wout[...])
                copy_out = pltpu.make_async_copy(stage_out, region(where, size), sem_out)
            copy_out.start()
            rows_each = stage.shape[4]
            cols_each = stage.shape[4] // ((context_ref.shape[1] if cross else width) // 16) * LANES
            tails = (2 if cross else 3) * width // cols_each
            first_row = base(layer) + (layout.kv2 if cross else layout.qkv)

            def copy_tail(step):
                return pltpu.make_async_copy(stage, region(first_row + step * rows_each, rows_each), sem)

            def tail(step, carry):
                cols = pl.ds(pl.multiple_of(step * cols_each, cols_each), cols_each)
                result = mm_tn(context[...], d_kv[:, cols]) if cross else mm(norm_t[...], d_q[:, cols])

                @pl.when(step > 0)
                def _():
                    copy_tail(step - 1).wait()

                put_tiles(stage, result)
                copy_tail(step).start()
                if in_tails:
                    @pl.when(step < in_tails)
                    def _():
                        reducer.step(start + in_samples + step)

                return carry

            lax.fori_loop(0, tails, tail, 0)
            copy_tail(tails - 1).wait()
            copy_out.wait()

        small = pltpu.VMEM((8, LANES), BF16)
        size = width // 16 * (width // LANES)
        if cross:
            ctx_width = context_ref.shape[1]
            pl.run_scoped(scoped, pltpu.VMEM((PAIR_ROWS, width), BF16), pltpu.VMEM((PAIR_ROWS, width), BF16),
                          pltpu.VMEM((kv_rows_all, 2 * width), BF16), small, pltpu.VMEM((width, width), F32),
                          pltpu.VMEM((width, width), F32), pltpu.VMEM((2, 2, 2, 2, ctx_width // 16 * 2, LANES), F32),
                          pltpu.VMEM((2, 2, 2, 2, 2 * size, LANES), F32), pltpu.SemaphoreType.DMA,
                          pltpu.SemaphoreType.DMA, pltpu.VMEM(context_ref.shape, BF16),
                          pltpu.VMEM(src['kv'].shape, BF16), pltpu.SemaphoreType.DMA((2,)))
        else:
            pl.run_scoped(scoped, pltpu.VMEM((PAIR_ROWS, width), BF16), pltpu.VMEM((count, 3 * width), BF16), small,
                          pltpu.VMEM((width, count), BF16), small, pltpu.VMEM((width, width), F32),
                          pltpu.VMEM((2, 2, 2, 2, width // 16 * 3, LANES), F32),
                          pltpu.VMEM((2, 2, 2, 2, size, LANES), F32), pltpu.SemaphoreType.DMA,
                          pltpu.SemaphoreType.DMA, small, small, pltpu.SemaphoreType.DMA((2,)))

    place.entry_barrier()
    hidden_copy(0).start()
    for layer in range(blocks):
        rows_copy(layer).start()
    d_rows_ref[...] = jnp.zeros_like(d_rows_ref)
    vec_ref[...] = jnp.zeros_like(vec_ref)

    def load_cot(cot, sem):
        copy = pltpu.make_async_copy(cot_ref, cot, sem)
        copy.start()
        copy.wait()
        each_chunk(lambda at: grad_ref.__setitem__(at, cot[at].astype(F32)))

    pl.run_scoped(load_cot, pltpu.VMEM(cot_ref.shape, BF16), pltpu.SemaphoreType.DMA)
    for layer in range(blocks):
        rows_copy(layer).wait()
    for index, (layer, kind) in enumerate(phases):
        hidden_copy(index).wait()
        if index + 1 < len(phases):
            hidden_copy(index + 1).start()
        if kind == 'h2':
            ff_phase(layer, index, plan[index])
        else:
            attention_phase(layer, index, plan[index], kind == 'h1')

    def finish(stage, sem, image, sem_image):
        def cast(at):
            image[at] = grad_ref[at].astype(BF16)

        each_chunk(cast)
        copy_image = pltpu.make_async_copy(image, gx_ref, sem_image)
        copy_image.start()
        per_device = 17 * width // 16
        stage[...] = jnp.zeros_like(stage)
        for layer in range(blocks):
            vec = vec_ref.at[layer]
            for row in range(9):
                for tile in range(width // LANES):
                    at = row * (width // LANES) + tile
                    vec[at:at + 1] = d_rows_ref[layer, row:row + 1, tile * LANES:(tile + 1) * LANES]
            lane = lax.broadcasted_iota(jnp.int32, (8, LANES), 1)
            for shard in range(16):
                row, off = divmod(shard * per_device, LANES)
                here, after = vec[row:row + 8], vec[row + 1:row + 9]
                if off:
                    here = jnp.where(lane < LANES - off, pltpu.roll(here, LANES - off, 1), pltpu.roll(after, LANES - off, 1))
                stage[shard // 8, shard // 4 % 2, shard // 2 % 2, shard % 2,
                      layer * layout.vec_rows:(layer + 1) * layout.vec_rows] = here
        copy = pltpu.make_async_copy(stage, region(layout.vec, stage.shape[4]), sem)
        copy.start()
        copy.wait()
        reducer.finish(plan[-1])
        copy_image.wait()

    pl.run_scoped(finish, pltpu.VMEM((2, 2, 2, 2, blocks * layout.vec_rows + layout.pad, LANES), F32),
                  pltpu.SemaphoreType.DMA, pltpu.VMEM(cot_ref.shape, BF16), pltpu.SemaphoreType.DMA)


def backward(cot, context, saved, tokens, ctx_len, total):
    count, width = cot.shape
    blocks = len(saved)
    layout = Layout(width, context.shape[1], blocks)
    cfg = (tokens, ctx_len, width, blocks, layout, total, PLAN)
    operands = [cot, context]
    for block in saved:
        operands += [block[name] for name in NAMES]
    any_spec = pl.BlockSpec(memory_space=pl.ANY)
    shape = saved[0]['rows'].shape
    gx, unused, out = pl.pallas_call(
        lambda *refs: backward_kernel(cfg, *refs),
        in_specs=[any_spec] * len(operands), out_specs=[any_spec] * 3,
        out_shape=[jax.ShapeDtypeStruct((count, width), BF16),
                   jax.ShapeDtypeStruct((2, 2, 2, 2, layout.rows, LANES), F32),
                   jax.ShapeDtypeStruct((layout.rows, LANES), F32)],
        scratch_shapes=[pltpu.VMEM((count, width), F32), pltpu.VMEM((2, count, width), F32),
                        pltpu.VMEM((blocks,) + shape, F32), pltpu.VMEM((blocks,) + shape, F32),
                        pltpu.VMEM((blocks, 96, LANES), F32), pltpu.SemaphoreType.DMA((2 + blocks,))] + Reducer.scratch(),
        compiler_params=pltpu.CompilerParams(collective_id=0, has_side_effects=True, vmem_limit_bytes=63 * 1024 * 1024),
        cost_estimate=cost(110e9, 300e6), name='backward',
    )(*operands)
    return gx, out, layout


PLAN = [(0, 4, 6), (6, 4, 0), (10, 6, 1), (17, 0, 8), (25, 5, 0), (30, 6, 1), 37]


def gather(local):
    return lax.all_gather(local, AXIS, axis=0, tiled=True)


def ungrad(out, layout, layer, blocks, width, ctx_width):
    rows = out[(blocks - 1 - layer) * layout.block:(blocks - layer) * layout.block]
    part = width // 16
    tiles = width // LANES
    inner = 4 * width

    def square(first, count):
        return rows[first:first + count * tiles * part].reshape(count * tiles, part, LANES).swapaxes(0, 1).reshape(-1)

    ff1 = rows[:layout.ff2].reshape(inner // FF_COLS, 2, FF_COLS // LANES, part, LANES)
    ff1 = ff1.transpose(3, 1, 0, 2, 4).reshape(-1)
    ff2 = rows[layout.ff2:layout.kv2].reshape(inner // 16 // 32, tiles, 32, LANES).transpose(0, 2, 1, 3).reshape(-1)
    kv2 = rows[layout.kv2:layout.q2].reshape(2 * tiles, ctx_width // 16, LANES).swapaxes(0, 1).reshape(-1)
    return [square(layout.qkv, 3), square(layout.out, 1), square(layout.q2, 1), kv2, square(layout.out2, 1), ff1, ff2]


def solution(mesh):
    n_dev = mesh.shape[AXIS]

    def local(tokens_x, context, cot_out, *shards):
        samples, tokens, width = tokens_x.shape
        ctx_len, ctx_width = context.shape[1:]
        blocks = shards[0].shape[0]
        total = samples * n_dev
        chunk = PAIR_ROWS
        shapes = weight_shapes(width, ctx_width)
        pieces = [[shard[layer].reshape(shape[0] // n_dev, shape[1]) for shard, shape in zip(shards[:7], shapes[:7])]
                  for layer in range(blocks)]
        vecs = lax.all_gather(shards[7].reshape(1, blocks, -1), AXIS, axis=0, tiled=True)
        vecs = jnp.swapaxes(vecs, 0, 1).reshape(blocks, -1).astype(F32)
        pad = -(-ctx_len // 16) * 16
        ctx_rows = jnp.pad(context, ((0, 0), (0, pad - ctx_len), (0, 0))).reshape(samples * pad, ctx_width)
        h = tokens_x.reshape(samples * tokens, width).astype(F32)
        saved = []
        for layer in range(blocks):
            w_qkv, w_out, w_q2, w_kv2, w_out2, w_ff1, w_ff2 = pieces[layer]
            small = gather(jnp.concatenate([w_qkv, w_out, w_q2, w_out2], axis=1))
            w_qkv = small[:, :3 * width]
            w_out, w_q2, w_out2 = (small[:, index * width:(index + 1) * width] for index in range(3, 6))
            w_kv2, w_ff1, w_ff2 = gather(w_kv2), gather(w_ff1), gather(w_ff2)
            rows = jnp.pad(vecs[layer, :9 * width].reshape(9, width), ((0, 7), (0, 0)))
            b1 = vecs[layer, 9 * width:17 * width].reshape(1, 8 * width)
            h1, qkv, out1 = self_forward(h, w_qkv, w_out, rows, tokens)
            h2, q, kv, out2 = cross_forward(h1, ctx_rows, w_q2, w_kv2, w_out2, rows, tokens, ctx_len, samples)
            h3, fa, fg, z = ff_forward(h2, w_ff1, w_ff2, b1, rows, chunk)
            saved.append(dict(zip(NAMES, (h, h1, h2, qkv, out1, q, kv, out2, fa, fg, z, w_qkv, w_out, w_q2, w_out2, w_ff1,
                                          w_ff2, rows))))
            h = h3
        out_tokens = h.astype(BF16).reshape(tokens_x.shape)
        gx, out, layout = backward(cot_out.reshape(samples * tokens, width), ctx_rows, saved, tokens, ctx_len, total)
        results = [ungrad(out, layout, layer, blocks, width, ctx_width) for layer in range(blocks)]
        stacked = [jnp.stack([result[index] for result in results]) for index in range(7)]
        vec = out[layout.vec:layout.vec + blocks * layout.vec_rows].reshape(blocks, -1)[:, :17 * width // n_dev]
        return tuple([out_tokens, gx.reshape(tokens_x.shape)] + stacked + [vec])

    param_spec = P(None, AXIS)
    in_specs = (P(AXIS), P(AXIS), P(AXIS)) + (param_spec,) * 8
    out_specs = (P(AXIS), P(AXIS)) + (param_spec,) * 8
    return jax.shard_map(local, mesh=mesh, in_specs=in_specs, out_specs=out_specs, check_vma=False)
```

```python
import functools
import math
from typing import Any, NamedTuple
import jax
import jax.numpy as jnp
from jax import lax
from jax.experimental import pallas as pl
from jax.experimental.pallas import tpu as pltpu
from jax.sharding import PartitionSpec as P

AXIS = 'fsdp'
HEAD = 64
EPS = 1e-5
SHARDS = 16
CUBE = (2, 2, 2, 2)
WEIGHT = (8, 4, 2, 1)
CHIP_WEIGHT = WEIGHT[1:]
CHIPS = 8
SUB = 8
FULL = slice(None)
SELF_ROWS, CROSS_ROWS = (0, 1, 6), (2, 3, 7)
F32 = jnp.float32
BF16 = jnp.bfloat16
LANES = 128
VMEM_BYTES = 63 * 2 ** 20
BELL = (2 * math.pi) ** -0.5
SLOT = LANES
PAIR_ROWS = 512
FF_COLS = 256

TAIL_P = 0.265
TAIL = (0.10574158579953814, 0.10524628753634038, 0.10270369607548423, 0.0603023517537824, 0.13797880111692826,
        -0.11640058407079061, 0.2178489286936914, -0.1442454807654402, 0.03082441619112092)


def mm(lhs, rhs):
    return jnp.dot(lhs, rhs, preferred_element_type=F32)


def mm_nt(lhs, rhs):
    return lax.dot_general(lhs, rhs, (((1,), (1,)), ((), ())), preferred_element_type=F32)


def mm_tn(lhs, rhs):
    return lax.dot_general(lhs, rhs, (((0,), (0,)), ((), ())), preferred_element_type=F32)


pipeline = functools.partial(pltpu.emit_pipeline, _explicit_indices=True)


def lane_mean(x):
    return jnp.mean(x, axis=-1, keepdims=True)


def lane_sum(x):
    return jnp.sum(x, axis=-1, keepdims=True)


def row_sum(x):
    return jnp.sum(x, axis=0, keepdims=True)


def line(ref, index):
    return ref[index:index + 1]


def add_line(ref, index, values):
    ref[index:index + 1] += values


def span(index, size):
    return pl.ds(pl.multiple_of(index * size, size), size)


def lanes(tile):
    return slice(tile * LANES, (tile + 1) * LANES)


def repeat(count, body):
    def one(index, carry):
        body(index)
        return carry

    lax.fori_loop(0, count, one, 0)


def normalize(x):
    centered = x - lane_mean(x)
    scale = lax.rsqrt(lane_mean(centered * centered) + EPS)
    return centered * scale, scale


def norm_back(x, d_norm, gain):
    hat, scale = normalize(x)
    d_hat = d_norm * gain
    pulled = d_hat - lane_mean(d_hat) - hat * lane_mean(d_hat * hat)
    return pulled * scale, row_sum(d_norm * hat), row_sum(d_norm)


def low_half(rows):
    return lax.broadcasted_iota(jnp.int32, (rows, LANES), 1) < HEAD


def head_stack(pair, low):
    zero = jnp.zeros_like(pair)
    return jnp.concatenate([jnp.where(low, pair, zero), jnp.where(low, zero, pair)], axis=0)


def head_unstack(stacked, low):
    half = stacked.shape[0] // 2
    return jnp.where(low, stacked[:half], stacked[half:])


def softmax_halves(scores, valid):
    half = scores.shape[1] // 2
    parts = []
    for index in range(2):
        part = scores[:, index * half:(index + 1) * half]
        if valid < half:
            part = jnp.where(lax.broadcasted_iota(jnp.int32, part.shape, 1) < valid, part, -jnp.inf)
        part = jnp.exp(part - jnp.max(part, axis=-1, keepdims=True))
        parts.append(part * (1.0 / lane_sum(part)))
    return parts


def pair_forward(query, keys, values, valid):
    low = low_half(keys.shape[0])
    scores = mm_nt(query * BF16(HEAD ** -0.5), head_stack(keys, low))
    probs = jnp.concatenate([part.astype(BF16) for part in softmax_halves(scores, valid)], axis=1)
    return mm(probs, head_stack(values, low)).astype(BF16)


def pair_backward(query, keys, values, d_out, valid):
    low = low_half(keys.shape[0])
    half = keys.shape[0]
    query = query * BF16(HEAD ** -0.5)
    key_stack = head_stack(keys, low)
    value_stack = head_stack(values, low)
    parts = softmax_halves(mm_nt(query, key_stack), valid)
    probs = jnp.concatenate([part.astype(BF16) for part in parts], axis=1)
    d_values = head_unstack(mm_tn(probs, d_out), low).astype(BF16)
    d_probs = mm_nt(d_out, value_stack)
    d_scores = []
    for index in range(2):
        part, d_part = parts[index], d_probs[:, index * half:(index + 1) * half]
        d_scores.append((part * (d_part - lane_sum(part * d_part))).astype(BF16))
    d_scores = jnp.concatenate(d_scores, axis=1)
    d_query = (mm(d_scores, key_stack) * HEAD ** -0.5).astype(BF16)
    d_keys = head_unstack(mm_tn(d_scores, query), low).astype(BF16)
    return d_query, d_keys, d_values


def normal_cdf(u):
    t = 1.0 / (1.0 + TAIL_P * jnp.abs(u))
    poly = TAIL[-1]
    for coef in TAIL[-2::-1]:
        poly = poly * t + coef
    bell = jnp.exp(u * u * -0.5)
    tail = bell * (t * poly)
    return jnp.where(u >= 0, 1.0 - tail, tail), bell


UNIT = 80
COLORS = 3
MACRO = COLORS * UNIT
SLOTS = 3
STREAMS = 2
STAGES = 4
CORE = 3
ORDERS = ((2, 1, 0), (1, 0, 2), (0, 2, 1))
MESH = pl.DeviceIdType.MESH


def bits_of(device):
    return [lax.rem(lax.div(device, weight), 2) for weight in WEIGHT]


class Place:
    def __init__(self):
        me = lax.axis_index(AXIS)
        self.bits = bits_of(me)
        self.others = [1 - bit for bit in self.bits]
        self.devices = [(me + (other - bit) * weight,) for bit, other, weight in zip(self.bits, self.others, WEIGHT)]

    def rows_of(self, ref, first, rows):
        half = ref.shape[CORE] // 2
        return pl.ds(pl.multiple_of(self.bits[CORE] * half + first, SUB), rows)

    def own(self, ref):
        return ref.at[(*self.bits[:CORE], self.rows_of(ref, 0, ref.shape[CORE] // 2))]

    def entry_barrier(self):
        barrier = pltpu.get_barrier_semaphore()
        for device in self.devices:
            pl.semaphore_signal(barrier, inc=1, device_id=device, device_id_type=MESH)
        pl.semaphore_wait(barrier, 4)


def pick(ref, lead, dim, value):
    return ref.at[(lead,) + (FULL,) * dim + (value,)]


class At(NamedTuple):
    stream: Any
    index: Any
    row: Any


class Reducer:
    def __init__(self, place, macros, scale, grads, out, refs):
        self.place, self.macros, self.scale, self.grads, self.out = place, macros, scale, grads, out
        self.own, self.held = refs[0], refs[1:1 + STAGES]
        self.send, self.recv, self.load = refs[1 + STAGES:]

    @staticmethod
    def scratch():
        held = [pltpu.VMEM((STREAMS * SLOTS * COLORS,) + (2,) * (3 - stage) + (UNIT, LANES), F32) for stage in range(STAGES)]
        sems = [pltpu.SemaphoreType.DMA((STREAMS, COLORS, STAGES)), pltpu.SemaphoreType.DMA((STREAMS * SLOTS * COLORS, STAGES)),
                pltpu.SemaphoreType.DMA((STREAMS, COLORS))]
        return [pltpu.VMEM((STREAMS * COLORS, *CUBE[1:], UNIT, LANES), F32)] + held + sems

    def axis(self, color, stage):
        return CORE if stage == 0 else ORDERS[color][stage - 1]

    def dim(self, color, stage):
        gone = ORDERS[color][:stage - 1]
        return sum(1 for axis in range(ORDERS[color][stage - 1]) if axis not in gone)

    def copy(self, at, color, stage):
        axis = self.axis(color, stage)
        other = self.place.others[axis]
        index = at.index + color
        if stage == 0:
            source = self.grads.at[:, :, :, other, pl.ds(at.row + color * UNIT, UNIT)]
        else:
            source = pick(self.held[stage - 1], index, self.dim(color, stage), other)
        return pltpu.make_async_remote_copy(
            src_ref=source, dst_ref=self.held[stage].at[index], send_sem=self.send.at[at.stream, color, stage],
            recv_sem=self.recv.at[index, stage], device_id=self.place.devices[axis], device_id_type=MESH)

    def own_copy(self, at, color):
        return pltpu.make_async_copy(self.grads.at[:, :, :, self.place.bits[CORE], pl.ds(at.row + color * UNIT, UNIT)],
                                     self.own.at[at.stream * COLORS + color], self.load.at[at.stream, color])

    def add(self, at, color, stage):
        index = at.index + color
        if stage == 0:
            self.held[0][index] += self.own[at.stream * COLORS + color]
            return
        mine = self.held[stage - 1][(index,) + (FULL,) * self.dim(color, stage)
                                    + (self.place.bits[self.axis(color, stage)],)]
        if stage < STAGES - 1:
            self.held[stage][index] += mine
        else:
            self.out[pl.ds(at.row + color * UNIT, UNIT)] = (self.held[stage][index] + mine) * self.scale

    def step(self, t):
        stream, tau = lax.rem(t, STREAMS), lax.div(t, STREAMS)

        def when_live(local, body):
            @pl.when((local >= 0) & (local * STREAMS + stream < self.macros))
            def _():
                body(At(stream, (stream * SLOTS + lax.rem(local, SLOTS)) * COLORS,
                        pl.multiple_of((local * STREAMS + stream) * MACRO, SUB)))

        def take(stage, at):
            for color in range(COLORS):
                copy = self.copy(at, color, stage)
                copy.wait_send()
                copy.wait_recv()
                if stage == 0:
                    self.own_copy(at, color).wait()
            for color in range(COLORS):
                self.add(at, color, stage)

        def give(stage, at):
            for color in range(COLORS):
                self.copy(at, color, stage).start()
                if stage == 0:
                    self.own_copy(at, color).start()

        for stage in reversed(range(STAGES)):
            when_live(tau - 1 - stage, functools.partial(take, stage))
        for stage in range(STAGES):
            when_live(tau - stage, functools.partial(give, stage))


class Piece(NamedTuple):
    ref: Any
    first: Any
    rows: Any
    cols: Any
    color: int
    number: int


class Gatherer:
    def __init__(self, place, macros, send, recv):
        self.place, self.macros, self.send, self.recv = place, [], send, recv
        number = 0
        for macro in macros:
            pieces = []
            for ref, color, first, rows, cols in macro:
                pieces.append(Piece(ref, first, rows, cols, color, number))
                number += 1
            self.macros.append(pieces)

    def copy(self, piece, stage):
        order = ORDERS[piece.color]
        index = [FULL if axis in order[:stage] else self.place.bits[axis] for axis in range(CORE)]
        block = piece.ref.at[(*index, self.place.rows_of(piece.ref, piece.first, piece.rows), piece.cols)]
        axis = order[stage] if stage < CORE else CORE
        return pltpu.make_async_remote_copy(
            src_ref=block, dst_ref=block, send_sem=self.send.at[piece.number, stage],
            recv_sem=self.recv.at[piece.number, stage], device_id=self.place.devices[axis], device_id_type=MESH)

    def step(self, t):
        for macro, pieces in enumerate(self.macros):
            stage = t - macro
            if stage in range(1, STAGES + 1):
                for piece in pieces:
                    copy = self.copy(piece, stage - 1)
                    copy.wait_send()
                    copy.wait_recv()
            if stage in range(STAGES):
                for piece in pieces:
                    self.copy(piece, stage).start()

    def beside(self, index, plan):
        first, count = plan
        for number in range(count):
            @pl.when(index == 2 * number + 1)
            def _(number=number):
                self.step(first + number)


def thirds(tiles):
    edges = [round(tiles * part / 3) * LANES for part in range(4)]
    return [slice(first, last) for first, last in zip(edges[:-1], edges[1:])]


FORWARD_PLAN = [(5, 3), (8, 3), (11, 5), (SHARDS, 2), (0, 0), (0, 0)]
MATS = ('qkv', 'out', 'q2', 'kv2', 'out2', 'ff1', 'ff2')
WEIGHTS = ('w_a', 'w_b', 'w_kv2', 'w_ff1', 'w_ff2')
KEPT = ('h', 'h1', 'h2', 'qkv', 'out1', 'q', 'kv', 'out2', 'fa', 'fg', 'z', 'rows')


def load(source, target, sem):
    copy = pltpu.make_async_copy(source, target, sem)
    copy.start()
    return copy


def fetch(source, cols, target, sems):
    def copy(shard):
        index = [lax.rem(lax.div(shard, weight), 2) for weight in CHIP_WEIGHT]
        return pltpu.make_async_copy(source.at[(*index, FULL, cols)], target.at[span(shard, source.shape[CORE])],
                                     sems.at[shard])

    repeat(CHIPS, lambda shard: copy(shard).start())
    return lambda: repeat(CHIPS, lambda shard: copy(shard).wait())


def macro_list(weights, vec):
    macros = []
    for block in weights:
        high = {name: block[name].shape[CORE] // 2 for name in WEIGHTS}
        cols = {name: thirds(block[name].shape[-1] // LANES) for name in ('w_a', 'w_b', 'w_kv2')}
        wide = block['w_ff1'].shape[-1] // 2

        def add(name, first, rows, cols):
            macros.append([(block[name], color, first, rows, part) for color, part in enumerate(cols)])

        add('w_a', 0, high['w_a'], cols['w_a'])
        for part in range(2):
            add('w_kv2', part * high['w_kv2'] // 2, high['w_kv2'] // 2, cols['w_kv2'])
        add('w_b', 0, high['w_b'], cols['w_b'])
        for part in range(2):
            add('w_ff1', 0, high['w_ff1'],
                [pl.ds(part * wide + third.start, third.stop - third.start) for third in thirds(wide // LANES)])
        tenth = high['w_ff2'] // 10
        macros.append([(block['w_ff2'], color, first * tenth, rows * tenth, FULL)
                       for color, (first, rows) in enumerate(((0, 3), (3, 4), (7, 3)))])
    macros[0].append((vec, 0, 0, vec.shape[CORE] // 2, FULL))
    return macros


def forward_kernel(cfg, *refs):
    tokens, width, blocks, per_vec = cfg
    heads = width // HEAD
    tiles = width // LANES
    tokens_ref, context_ref = refs[:2]
    raw_refs = refs[2:2 + len(MATS) + 1]
    refs = refs[2 + len(raw_refs):]
    kept = [dict(zip(KEPT, refs[layer * len(KEPT):])) for layer in range(blocks)]
    refs = refs[blocks * len(KEPT):]
    weights = [dict(zip(WEIGHTS, refs[layer * len(WEIGHTS):])) for layer in range(blocks)]
    refs = refs[blocks * len(WEIGHTS):]
    vec_all_ref, ctx_out_ref, tokens_out_ref, hidden, context, rows_ref, vec_ref, sems, send, recv = refs
    samples, ctx_len = context_ref.shape[:2]
    pad = context.shape[0] // samples
    count = tokens_ref.shape[0]
    chunk = PAIR_ROWS
    per_step = chunk // tokens
    place = Place()
    gatherer = Gatherer(place, macro_list(weights, vec_all_ref), send, recv)

    def each_chunk(body):
        repeat(count // chunk, lambda index: body(span(index, chunk)))

    def startup(image, wide, flat, vec_piece, raws, pieces, raw_sems, own_sems):
        first = [load(tokens_ref, image, sems.at[0]), load(context_ref, wide, sems.at[1])]
        loads = [load(source, target, raw_sems.at[index])
                 for index, (source, target) in enumerate(zip(raw_refs, raws))]

        def tile(layer, name, target, first_col):
            raw = raws[MATS.index(name)]
            total = raw.shape[0]
            flat[:total] = raw[:, layer].astype(F32)
            rows = target.shape[0]
            many = total // rows
            for index in range(many):
                at = first_col + index * LANES
                target[:, at:at + LANES] = flat[pl.ds(index, rows, stride=many)].astype(BF16)

        def own(layer, name):
            number = layer * len(WEIGHTS) + WEIGHTS.index(name)
            return load(pieces[number], place.own(weights[layer][name]), own_sems.at[number])

        def prepare(layer, name):
            target = pieces[layer * len(WEIGHTS) + WEIGHTS.index(name)]
            if name == 'w_a':
                tile(layer, 'qkv', target, 0)
                tile(layer, 'out', target, 3 * width)
            elif name == 'w_b':
                tile(layer, 'q2', target, 0)
                tile(layer, 'out2', target, width)
            else:
                tile(layer, name[2:], target, 0)
            return own(layer, name)

        for copy in loads:
            copy.wait()
        vec_piece[:] = jnp.zeros_like(vec_piece)
        for layer in range(blocks):
            flat[:per_vec] = raws[-1][:, layer].astype(F32)
            vec_piece[layer * SUB:layer * SUB + per_vec] = flat[:per_vec].astype(BF16)
        pending = [prepare(0, 'w_a'), load(vec_piece, place.own(vec_all_ref), sems.at[2])]
        place.entry_barrier()
        later = [[(0, 'w_kv2')], [(0, 'w_b'), (0, 'w_ff1'), (0, 'w_ff2')], [(1, 'w_a'), (1, 'w_kv2'), (1, 'w_b')],
                 [(1, 'w_ff1'), (1, 'w_ff2')]]
        for t, jobs in enumerate(later):
            for copy in pending:
                copy.wait()
            gatherer.step(t)
            pending = [prepare(layer, name) for layer, name in jobs if layer < blocks]
        for copy in first:
            copy.wait()
        each_chunk(lambda at: hidden.at[0].__setitem__(at, image[at].astype(F32)))
        context[:] = jnp.zeros_like(context)
        for sample in range(samples):
            context[sample * pad:sample * pad + ctx_len] = wide[sample]
        for copy in pending:
            copy.wait()
        gatherer.step(len(later))

    def raw_shape(index):
        return pltpu.VMEM(raw_refs[index].shape, BF16)

    pl.run_scoped(startup, pltpu.VMEM(tokens_ref.shape, BF16), pltpu.VMEM(context_ref.shape, BF16),
                  pltpu.VMEM((max(ref.shape[0] for ref in raw_refs), LANES), F32), pltpu.VMEM((blocks * SUB, LANES), BF16),
                  [raw_shape(index) for index in range(len(raw_refs))],
                  [pltpu.VMEM((block[name].shape[CORE] // 2, block[name].shape[-1]), BF16)
                   for block in weights for name in WEIGHTS],
                  pltpu.SemaphoreType.DMA((len(raw_refs),)), pltpu.SemaphoreType.DMA((blocks * len(WEIGHTS),)))
    ctx_copy = load(context, ctx_out_ref, sems.at[3])

    def unpack(parts, sem):
        load(vec_all_ref, parts, sem).wait()
        vec_ref[:] = jnp.zeros_like(vec_ref)
        rows_ref[:] = jnp.zeros_like(rows_ref)
        lane = lax.broadcasted_iota(jnp.int32, (SUB, LANES), 1)
        per_device = 17 * width // SHARDS
        for layer in range(blocks):
            vec = vec_ref.at[layer]
            for shard in range(SHARDS):
                chip, core = divmod(shard, 2)
                bits = [chip // weight % 2 for weight in CHIP_WEIGHT]
                part = parts[(*bits, pl.ds((core * blocks + layer) * SUB, SUB))].astype(F32)
                row, off = divmod(shard * per_device, LANES)
                if off:
                    part = pltpu.roll(part, off, 1)
                    vec[pl.ds(row + 1, SUB)] += jnp.where(lane < off, part, 0.0)
                vec[pl.ds(row, SUB)] += jnp.where(lane >= off, part, 0.0)
            for row in range(9):
                for tile in range(tiles):
                    rows_ref[layer, row:row + 1, lanes(tile)] = line(vec, row * tiles + tile)

    pl.run_scoped(unpack, pltpu.VMEM(vec_all_ref.shape, BF16), pltpu.SemaphoreType.DMA)
    rows_copies = [load(rows_ref.at[layer], kept[layer]['rows'], sems.at[4 + layer]) for layer in range(blocks)]

    def attention(layer, source, target, cross, plan):
        rows = rows_ref.at[layer]
        packed = weights[layer]['w_b' if cross else 'w_a']
        inner = packed.shape[-1] - width
        gain, shift, bias = CROSS_ROWS if cross else SELF_ROWS

        def scoped(w_in, w_out, w_kv, kv, in_sems):
            waits = [fetch(packed, pl.ds(0, inner), w_in, in_sems.at[0]), fetch(packed, pl.ds(inner, width), w_out, in_sems.at[1])]
            if cross:
                fetch(weights[layer]['w_kv2'], FULL, w_kv, in_sems.at[2])()
                fresh = mm(context[:], w_kv[:]).astype(BF16)
                for index in range(samples):
                    kv[index * SLOT:index * SLOT + pad] = fresh[index * pad:(index + 1) * pad]
                    kv[index * SLOT + pad:(index + 1) * SLOT] = jnp.zeros((SLOT - pad, 2 * width), BF16)
                kv_copy = load(kv, kept[layer]['kv'], in_sems.at[2, 0])
            for wait in waits:
                wait()

            def body(idx, qkv, mixed):
                step = idx.index[0]
                at_rows = span(step, chunk)
                hat, unused = normalize(source[at_rows])
                norm = (hat * line(rows, gain) + line(rows, shift)).astype(BF16)
                qkv[:] = mm(norm, w_in[:]).astype(BF16)

                def sample(number):
                    at = span(number, tokens)
                    index = step * per_step + number
                    for pair in range(heads // 2):
                        cols, k_cols, v_cols = (slice(part * width + pair * LANES, part * width + (pair + 1) * LANES)
                                                for part in range(COLORS))
                        if cross:
                            kv_at = span(index, SLOT)
                            mixed[at, cols] = pair_forward(qkv[at, cols], kv[kv_at, cols], kv[kv_at, k_cols], ctx_len)
                        else:
                            mixed[at, cols] = pair_forward(qkv[at, cols], qkv[at, k_cols], qkv[at, v_cols], tokens)
                    gatherer.beside(index, plan)

                repeat(per_step, sample)
                target[at_rows] = source[at_rows] + mm(mixed[:], w_out[:]) + line(rows, bias)

            block = lambda cols: pl.BlockSpec((chunk, cols), lambda step: (step, 0))
            pipeline(body, grid=(count // chunk,), out_specs=[block(inner), block(width)])(
                kept[layer]['q' if cross else 'qkv'], kept[layer]['out2' if cross else 'out1'])
            if cross:
                kv_copy.wait()

        small = pltpu.VMEM((SUB, LANES), BF16)
        pl.run_scoped(scoped, pltpu.VMEM((width, inner), BF16), pltpu.VMEM((width, width), BF16),
                      pltpu.VMEM((context_ref.shape[2], 2 * width), BF16) if cross else small,
                      pltpu.VMEM((samples * SLOT, 2 * width), BF16) if cross else small, pltpu.SemaphoreType.DMA((3, CHIPS)))

    def feed_forward(layer, source, target, plan):
        rows = rows_ref.at[layer]
        vec = vec_ref.at[layer]
        inner = weights[layer]['w_ff1'].shape[-1] // 2
        steps = inner // FF_COLS
        part = FF_COLS // LANES

        def scoped(norm, w1, w2, w_sems):
            waits = [fetch(weights[layer]['w_ff1'], FULL, w1, w_sems.at[0]), fetch(weights[layer]['w_ff2'], FULL, w2, w_sems.at[1])]

            def begin(at):
                hat, unused = normalize(source[at])
                norm[at] = (hat * line(rows, 4) + line(rows, 5)).astype(BF16)
                target[at] = source[at] + line(rows, SUB)

            each_chunk(begin)
            for wait in waits:
                wait()

            def body(idx, fa, fg, z):
                step = idx.index[0]
                cols, gate_cols = span(step, FF_COLS), span(step + steps, FF_COLS)

                def bias(half):
                    first = 9 * tiles + (half * steps + step) * part
                    return jnp.concatenate([vec[pl.ds(first + index, 1)] for index in range(part)], axis=1)

                bias_a, bias_g = bias(0), bias(1)

                def one(at):
                    gate = mm(norm[at], w1[:, gate_cols]) + bias_g
                    cdf, bell = normal_cdf(gate)
                    factor = gate * cdf
                    value = mm(norm[at], w1[:, cols]) + bias_a
                    z[at] = (value * factor).astype(BF16)
                    fa[at] = factor
                    fg[at] = value * (cdf + gate * bell * BELL)
                    target[at] += mm(z[at], w2[cols])

                each_chunk(one)
                gatherer.beside(step, plan)

            block = ff_block(count)
            pipeline(body, grid=(steps,), out_specs=[block, block, block])(
                kept[layer]['fa'], kept[layer]['fg'], kept[layer]['z'])

        pl.run_scoped(scoped, pltpu.VMEM((count, width), BF16), pltpu.VMEM((width, 2 * inner), BF16),
                      pltpu.VMEM((inner, width), BF16), pltpu.SemaphoreType.DMA((2, CHIPS)))

    phases = len(FORWARD_PLAN)
    saves = [load(hidden.at[0], kept[0]['h'], sems.at[6]), None]
    for phase in range(phases):
        layer, kind = divmod(phase, 3)
        source, target = hidden.at[phase % 2], hidden.at[(phase + 1) % 2]
        other = (phase + 1) % 2
        if saves[other] is not None:
            saves[other].wait()
        if kind < 2:
            attention(layer, source, target, kind == 1, FORWARD_PLAN[phase])
        else:
            feed_forward(layer, source, target, FORWARD_PLAN[phase])
        following = divmod(phase + 1, 3)
        saves[other] = None
        if phase + 1 < phases:
            saves[other] = load(target, kept[following[0]][KEPT[following[1]]], sems.at[6 + other])

    def finish(image):
        each_chunk(lambda at: image.__setitem__(at, hidden[phases % 2, at].astype(BF16)))
        load(image, tokens_out_ref, sems.at[0]).wait()

    pl.run_scoped(finish, pltpu.VMEM(tokens_ref.shape, BF16))
    for copy in [copy for copy in saves if copy is not None] + [ctx_copy] + rows_copies:
        copy.wait()


def settings(number):
    return dict(compiler_params=pltpu.CompilerParams(collective_id=number, has_side_effects=True,
                                                     vmem_limit_bytes=VMEM_BYTES),
                cost_estimate=pl.CostEstimate(flops=10 ** 11, bytes_accessed=10 ** 8, transcendentals=0))


def ff_block(count):
    return pl.BlockSpec((None, count, FF_COLS), lambda step: (step, 0, 0))


def any_specs(count):
    return [pl.BlockSpec(memory_space=pl.ANY)] * count


def forward(tokens_x, context, raws):
    samples, tokens, width = tokens_x.shape
    ctx_width = context.shape[2]
    blocks = raws[0].shape[1]
    count, inner = samples * tokens, 4 * width
    pad = -(-context.shape[1] // SHARDS) * SHARDS
    steps = inner // FF_COLS
    plain = jax.ShapeDtypeStruct((count, width), F32)
    half = jax.ShapeDtypeStruct((count, width), BF16)
    wide = jax.ShapeDtypeStruct((steps, count, FF_COLS), F32)
    kept = [plain, plain, plain, jax.ShapeDtypeStruct((count, 3 * width), BF16), half, half,
            jax.ShapeDtypeStruct((samples * SLOT, 2 * width), BF16), half, wide, wide,
            jax.ShapeDtypeStruct(wide.shape, BF16), jax.ShapeDtypeStruct((SHARDS, width), F32)]
    whole_of = lambda rows, cols: jax.ShapeDtypeStruct((*CUBE[:CORE], rows // CHIPS, cols), BF16)
    weights = [whole_of(width, 4 * width), whole_of(width, 2 * width), whole_of(ctx_width, 2 * width),
               whole_of(width, 2 * inner), whole_of(inner, width)]
    extra = [whole_of(SHARDS * blocks * SUB, LANES), jax.ShapeDtypeStruct((samples * pad, ctx_width), BF16), half]
    shapes = kept * blocks + weights * blocks + extra
    pieces = 1 + 3 * 7 * blocks
    outs = pl.pallas_call(
        functools.partial(forward_kernel, (tokens, width, blocks, raws[-1].shape[0])),
        in_specs=any_specs(2 + len(raws)), out_specs=any_specs(len(shapes)), out_shape=shapes,
        scratch_shapes=[pltpu.VMEM((2, count, width), F32), pltpu.VMEM((samples * pad, ctx_width), BF16),
                        pltpu.VMEM((blocks, SHARDS, width), F32), pltpu.VMEM((blocks, 96, LANES), F32),
                        pltpu.SemaphoreType.DMA((8,)), pltpu.SemaphoreType.DMA((pieces, STAGES)),
                        pltpu.SemaphoreType.DMA((pieces, STAGES))],
        name='forward', **settings(1),
    )(tokens_x.reshape(count, width), context, *raws)
    kept_of = [outs[layer * len(kept):(layer + 1) * len(kept)] for layer in range(blocks)]
    outs = outs[blocks * len(kept):]
    weights_of = [[whole.reshape(-1, whole.shape[-1]) for whole in outs[layer * len(weights):(layer + 1) * len(weights)]]
                  for layer in range(blocks)]
    saved = [dict(zip(KEPT + WEIGHTS, list(one) + list(two))) for one, two in zip(kept_of, weights_of)]
    return saved, outs[-2], outs[-1]


def view(values, *lead):
    return values.reshape(CUBE + lead + (LANES,))


def put_tiles(stage, values, first=0):
    rows = values.shape[0] // SHARDS
    for tile in range(values.shape[1] // LANES):
        at = first + tile * rows
        stage[:, :, :, :, at:at + rows] = view(values[:, lanes(tile)], rows)


class Layout:
    def __init__(self, width, ctx_width, blocks):
        unit = width // SHARDS * (width // LANES)
        self.ff1, self.ff2 = 0, 8 * unit
        self.kv2 = 12 * unit
        self.q2 = self.kv2 + ctx_width // SHARDS * (2 * width // LANES)
        self.out2 = self.q2 + unit
        self.qkv = self.out2 + unit
        self.out = self.qkv + 3 * unit
        self.block = self.out + unit
        self.vec = blocks * self.block
        self.vec_rows = -(-17 * width // SHARDS // LANES // SUB) * SUB
        used = self.vec + blocks * self.vec_rows
        self.macros = -(-used // MACRO)
        self.pad = self.macros * MACRO - used
        self.rows = self.macros * MACRO


NAMES = KEPT + WEIGHTS


def backward_kernel(cfg, *refs):
    tokens, ctx_len, width, blocks, layout, total, plan = cfg
    heads = width // HEAD
    cot_ref, context_ref = refs[:2]
    saved = [dict(zip(NAMES, refs[2 + layer * len(NAMES):])) for layer in range(blocks)]
    refs = refs[2 + blocks * len(NAMES):]
    gx_ref, grads_ref = refs[:2]
    out_refs, refs = refs[2:3 + len(MATS)], refs[3 + len(MATS):]
    grad_ref, hidden_ref, rows_ref, d_rows_ref, vec_ref, out_ref, in_sems = refs[:7]
    place = Place()
    reducer = Reducer(place, layout.macros, 1.0 / total, grads_ref, out_ref, refs[7:])
    count = grad_ref.shape[0]
    chunk = PAIR_ROWS
    chunks = count // chunk
    phases = [(layer, kind) for layer in reversed(range(blocks)) for kind in ('h2', 'h1', 'h')]

    def hidden_copy(index):
        layer, kind = phases[index]
        return pltpu.make_async_copy(saved[layer][kind], hidden_ref.at[index % 2], in_sems.at[index % 2])

    def rows_copy(layer):
        return pltpu.make_async_copy(saved[layer]['rows'], rows_ref.at[layer], in_sems.at[2 + layer])

    def base(layer):
        return (blocks - 1 - layer) * layout.block

    def region(row, size):
        return grads_ref.at[:, :, :, :, pl.ds(pl.multiple_of(row, SUB), size)]

    def each_chunk(body):
        def one(index, carry):
            body(span(index, chunk))
            return carry
        lax.fori_loop(0, chunks, one, 0)

    def ff_phase(layer, index, first):
        hidden = hidden_ref.at[index % 2]
        rows = rows_ref.at[layer]
        d_rows = d_rows_ref.at[layer]
        vec = vec_ref.at[layer]
        src = saved[layer]
        w1_all, w2_all = src['w_ff1'], src['w_ff2']
        inner = w2_all.shape[0]
        steps = inner // FF_COLS
        start, lag, limit = first

        def scoped(norm_t, grad_bf, du, w1, acc, stage1, stage2, sem1, sem2):
            def begin(at):
                hat, unused = normalize(hidden[at])
                norm_t[:, at] = (hat * line(rows, 4) + line(rows, 5)).astype(BF16).T
                grad_bf[at] = grad_ref[at].astype(BF16)
                add_line(d_rows, 8, row_sum(grad_ref[at]))
                acc[at] = jnp.zeros((chunk, width), F32)

            each_chunk(begin)

            def copy1(step):
                return pltpu.make_async_copy(stage1, region(base(layer) + layout.ff1 + step * 160, 160), sem1)

            def copy2(step, part):
                block = step * 8 + part
                shard = lax.div(block, 5)
                row = pl.multiple_of(base(layer) + layout.ff2 + lax.rem(block, 5) * 160, SUB)
                bits = bits_of(shard)
                return pltpu.make_async_copy(stage2.at[part], grads_ref.at[(*bits, pl.ds(row, 160))], sem2.at[part])

            def wait(step):
                copy1(step).wait()
                for part in range(8):
                    copy2(step, part).wait()

            def body(idx, w1a, w1g, w2, fa, fg, z):
                step = idx.index[0]
                w1[:, :FF_COLS] = w1a[:]
                w1[:, FF_COLS:] = w1g[:]

                def part(number, sums):
                    at = span(number, chunk)
                    dz = mm_nt(grad_bf[at], w2[:]).astype(BF16).astype(F32)
                    du_a = dz * fa[at]
                    du_g = dz * fg[at]
                    du[at, :FF_COLS] = du_a.astype(BF16)
                    du[at, FF_COLS:] = du_g.astype(BF16)
                    acc[at] += mm_nt(du[at], w1[:])
                    return (sums[0] + row_sum(du_a), sums[1] + row_sum(du_g))

                zero = jnp.zeros((1, FF_COLS), F32)
                sums = lax.fori_loop(0, chunks, part, (zero, zero))
                for half in range(2):
                    for tile in range(2):
                        row = 9 * width // LANES + half * (inner // LANES) + 2 * step + tile
                        vec[pl.ds(row, 1)] = sums[half][:, lanes(tile)]

                @pl.when(step > 0)
                def _():
                    wait(step - 1)

                if limit > 0:
                    @pl.when((step >= lag) & (step < lag + limit))
                    def _():
                        reducer.step(start + step - lag)

                put_tiles(stage1, mm(norm_t[:], du[:, :FF_COLS]))
                put_tiles(stage1, mm(norm_t[:], du[:, FF_COLS:]), 80)
                d_w2 = mm_tn(z[:], grad_bf[:])
                for tile in range(width // LANES):
                    stage2[:, tile * 32:(tile + 1) * 32] = d_w2[:, lanes(tile)].reshape(8, 32, LANES)
                copy1(step).start()
                for number in range(8):
                    copy2(step, number).start()

            column = pl.BlockSpec((width, FF_COLS), lambda step: (0, step))
            kept = ff_block(count)
            pipeline(
                body, grid=(steps,),
                in_specs=[column, pl.BlockSpec((width, FF_COLS), lambda step: (0, step + steps)),
                          pl.BlockSpec((FF_COLS, width), lambda step: (step, 0)), kept, kept, kept],
            )(w1_all, w1_all, w2_all, src['fa'], src['fg'], src['z'])

            def finish(at):
                d_res, d_gain, d_shift = norm_back(hidden[at], acc[at], line(rows, 4))
                grad_ref[at] += d_res
                add_line(d_rows, 4, d_gain)
                add_line(d_rows, 5, d_shift)

            each_chunk(finish)
            wait(steps - 1)

        pl.run_scoped(scoped, pltpu.VMEM((width, count), BF16), pltpu.VMEM((count, width), BF16),
                      pltpu.VMEM((count, 2 * FF_COLS), BF16), pltpu.VMEM((width, 2 * FF_COLS), BF16),
                      pltpu.VMEM((count, width), F32), pltpu.VMEM((*CUBE, 160, LANES), F32),
                      pltpu.VMEM((8, 160, LANES), F32), pltpu.SemaphoreType.DMA, pltpu.SemaphoreType.DMA((8,)))

    def attention_phase(layer, index, first, cross):
        hidden = hidden_ref.at[index % 2]
        rows = rows_ref.at[layer]
        d_rows = d_rows_ref.at[layer]
        src = saved[layer]
        packed = src['w_b' if cross else 'w_a']
        inner = packed.shape[1] - width
        steps = count // PAIR_ROWS
        per_step = PAIR_ROWS // tokens
        start, in_samples, in_tails = first
        gain, shift, bias = CROSS_ROWS if cross else SELF_ROWS
        samples = count // tokens
        pad = context_ref.shape[0] // samples
        kv_rows_all = context_ref.shape[0] if cross else count

        def scoped(d_mix, d_q, d_kv, norm_t, d_wq, d_wout, stage, stage_out, sem, sem_out, w_in, w_out, in_sems_, context, kv, ctx_sems):
            if cross:
                loads = [pltpu.make_async_copy(context_ref, context, ctx_sems.at[0]),
                         pltpu.make_async_copy(src['kv'], kv, ctx_sems.at[1])]
                for copy in loads:
                    copy.start()
                d_wq[:] = jnp.zeros_like(d_wq)
                for copy in loads:
                    copy.wait()
            d_wout[:] = jnp.zeros_like(d_wout)
            for copy in [load(packed.at[:, pl.ds(0, inner)], w_in, in_sems_.at[0]),
                         load(packed.at[:, pl.ds(inner, width)], w_out, in_sems_.at[1])]:
                copy.wait()

            def body(idx, qkv, mixed):
                step = idx.index[0]
                at_rows = span(step, PAIR_ROWS)
                grad_bf = grad_ref[at_rows].astype(BF16)
                add_line(d_rows, bias, row_sum(grad_ref[at_rows]))
                d_wout[:] += mm_tn(mixed[:], grad_bf)
                d_mix[:] = mm_nt(grad_bf, w_out[:]).astype(BF16)

                def sample(number, carry):
                    at = span(number, tokens)
                    sample_index = step * per_step + number
                    if cross:
                        kv_at = span(sample_index, SLOT)
                        d_kv_at = span(sample_index, pad)
                        d_q_at = at
                    else:
                        d_q_at = span(sample_index, tokens)
                    for pair in range(heads // 2):
                        cols = lanes(pair)
                        k_cols = slice(width + pair * LANES, width + (pair + 1) * LANES)
                        v_cols = slice(2 * width + pair * LANES, 2 * width + (pair + 1) * LANES)
                        if cross:
                            d_query, d_keys, d_values = pair_backward(qkv[at, cols], kv[kv_at, cols], kv[kv_at, k_cols],
                                                                      d_mix[at, cols], ctx_len)
                            d_kv[d_kv_at, cols] = d_keys[:pad]
                            d_kv[d_kv_at, k_cols] = d_values[:pad]
                        else:
                            d_query, d_keys, d_values = pair_backward(qkv[at, cols], qkv[at, k_cols], qkv[at, v_cols],
                                                                      d_mix[at, cols], tokens)
                            d_q[d_q_at, k_cols] = d_keys
                            d_q[d_q_at, v_cols] = d_values
                        d_q[d_q_at, cols] = d_query
                    @pl.when(sample_index < in_samples)
                    def _():
                        reducer.step(start + sample_index)

                    return carry

                lax.fori_loop(0, per_step, sample, 0)
                hat, unused = normalize(hidden[at_rows])
                norm = (hat * line(rows, gain) + line(rows, shift)).astype(BF16)
                if cross:
                    d_wq[:] += mm_tn(norm, d_q[:])
                    d_norm = mm_nt(d_q[:], w_in[:])
                else:
                    norm_t[:, at_rows] = norm.T
                    d_norm = mm_nt(d_q[at_rows], w_in[:])
                d_res, d_gain, d_shift = norm_back(hidden[at_rows], d_norm, line(rows, gain))
                grad_ref[at_rows] += d_res
                add_line(d_rows, gain, d_gain)
                add_line(d_rows, shift, d_shift)

            block = lambda ref: pl.BlockSpec((PAIR_ROWS, ref.shape[1]), lambda step: (step, 0))
            operands = [src['q' if cross else 'qkv'], src['out2' if cross else 'out1']]
            pipeline(
                body, grid=(steps,), in_specs=[block(operands[0]), block(operands[1])],
            )(*operands)
            where = base(layer) + (layout.out2 if cross else layout.out)
            size = width // SHARDS * (width // LANES)
            if cross:
                put_tiles(stage_out, d_wq[:])
                put_tiles(stage_out, d_wout[:], size)
                copy_out = pltpu.make_async_copy(stage_out, region(base(layer) + layout.q2, 2 * size), sem_out)
            else:
                put_tiles(stage_out, d_wout[:])
                copy_out = pltpu.make_async_copy(stage_out, region(where, size), sem_out)
            copy_out.start()
            rows_each = stage.shape[4]
            cols_each = stage.shape[4] // ((context_ref.shape[1] if cross else width) // SHARDS) * LANES
            tails = (2 if cross else 3) * width // cols_each
            first_row = base(layer) + (layout.kv2 if cross else layout.qkv)

            def copy_tail(step):
                return pltpu.make_async_copy(stage, region(first_row + step * rows_each, rows_each), sem)

            def tail(step, carry):
                cols = span(step, cols_each)
                result = mm_tn(context[:], d_kv[:, cols]) if cross else mm(norm_t[:], d_q[:, cols])

                @pl.when(step > 0)
                def _():
                    copy_tail(step - 1).wait()

                put_tiles(stage, result)
                copy_tail(step).start()
                if in_tails:
                    @pl.when(step < in_tails)
                    def _():
                        reducer.step(start + in_samples + step)

                return carry

            lax.fori_loop(0, tails, tail, 0)
            copy_tail(tails - 1).wait()
            copy_out.wait()

        small = pltpu.VMEM((SUB, LANES), BF16)
        w_scratch = [pltpu.VMEM((width, inner), BF16), pltpu.VMEM((width, width), BF16), pltpu.SemaphoreType.DMA((2,))]
        size = width // SHARDS * (width // LANES)
        if cross:
            ctx_width = context_ref.shape[1]
            pl.run_scoped(scoped, pltpu.VMEM((PAIR_ROWS, width), BF16), pltpu.VMEM((PAIR_ROWS, width), BF16),
                          pltpu.VMEM((kv_rows_all, 2 * width), BF16), small, pltpu.VMEM((width, width), F32),
                          pltpu.VMEM((width, width), F32), pltpu.VMEM((*CUBE, ctx_width // SHARDS * 2, LANES), F32),
                          pltpu.VMEM((*CUBE, 2 * size, LANES), F32), pltpu.SemaphoreType.DMA,
                          pltpu.SemaphoreType.DMA, *w_scratch, pltpu.VMEM(context_ref.shape, BF16),
                          pltpu.VMEM(src['kv'].shape, BF16), pltpu.SemaphoreType.DMA((2,)))
        else:
            pl.run_scoped(scoped, pltpu.VMEM((PAIR_ROWS, width), BF16), pltpu.VMEM((count, 3 * width), BF16), small,
                          pltpu.VMEM((width, count), BF16), small, pltpu.VMEM((width, width), F32),
                          pltpu.VMEM((*CUBE, width // SHARDS * 3, LANES), F32),
                          pltpu.VMEM((*CUBE, size, LANES), F32), pltpu.SemaphoreType.DMA,
                          pltpu.SemaphoreType.DMA, *w_scratch, small, small, pltpu.SemaphoreType.DMA((2,)))

    place.entry_barrier()
    hidden_copy(0).start()
    for layer in range(blocks):
        rows_copy(layer).start()
    d_rows_ref[:] = jnp.zeros_like(d_rows_ref)
    vec_ref[:] = jnp.zeros_like(vec_ref)

    def load_cot(cot, sem):
        copy = pltpu.make_async_copy(cot_ref, cot, sem)
        copy.start()
        copy.wait()
        each_chunk(lambda at: grad_ref.__setitem__(at, cot[at].astype(F32)))

    pl.run_scoped(load_cot, pltpu.VMEM(cot_ref.shape, BF16), pltpu.SemaphoreType.DMA)
    for layer in range(blocks):
        rows_copy(layer).wait()
    for index, (layer, kind) in enumerate(phases):
        hidden_copy(index).wait()
        if index + 1 < len(phases):
            hidden_copy(index + 1).start()
        if kind == 'h2':
            ff_phase(layer, index, plan[index])
        else:
            attention_phase(layer, index, plan[index], kind == 'h1')

    def finish(stage, sem, image, sem_image, vec_out, images, out_sems):
        def cast(at):
            image[at] = grad_ref[at].astype(BF16)

        each_chunk(cast)
        copy_image = pltpu.make_async_copy(image, gx_ref, sem_image)
        copy_image.start()
        per_device = 17 * width // SHARDS
        stage[:] = jnp.zeros_like(stage)
        for layer in range(blocks):
            vec = vec_ref.at[layer]
            for row in range(9):
                for tile in range(width // LANES):
                    at = row * (width // LANES) + tile
                    vec[at:at + 1] = d_rows_ref[layer, row:row + 1, lanes(tile)]
            lane = lax.broadcasted_iota(jnp.int32, (SUB, LANES), 1)
            for shard in range(SHARDS):
                row, off = divmod(shard * per_device, LANES)
                here, after = vec[pl.ds(row, SUB)], vec[pl.ds(row + 1, SUB)]
                if off:
                    here = jnp.where(lane < LANES - off, pltpu.roll(here, LANES - off, 1), pltpu.roll(after, LANES - off, 1))
                bits = [shard // weight % 2 for weight in WEIGHT]
                stage[(*bits, pl.ds(layer * layout.vec_rows, layout.vec_rows))] = here
        copy = pltpu.make_async_copy(stage, region(layout.vec, stage.shape[4]), sem)
        copy.start()
        copy.wait()

        def convert(layer, name):
            target = images[MATS.index(name)]
            first = base(layer) + getattr(layout, name)
            part = width // SHARDS
            total = target.shape[0]
            many = total // (context_ref.shape[1] // SHARDS if name == 'kv2' else part)

            def put(tile, size, stride, row):
                target[pl.ds(tile, size, stride=stride), layer] = out_ref[row:row + size]

            if name == 'ff1':
                for index in range(many):
                    half, at = divmod(index, many // 2)
                    step, tile = divmod(at, 2)
                    put(index, part, many, first + step * 160 + half * 80 + tile * part)
            elif name == 'ff2':
                tiles = width // LANES
                for block in range(total // 160):
                    for tile in range(tiles):
                        put(block * 160 + tile, 32, tiles, first + block * 160 + tile * 32)
            else:
                for index in range(many):
                    put(index, total // many, many, first + index * (total // many))

        jobs = [(blocks - 1, name) for name in MATS] + [(0, name) for name in ('ff1', 'ff2', '', 'kv2', 'q2', 'out2')]

        def tail(index):
            reducer.step(plan[-1] + index)
            for number, (layer, name) in enumerate(jobs):
                if name:
                    @pl.when(index == min(number, layout.macros + STREAMS * STAGES - plan[-1] - 1))
                    def _(layer=layer, name=name):
                        convert(layer, name)

        repeat(layout.macros + STREAMS * STAGES - plan[-1], tail)
        convert(0, 'qkv')
        convert(0, 'out')
        copies = [load(source, target, out_sems.at[number])
                  for number, (source, target) in enumerate(zip(images, out_refs))]
        for layer in range(blocks):
            for row in range(-(-per_device // LANES)):
                at = layout.vec + layer * layout.vec_rows + row
                size = min(LANES, per_device - row * LANES)
                vec_out[layer:layer + 1, row * LANES:row * LANES + size] = line(out_ref, at)[:, :size]
        load(vec_out, out_refs[-1], sem).wait()
        for copy in copies:
            copy.wait()
        copy_image.wait()

    pl.run_scoped(finish, pltpu.VMEM((*CUBE, blocks * layout.vec_rows + layout.pad, LANES), F32),
                  pltpu.SemaphoreType.DMA, pltpu.VMEM(cot_ref.shape, BF16), pltpu.SemaphoreType.DMA,
                  pltpu.VMEM(out_refs[-1].shape, F32), [pltpu.VMEM(ref.shape, F32) for ref in out_refs[:-1]],
                  pltpu.SemaphoreType.DMA((len(MATS),)))


def backward(cot, context, saved, tokens, ctx_len, total, out_shapes):
    count, width = cot.shape
    blocks = len(saved)
    layout = Layout(width, context.shape[1], blocks)
    cfg = (tokens, ctx_len, width, blocks, layout, total, PLAN)
    operands = [cot, context]
    for block in saved:
        operands += [block[name] for name in NAMES]
    shape = saved[0]['rows'].shape
    outs = pl.pallas_call(
        functools.partial(backward_kernel, cfg),
        in_specs=any_specs(len(operands)), out_specs=any_specs(3 + len(MATS)),
        out_shape=[jax.ShapeDtypeStruct((count, width), BF16),
                   jax.ShapeDtypeStruct((*CUBE, layout.rows, LANES), F32)]
        + [jax.ShapeDtypeStruct(shape, F32) for shape in out_shapes],
        scratch_shapes=[pltpu.VMEM((count, width), F32), pltpu.VMEM((2, count, width), F32),
                        pltpu.VMEM((blocks,) + shape, F32), pltpu.VMEM((blocks,) + shape, F32),
                        pltpu.VMEM((blocks, 96, LANES), F32), pltpu.VMEM((layout.rows, LANES), F32),
                        pltpu.SemaphoreType.DMA((2 + blocks,))] + Reducer.scratch(),
        name='backward', **settings(0),
    )(*operands)
    return outs[0], outs[2:]


PLAN = [(0, 4, 6), (6, 4, 0), (10, 6, 1), (17, 0, SUB), (25, 5, 0), (30, 6, 1), 37]


def solution(mesh):
    n_dev = mesh.shape[AXIS]

    def local(tokens_x, context, cot_out, *shards):
        samples, tokens, width = tokens_x.shape
        blocks = shards[0].shape[0]
        spare = -shards[-1].shape[1] % LANES
        padded = shards[:-1] + (jnp.pad(shards[-1], ((0, 0), (0, spare))),)
        raws = [shard.reshape(blocks, -1, LANES).swapaxes(0, 1) for shard in padded]
        saved, ctx_rows, out_tokens = forward(tokens_x, context, raws)
        out_shapes = [raw.shape for raw in raws[:-1]] + [shards[-1].shape]
        grad_x, grads = backward(cot_out.reshape(samples * tokens, width), ctx_rows, saved, tokens, context.shape[1],
                                 samples * n_dev, out_shapes)
        grads = [grad.swapaxes(0, 1).reshape(blocks, -1) for grad in grads[:-1]] + [grads[-1]]
        return (out_tokens.reshape(tokens_x.shape), grad_x.reshape(tokens_x.shape), *grads)

    param_spec = P(None, AXIS)
    in_specs = (P(AXIS), P(AXIS), P(AXIS)) + (param_spec,) * 8
    out_specs = (P(AXIS), P(AXIS)) + (param_spec,) * 8
    return jax.shard_map(local, mesh=mesh, in_specs=in_specs, out_specs=out_specs, check_vma=False)
```

```python
import functools
import math
from typing import Any, NamedTuple
import jax
import jax.numpy as jnp
from jax import lax
from jax.experimental import pallas as pl
from jax.experimental.pallas import tpu as pltpu
from jax.sharding import PartitionSpec as P

AXIS = 'fsdp'
HEAD = 64
EPS = 1e-5
SHARDS = 16
CUBE = (2, 2, 2, 2)
WEIGHT = (8, 4, 2, 1)
CHIP_WEIGHT = WEIGHT[1:]
CHIPS = 8
SUB = 8
FULL = slice(None)
SELF_ROWS, CROSS_ROWS = (0, 1, 6), (2, 3, 7)
F32 = jnp.float32
BF16 = jnp.bfloat16
LANES = 128
VMEM_BYTES = 63 * 2 ** 20
BELL = (2 * math.pi) ** -0.5
LN_ROWS = 128
PAIR_ROWS = 512
FF_ROWS = 256
FF_COLS = 256

TAIL_P = 0.265
TAIL = (0.10574158579953814, 0.10524628753634038, 0.10270369607548423, 0.0603023517537824, 0.13797880111692826,
        -0.11640058407079061, 0.2178489286936914, -0.1442454807654402, 0.03082441619112092)


def mm(lhs, rhs):
    return jnp.dot(lhs, rhs, preferred_element_type=F32)


def mm_nt(lhs, rhs):
    return lax.dot_general(lhs, rhs, (((1,), (1,)), ((), ())), preferred_element_type=F32)


def mm_tn(lhs, rhs):
    return lax.dot_general(lhs, rhs, (((0,), (0,)), ((), ())), preferred_element_type=F32)


pipeline = functools.partial(pltpu.emit_pipeline, _explicit_indices=True)


def lane_mean(x):
    return jnp.mean(x, axis=-1, keepdims=True)


def lane_sum(x):
    return jnp.sum(x, axis=-1, keepdims=True)


def row_sum(x):
    return jnp.sum(x, axis=0, keepdims=True)


def line(ref, index):
    return ref[index:index + 1]


def add_line(ref, index, values):
    ref[index:index + 1] += values


def span(index, size):
    return pl.ds(pl.multiple_of(index * size, size), size)


def pieces_of(first, size):
    return [pl.ds(pl.multiple_of(first + piece * LN_ROWS, LN_ROWS), LN_ROWS) for piece in range(size // LN_ROWS)]


def lanes(tile):
    return slice(tile * LANES, (tile + 1) * LANES)


def repeat(count, body):
    def one(index, carry):
        body(index)
        return carry

    lax.fori_loop(0, count, one, 0)


def normalize(x):
    centered = x - lane_mean(x)
    scale = lax.rsqrt(lane_mean(centered * centered) + EPS)
    return centered * scale, scale


def norm_back(x, d_norm, gain):
    hat, scale = normalize(x)
    d_hat = d_norm * gain
    pulled = d_hat - lane_mean(d_hat) - hat * lane_mean(d_hat * hat)
    return pulled * scale, row_sum(d_norm * hat), row_sum(d_norm)


def low_half(rows):
    return lax.broadcasted_iota(jnp.int32, (rows, LANES), 1) < HEAD


def head_stack(pair, low):
    zero = jnp.zeros_like(pair)
    return jnp.concatenate([jnp.where(low, pair, zero), jnp.where(low, zero, pair)], axis=0)


def head_unstack(stacked, low):
    half = stacked.shape[0] // 2
    return jnp.where(low, stacked[:half], stacked[half:])


def softmax_halves(scores, valid):
    half = scores.shape[0] // 2
    parts = []
    for part in (scores[:half], scores[half:]):
        if valid < half:
            part = jnp.where(lax.broadcasted_iota(jnp.int32, part.shape, 0) < valid, part, -jnp.inf)
        part = jnp.exp(part - jnp.max(part, axis=0, keepdims=True))
        parts.append(part * (1.0 / row_sum(part)))
    return parts


def stack_bf16(parts):
    return jnp.concatenate([part.astype(BF16) for part in parts], axis=0)


def rows_at(number):
    return slice(number * FF_ROWS, (number + 1) * FF_ROWS)


def ahead(count, first, second):
    ready = first(0)
    for index in range(count):
        now = ready
        if index + 1 < count:
            ready = first(index + 1)
        second(index, now)


def scaled(query):
    return query * BF16(HEAD ** -0.5)


def pair_scores(query, keys):
    return mm_nt(head_stack(keys, low_half(keys.shape[0])), scaled(query))


def pair_forward(scores, values, valid):
    probs = stack_bf16(softmax_halves(scores, valid))
    return mm_tn(head_stack(values, low_half(values.shape[0])), probs).astype(BF16).T


def pair_backward_scores(query, keys, values, d_out):
    low = low_half(keys.shape[0])
    return mm_nt(head_stack(keys, low), scaled(query)), mm_nt(head_stack(values, low), d_out)


def pair_backward(scores, d_probs, query, keys, d_out, valid):
    low = low_half(keys.shape[0])
    half = keys.shape[0]
    parts = softmax_halves(scores, valid)
    d_values = head_unstack(mm(stack_bf16(parts), d_out), low).astype(BF16)
    d_scores = []
    for part, d_part in zip(parts, (d_probs[:half], d_probs[half:])):
        d_scores.append(part * (d_part - row_sum(part * d_part)))
    d_scores = stack_bf16(d_scores)
    d_query = (mm_tn(head_stack(keys, low), d_scores) * HEAD ** -0.5).astype(BF16).T
    return d_query, head_unstack(mm(d_scores, scaled(query)), low).astype(BF16), d_values


def normal_cdf(u):
    t = 1.0 / (1.0 + TAIL_P * jnp.abs(u))
    poly = TAIL[-1]
    for coef in TAIL[-2::-1]:
        poly = poly * t + coef
    bell = jnp.exp(u * u * -0.5)
    tail = bell * (t * poly)
    return jnp.where(u >= 0, 1.0 - tail, tail), bell


UNIT = 80
COLORS = 3
MACRO = COLORS * UNIT
SLOTS = 3
STREAMS = 2
STAGES = 4
CORE = 3
ORDERS = ((2, 1, 0), (1, 0, 2), (0, 2, 1))
MESH = pl.DeviceIdType.MESH


def bits_of(device):
    return [lax.rem(lax.div(device, weight), 2) for weight in WEIGHT]


class Place:
    def __init__(self):
        me = lax.axis_index(AXIS)
        self.bits = bits_of(me)
        self.others = [1 - bit for bit in self.bits]
        self.devices = [(me + (other - bit) * weight,) for bit, other, weight in zip(self.bits, self.others, WEIGHT)]

    def rows_of(self, ref, first, rows):
        half = ref.shape[CORE] // 2
        return pl.ds(pl.multiple_of(self.bits[CORE] * half + first, SUB), rows)

    def own(self, ref):
        return ref.at[(*self.bits[:CORE], self.rows_of(ref, 0, ref.shape[CORE] // 2))]

    def entry_barrier(self):
        barrier = pltpu.get_barrier_semaphore()
        for device in self.devices:
            pl.semaphore_signal(barrier, inc=1, device_id=device, device_id_type=MESH)
        pl.semaphore_wait(barrier, 4)


def pick(ref, lead, dim, value):
    return ref.at[(lead,) + (FULL,) * dim + (value,)]


class At(NamedTuple):
    stream: Any
    index: Any
    row: Any


class Reducer:
    def __init__(self, place, macros, scale, grads, out, refs):
        self.place, self.macros, self.scale, self.grads, self.out = place, macros, scale, grads, out
        self.own, self.held = refs[0], refs[1:1 + STAGES]
        self.send, self.recv, self.load = refs[1 + STAGES:]

    @staticmethod
    def scratch():
        held = [pltpu.VMEM((STREAMS * SLOTS * COLORS,) + (2,) * (3 - stage) + (UNIT, LANES), F32) for stage in range(STAGES)]
        sems = [pltpu.SemaphoreType.DMA((STREAMS, COLORS, STAGES)), pltpu.SemaphoreType.DMA((STREAMS * SLOTS * COLORS, STAGES)),
                pltpu.SemaphoreType.DMA((STREAMS, COLORS))]
        return [pltpu.VMEM((STREAMS * COLORS, *CUBE[1:], UNIT, LANES), F32)] + held + sems

    def axis(self, color, stage):
        return CORE if stage == 0 else ORDERS[color][stage - 1]

    def dim(self, color, stage):
        gone = ORDERS[color][:stage - 1]
        return sum(1 for axis in range(ORDERS[color][stage - 1]) if axis not in gone)

    def copy(self, at, color, stage):
        axis = self.axis(color, stage)
        other = self.place.others[axis]
        index = at.index + color
        if stage == 0:
            source = self.grads.at[:, :, :, other, pl.ds(at.row + color * UNIT, UNIT)]
        else:
            source = pick(self.held[stage - 1], index, self.dim(color, stage), other)
        return pltpu.make_async_remote_copy(
            src_ref=source, dst_ref=self.held[stage].at[index], send_sem=self.send.at[at.stream, color, stage],
            recv_sem=self.recv.at[index, stage], device_id=self.place.devices[axis], device_id_type=MESH)

    def own_copy(self, at, color):
        return pltpu.make_async_copy(self.grads.at[:, :, :, self.place.bits[CORE], pl.ds(at.row + color * UNIT, UNIT)],
                                     self.own.at[at.stream * COLORS + color], self.load.at[at.stream, color])

    def add(self, at, color, stage):
        index = at.index + color
        if stage == 0:
            self.held[0][index] += self.own[at.stream * COLORS + color]
            return
        mine = self.held[stage - 1][(index,) + (FULL,) * self.dim(color, stage)
                                    + (self.place.bits[self.axis(color, stage)],)]
        if stage < STAGES - 1:
            self.held[stage][index] += mine
        else:
            self.out[pl.ds(at.row + color * UNIT, UNIT)] = (self.held[stage][index] + mine) * self.scale

    def step(self, t):
        stream, tau = lax.rem(t, STREAMS), lax.div(t, STREAMS)

        def when_live(local, body):
            @pl.when((local >= 0) & (local * STREAMS + stream < self.macros))
            def _():
                body(At(stream, (stream * SLOTS + lax.rem(local, SLOTS)) * COLORS,
                        pl.multiple_of((local * STREAMS + stream) * MACRO, SUB)))

        def take(stage, at):
            for color in range(COLORS):
                copy = self.copy(at, color, stage)
                copy.wait_send()
                copy.wait_recv()
                if stage == 0:
                    self.own_copy(at, color).wait()
            for color in range(COLORS):
                self.add(at, color, stage)

        def give(stage, at):
            for color in range(COLORS):
                self.copy(at, color, stage).start()
                if stage == 0:
                    self.own_copy(at, color).start()

        for stage in reversed(range(STAGES)):
            when_live(tau - 1 - stage, functools.partial(take, stage))
        for stage in range(STAGES):
            when_live(tau - stage, functools.partial(give, stage))


class Piece(NamedTuple):
    ref: Any
    first: Any
    rows: Any
    cols: Any
    color: int
    number: int


class Gatherer:
    def __init__(self, place, macros, send, recv):
        self.place, self.macros, self.send, self.recv = place, [], send, recv
        number = 0
        for macro in macros:
            pieces = []
            for ref, color, first, rows, cols in macro:
                pieces.append(Piece(ref, first, rows, cols, color, number))
                number += 1
            self.macros.append(pieces)

    def copy(self, piece, stage):
        order = ORDERS[piece.color]
        index = [FULL if axis in order[:stage] else self.place.bits[axis] for axis in range(CORE)]
        block = piece.ref.at[(*index, self.place.rows_of(piece.ref, piece.first, piece.rows), piece.cols)]
        axis = order[stage] if stage < CORE else CORE
        return pltpu.make_async_remote_copy(
            src_ref=block, dst_ref=block, send_sem=self.send.at[piece.number, stage],
            recv_sem=self.recv.at[piece.number, stage], device_id=self.place.devices[axis], device_id_type=MESH)

    def step(self, t):
        for macro, pieces in enumerate(self.macros):
            stage = t - macro
            if stage in range(1, STAGES + 1):
                for piece in pieces:
                    copy = self.copy(piece, stage - 1)
                    copy.wait_send()
                    copy.wait_recv()
            if stage in range(STAGES):
                for piece in pieces:
                    self.copy(piece, stage).start()

    def beside(self, index, plan):
        first, count = plan
        for number in range(count):
            @pl.when(index == 2 * number + 1)
            def _(number=number):
                self.step(first + number)


def thirds(tiles):
    edges = [round(tiles * part / 3) * LANES for part in range(4)]
    return [slice(first, last) for first, last in zip(edges[:-1], edges[1:])]


FORWARD_PLAN = [(5, 3), (8, 3), (11, 5), (SHARDS, 2), (0, 0), (0, 0)]
MATS = ('qkv', 'out', 'q2', 'kv2', 'out2', 'ff1', 'ff2')
WEIGHTS = ('w_a', 'w_b', 'w_kv2', 'w_ff1', 'w_ff2')
KEPT = ('h', 'h1', 'h2', 'qkv', 'out1', 'q', 'kv', 'out2', 'fa', 'fg', 'z', 'rows')


def load(source, target, sem):
    copy = pltpu.make_async_copy(source, target, sem)
    copy.start()
    return copy


def fetch(source, cols, target, sems):
    def copy(shard):
        index = [lax.rem(lax.div(shard, weight), 2) for weight in CHIP_WEIGHT]
        return pltpu.make_async_copy(source.at[(*index, FULL, cols)], target.at[span(shard, source.shape[CORE])],
                                     sems.at[shard])

    repeat(CHIPS, lambda shard: copy(shard).start())
    return lambda: repeat(CHIPS, lambda shard: copy(shard).wait())


def macro_list(weights, vec):
    macros = []
    for block in weights:
        high = {name: block[name].shape[CORE] // 2 for name in WEIGHTS}
        cols = {name: thirds(block[name].shape[-1] // LANES) for name in ('w_a', 'w_b', 'w_kv2')}
        wide = block['w_ff1'].shape[-1] // 2

        def add(name, first, rows, cols):
            macros.append([(block[name], color, first, rows, part) for color, part in enumerate(cols)])

        add('w_a', 0, high['w_a'], cols['w_a'])
        for part in range(2):
            add('w_kv2', part * high['w_kv2'] // 2, high['w_kv2'] // 2, cols['w_kv2'])
        add('w_b', 0, high['w_b'], cols['w_b'])
        for part in range(2):
            add('w_ff1', 0, high['w_ff1'],
                [pl.ds(part * wide + third.start, third.stop - third.start) for third in thirds(wide // LANES)])
        tenth = high['w_ff2'] // 10
        macros.append([(block['w_ff2'], color, first * tenth, rows * tenth, FULL)
                       for color, (first, rows) in enumerate(((0, 3), (3, 4), (7, 3)))])
    macros[0].append((vec, 0, 0, vec.shape[CORE] // 2, FULL))
    return macros


def forward_kernel(cfg, *refs):
    tokens, width, blocks, per_vec = cfg
    heads = width // HEAD
    tiles = width // LANES
    tokens_ref, context_ref = refs[:2]
    raw_refs = refs[2:2 + len(MATS) + 1]
    refs = refs[2 + len(raw_refs):]
    kept = [dict(zip(KEPT, refs[layer * len(KEPT):])) for layer in range(blocks)]
    refs = refs[blocks * len(KEPT):]
    weights = [dict(zip(WEIGHTS, refs[layer * len(WEIGHTS):])) for layer in range(blocks)]
    refs = refs[blocks * len(WEIGHTS):]
    vec_all_ref, ctx_out_ref, tokens_out_ref, hidden, context, rows_ref, vec_ref, sems, send, recv = refs
    samples, ctx_len = context_ref.shape[:2]
    pad = context.shape[0] // samples
    count = tokens_ref.shape[0]
    chunk = PAIR_ROWS
    per_step = chunk // tokens
    place = Place()
    gatherer = Gatherer(place, macro_list(weights, vec_all_ref), send, recv)

    def each_piece(body):
        repeat(count // chunk, lambda index: [body(at) for at in pieces_of(index * chunk, chunk)])

    def startup(image, wide, flat, vec_piece, raws, pieces, raw_sems, own_sems):
        first = [load(tokens_ref, image, sems.at[0]), load(context_ref, wide, sems.at[1])]
        loads = [load(source, target, raw_sems.at[index])
                 for index, (source, target) in enumerate(zip(raw_refs, raws))]

        def tile(layer, name, target, first_col):
            raw = raws[MATS.index(name)]
            flat[:raw.shape[0]] = raw[:].astype(F32)
            rows = target.shape[0]
            stride = raw.shape[0] // rows
            for index in range(stride // blocks):
                at = first_col + index * LANES
                target[:, at:at + LANES] = flat[pl.ds(index * blocks + layer, rows, stride=stride)].astype(BF16)

        def own(layer, name):
            number = layer * len(WEIGHTS) + WEIGHTS.index(name)
            return load(pieces[number], place.own(weights[layer][name]), own_sems.at[number])

        def prepare(layer, name):
            target = pieces[layer * len(WEIGHTS) + WEIGHTS.index(name)]
            if name == 'w_a':
                tile(layer, 'qkv', target, 0)
                tile(layer, 'out', target, 3 * width)
            elif name == 'w_b':
                tile(layer, 'q2', target, 0)
                tile(layer, 'out2', target, width)
            else:
                tile(layer, name[2:], target, 0)
            return own(layer, name)

        for copy in loads:
            copy.wait()
        vec_piece[:] = jnp.zeros_like(vec_piece)
        for layer in range(blocks):
            flat[:per_vec] = raws[-1][:, layer].astype(F32)
            vec_piece[layer * SUB:layer * SUB + per_vec] = flat[:per_vec].astype(BF16)
        pending = [prepare(0, 'w_a'), load(vec_piece, place.own(vec_all_ref), sems.at[2])]
        place.entry_barrier()
        later = [[(0, 'w_kv2')], [(0, 'w_b'), (0, 'w_ff1'), (0, 'w_ff2')], [(1, 'w_a'), (1, 'w_kv2'), (1, 'w_b')],
                 [(1, 'w_ff1'), (1, 'w_ff2')]]
        for t, jobs in enumerate(later):
            for copy in pending:
                copy.wait()
            gatherer.step(t)
            pending = [prepare(layer, name) for layer, name in jobs if layer < blocks]
        for copy in first:
            copy.wait()
        each_piece(lambda at: hidden.at[0].__setitem__(at, image[at].astype(F32)))
        context[:] = jnp.zeros_like(context)
        for sample in range(samples):
            context[sample * pad:sample * pad + ctx_len] = wide[sample]
        for copy in pending:
            copy.wait()
        gatherer.step(len(later))

    def raw_shape(index):
        return pltpu.VMEM(raw_refs[index].shape, BF16)

    pl.run_scoped(startup, pltpu.VMEM(tokens_ref.shape, BF16), pltpu.VMEM(context_ref.shape, BF16),
                  pltpu.VMEM((max(ref.shape[0] for ref in raw_refs), LANES), F32), pltpu.VMEM((blocks * SUB, LANES), BF16),
                  [raw_shape(index) for index in range(len(raw_refs))],
                  [pltpu.VMEM((block[name].shape[CORE] // 2, block[name].shape[-1]), BF16)
                   for block in weights for name in WEIGHTS],
                  pltpu.SemaphoreType.DMA((len(raw_refs),)), pltpu.SemaphoreType.DMA((blocks * len(WEIGHTS),)))
    ctx_copy = load(context, ctx_out_ref, sems.at[3])

    def unpack(parts, sem):
        load(vec_all_ref, parts, sem).wait()
        vec_ref[:] = jnp.zeros_like(vec_ref)
        rows_ref[:] = jnp.zeros_like(rows_ref)
        lane = lax.broadcasted_iota(jnp.int32, (SUB, LANES), 1)
        per_device = 17 * width // SHARDS
        for layer in range(blocks):
            vec = vec_ref.at[layer]
            for shard in range(SHARDS):
                chip, core = divmod(shard, 2)
                bits = [chip // weight % 2 for weight in CHIP_WEIGHT]
                part = parts[(*bits, pl.ds((core * blocks + layer) * SUB, SUB))].astype(F32)
                row, off = divmod(shard * per_device, LANES)
                if off:
                    part = pltpu.roll(part, off, 1)
                    vec[pl.ds(row + 1, SUB)] += jnp.where(lane < off, part, 0.0)
                vec[pl.ds(row, SUB)] += jnp.where(lane >= off, part, 0.0)
            for row in range(9):
                for tile in range(tiles):
                    rows_ref[layer, row:row + 1, lanes(tile)] = line(vec, row * tiles + tile)

    pl.run_scoped(unpack, pltpu.VMEM(vec_all_ref.shape, BF16), pltpu.SemaphoreType.DMA)
    rows_copies = [load(rows_ref.at[layer], kept[layer]['rows'], sems.at[4 + layer]) for layer in range(blocks)]

    def attention(layer, source, target, cross, plan):
        rows = rows_ref.at[layer]
        packed = weights[layer]['w_b' if cross else 'w_a']
        inner = packed.shape[-1] - width
        gain, shift, bias = CROSS_ROWS if cross else SELF_ROWS

        def scoped(norm, w_in, w_out, w_kv, kv, in_sems):
            waits = [fetch(packed, pl.ds(0, inner), w_in, in_sems.at[0]), fetch(packed, pl.ds(inner, width), w_out, in_sems.at[1])]
            if cross:
                fetch(weights[layer]['w_kv2'], FULL, w_kv, in_sems.at[2])()
                kv[:] = mm(context[:], w_kv[:]).astype(BF16)
                kv_copy = load(kv, kept[layer]['kv'], in_sems.at[2, 0])
            for wait in waits:
                wait()

            def body(idx, qkv, mixed):
                step = idx.index[0]
                at_rows = span(step, chunk)
                for at, here in zip(pieces_of(step * chunk, chunk), pieces_of(0, chunk)):
                    hat, unused = normalize(source[at])
                    norm[here] = (hat * line(rows, gain) + line(rows, shift)).astype(BF16)
                qkv[:] = mm(norm[:], w_in[:]).astype(BF16)

                def sample(number):
                    at = span(number, tokens)
                    index = step * per_step + number
                    kv_at = span(index, pad) if cross else at
                    k_ref, k_first, limit = (kv, 0, ctx_len) if cross else (qkv, width, tokens)

                    def scores(pair):
                        return pair_scores(qkv[at, lanes(pair)], k_ref[kv_at, lanes(pair + k_first // LANES)])

                    def rest(pair, ready):
                        values = k_ref[kv_at, lanes(pair + (k_first + width) // LANES)]
                        mixed[at, lanes(pair)] = pair_forward(ready, values, limit)

                    ahead(heads // 2, scores, rest)
                    gatherer.beside(index, plan)

                repeat(per_step, sample)
                target[at_rows] = source[at_rows] + mm(mixed[:], w_out[:]) + line(rows, bias)

            block = lambda cols: pl.BlockSpec((chunk, cols), lambda step: (step, 0))
            pipeline(body, grid=(count // chunk,), out_specs=[block(inner), block(width)])(
                kept[layer]['q' if cross else 'qkv'], kept[layer]['out2' if cross else 'out1'])
            if cross:
                kv_copy.wait()

        small = pltpu.VMEM((SUB, LANES), BF16)
        pl.run_scoped(scoped, pltpu.VMEM((chunk, width), BF16), pltpu.VMEM((width, inner), BF16),
                      pltpu.VMEM((width, width), BF16), pltpu.VMEM((context_ref.shape[2], 2 * width), BF16) if cross else small,
                      pltpu.VMEM((samples * pad, 2 * width), BF16) if cross else small, pltpu.SemaphoreType.DMA((3, CHIPS)))

    def feed_forward(layer, source, target, plan):
        rows = rows_ref.at[layer]
        vec = vec_ref.at[layer]
        inner = weights[layer]['w_ff1'].shape[-1] // 2
        steps = inner // FF_COLS
        part = FF_COLS // LANES

        def scoped(norm, w1, w2, w_sems):
            waits = [fetch(weights[layer]['w_ff1'], FULL, w1, w_sems.at[0]), fetch(weights[layer]['w_ff2'], FULL, w2, w_sems.at[1])]

            def begin(at):
                hat, unused = normalize(source[at])
                norm[at] = (hat * line(rows, 4) + line(rows, 5)).astype(BF16)
                target[at] = source[at] + line(rows, SUB)

            each_piece(begin)
            for wait in waits:
                wait()

            def body(idx, fa, fg, z):
                step = idx.index[0]
                cols, gate_cols = span(step, FF_COLS), span(step + steps, FF_COLS)

                def bias(half):
                    first = 9 * tiles + (half * steps + step) * part
                    return jnp.concatenate([vec[pl.ds(first + index, 1)] for index in range(part)], axis=1)

                bias_a, bias_g = bias(0), bias(1)

                def hidden_of(number):
                    normed = norm[rows_at(number)]
                    return mm(normed, w1[:, gate_cols]) + bias_g, mm(normed, w1[:, cols]) + bias_a

                def rest(number, ready):
                    at = rows_at(number)
                    gate, value = ready
                    cdf, bell = normal_cdf(gate)
                    factor = gate * cdf
                    z[at] = (value * factor).astype(BF16)
                    fa[at] = factor
                    fg[at] = value * (cdf + gate * bell * BELL)
                    target[at] += mm(z[at], w2[cols])

                ahead(count // FF_ROWS, hidden_of, rest)
                gatherer.beside(step, plan)

            block = ff_block(count)
            pipeline(body, grid=(steps,), out_specs=[block, block, block])(
                kept[layer]['fa'], kept[layer]['fg'], kept[layer]['z'])

        pl.run_scoped(scoped, pltpu.VMEM((count, width), BF16), pltpu.VMEM((width, 2 * inner), BF16),
                      pltpu.VMEM((inner, width), BF16), pltpu.SemaphoreType.DMA((2, CHIPS)))

    phases = len(FORWARD_PLAN)
    saves = [load(hidden.at[0], kept[0]['h'], sems.at[6]), None]
    for phase in range(phases):
        layer, kind = divmod(phase, 3)
        source, target = hidden.at[phase % 2], hidden.at[(phase + 1) % 2]
        other = (phase + 1) % 2
        if saves[other] is not None:
            saves[other].wait()
        if kind < 2:
            attention(layer, source, target, kind == 1, FORWARD_PLAN[phase])
        else:
            feed_forward(layer, source, target, FORWARD_PLAN[phase])
        following = divmod(phase + 1, 3)
        saves[other] = None
        if phase + 1 < phases:
            saves[other] = load(target, kept[following[0]][KEPT[following[1]]], sems.at[6 + other])

    def finish(image):
        each_piece(lambda at: image.__setitem__(at, hidden[phases % 2, at].astype(BF16)))
        load(image, tokens_out_ref, sems.at[0]).wait()

    pl.run_scoped(finish, pltpu.VMEM(tokens_ref.shape, BF16))
    for copy in [copy for copy in saves if copy is not None] + [ctx_copy] + rows_copies:
        copy.wait()


def settings(number):
    return dict(compiler_params=pltpu.CompilerParams(collective_id=number, has_side_effects=True,
                                                     vmem_limit_bytes=VMEM_BYTES),
                cost_estimate=pl.CostEstimate(flops=10 ** 11, bytes_accessed=10 ** 8, transcendentals=0))


def ff_block(count):
    return pl.BlockSpec((None, count, FF_COLS), lambda step: (step, 0, 0))


def any_specs(count):
    return [pl.BlockSpec(memory_space=pl.ANY)] * count


def forward(tokens_x, context, raws, blocks):
    samples, tokens, width = tokens_x.shape
    ctx_width = context.shape[2]
    count, inner = samples * tokens, 4 * width
    pad = -(-context.shape[1] // SHARDS) * SHARDS
    steps = inner // FF_COLS
    plain = jax.ShapeDtypeStruct((count, width), F32)
    half = jax.ShapeDtypeStruct((count, width), BF16)
    wide = jax.ShapeDtypeStruct((steps, count, FF_COLS), F32)
    kept = [plain, plain, plain, jax.ShapeDtypeStruct((count, 3 * width), BF16), half, half,
            jax.ShapeDtypeStruct((samples * pad, 2 * width), BF16), half, wide, wide,
            jax.ShapeDtypeStruct(wide.shape, BF16), jax.ShapeDtypeStruct((SHARDS, width), F32)]
    whole_of = lambda rows, cols: jax.ShapeDtypeStruct((*CUBE[:CORE], rows // CHIPS, cols), BF16)
    weights = [whole_of(width, 4 * width), whole_of(width, 2 * width), whole_of(ctx_width, 2 * width),
               whole_of(width, 2 * inner), whole_of(inner, width)]
    extra = [whole_of(SHARDS * blocks * SUB, LANES), jax.ShapeDtypeStruct((samples * pad, ctx_width), BF16), half]
    shapes = kept * blocks + weights * blocks + extra
    pieces = 1 + 3 * 7 * blocks
    outs = pl.pallas_call(
        functools.partial(forward_kernel, (tokens, width, blocks, raws[-1].shape[0])),
        in_specs=any_specs(2 + len(raws)), out_specs=any_specs(len(shapes)), out_shape=shapes,
        scratch_shapes=[pltpu.VMEM((2, count, width), F32), pltpu.VMEM((samples * pad, ctx_width), BF16),
                        pltpu.VMEM((blocks, SHARDS, width), F32), pltpu.VMEM((blocks, 96, LANES), F32),
                        pltpu.SemaphoreType.DMA((8,)), pltpu.SemaphoreType.DMA((pieces, STAGES)),
                        pltpu.SemaphoreType.DMA((pieces, STAGES))],
        name='forward', **settings(1),
    )(tokens_x.reshape(count, width), context, *raws)
    kept_of = [outs[layer * len(kept):(layer + 1) * len(kept)] for layer in range(blocks)]
    outs = outs[blocks * len(kept):]
    weights_of = [[whole.reshape(-1, whole.shape[-1]) for whole in outs[layer * len(weights):(layer + 1) * len(weights)]]
                  for layer in range(blocks)]
    saved = [dict(zip(KEPT + WEIGHTS, list(one) + list(two))) for one, two in zip(kept_of, weights_of)]
    return saved, outs[-2], outs[-1]


def view(values, *lead):
    return values.reshape(CUBE + lead + (LANES,))


def put_tiles(stage, values, first=0):
    rows = values.shape[0] // SHARDS
    for tile in range(values.shape[1] // LANES):
        at = first + tile * rows
        stage[:, :, :, :, at:at + rows] = view(values[:, lanes(tile)], rows)


class Layout:
    def __init__(self, width, ctx_width, blocks):
        unit = width // SHARDS * (width // LANES)
        self.ff1, self.ff2 = 0, 8 * unit
        self.kv2 = 12 * unit
        self.q2 = self.kv2 + ctx_width // SHARDS * (2 * width // LANES)
        self.out2 = self.q2 + unit
        self.qkv = self.out2 + unit
        self.out = self.qkv + 3 * unit
        self.block = self.out + unit
        self.vec = blocks * self.block
        self.vec_rows = -(-17 * width // SHARDS // LANES // SUB) * SUB
        used = self.vec + blocks * self.vec_rows
        self.macros = -(-used // MACRO)
        self.pad = self.macros * MACRO - used
        self.rows = self.macros * MACRO


NAMES = KEPT + WEIGHTS


def backward_kernel(cfg, *refs):
    tokens, ctx_len, width, blocks, layout, total, plan = cfg
    heads = width // HEAD
    cot_ref, context_ref = refs[:2]
    saved = [dict(zip(NAMES, refs[2 + layer * len(NAMES):])) for layer in range(blocks)]
    refs = refs[2 + blocks * len(NAMES):]
    gx_ref, grads_ref, sum_ref = refs[:3]
    refs = refs[3:]
    grad_ref, hidden_ref, rows_ref, d_rows_ref, vec_ref, out_ref, in_sems = refs[:7]
    place = Place()
    reducer = Reducer(place, layout.macros, 1.0 / total, grads_ref, out_ref, refs[7:])
    count = grad_ref.shape[0]
    chunk = PAIR_ROWS
    chunks = count // chunk
    phases = [(layer, kind) for layer in reversed(range(blocks)) for kind in ('h2', 'h1', 'h')]

    def hidden_copy(index):
        layer, kind = phases[index]
        return pltpu.make_async_copy(saved[layer][kind], hidden_ref.at[index % 2], in_sems.at[index % 2])

    def rows_copy(layer):
        return pltpu.make_async_copy(saved[layer]['rows'], rows_ref.at[layer], in_sems.at[2 + layer])

    def base(layer):
        return (blocks - 1 - layer) * layout.block

    def region(row, size):
        return grads_ref.at[:, :, :, :, pl.ds(pl.multiple_of(row, SUB), size)]

    def each_piece(body):
        repeat(chunks, lambda index: [body(at) for at in pieces_of(index * chunk, chunk)])

    def ff_phase(layer, index, first):
        hidden = hidden_ref.at[index % 2]
        rows = rows_ref.at[layer]
        d_rows = d_rows_ref.at[layer]
        vec = vec_ref.at[layer]
        src = saved[layer]
        w1_all, w2_all = src['w_ff1'], src['w_ff2']
        inner = w2_all.shape[0]
        steps = inner // FF_COLS
        start, lag, limit = first

        def scoped(norm_t, grad_bf, du, w1, acc, stage1, stage2, sem1, sem2):
            def begin(at):
                hat, unused = normalize(hidden[at])
                norm_t[:, at] = (hat * line(rows, 4) + line(rows, 5)).astype(BF16).T
                grad_bf[at] = grad_ref[at].astype(BF16)
                add_line(d_rows, 8, row_sum(grad_ref[at]))
                acc[at] = jnp.zeros((LN_ROWS, width), F32)

            each_piece(begin)

            def copy1(step):
                return pltpu.make_async_copy(stage1, region(base(layer) + layout.ff1 + step * 160, 160), sem1)

            def copy2(step, part):
                block = step * 8 + part
                shard = lax.div(block, 5)
                row = pl.multiple_of(base(layer) + layout.ff2 + lax.rem(block, 5) * 160, SUB)
                bits = bits_of(shard)
                return pltpu.make_async_copy(stage2.at[part], grads_ref.at[(*bits, pl.ds(row, 160))], sem2.at[part])

            def wait(step):
                copy1(step).wait()
                for part in range(8):
                    copy2(step, part).wait()

            def body(idx, w1a, w1g, w2, fa, fg, z):
                step = idx.index[0]
                w1[:, :FF_COLS] = w1a[:]
                w1[:, FF_COLS:] = w1g[:]

                sums = [jnp.zeros((1, FF_COLS), F32)] * 2

                def d_gated(number):
                    return mm_nt(grad_bf[rows_at(number)], w2[:]).astype(BF16).astype(F32)

                def rest(number, dz):
                    at = rows_at(number)
                    for half, factor in enumerate((fa, fg)):
                        part = dz * factor[at]
                        du[at, half * FF_COLS:(half + 1) * FF_COLS] = part.astype(BF16)
                        sums[half] += row_sum(part)
                    acc[at] += mm_nt(du[at], w1[:])

                ahead(count // FF_ROWS, d_gated, rest)
                for half in range(2):
                    for tile in range(2):
                        row = 9 * width // LANES + half * (inner // LANES) + 2 * step + tile
                        vec[pl.ds(row, 1)] = sums[half][:, lanes(tile)]

                @pl.when(step > 0)
                def _():
                    wait(step - 1)

                if lag:
                    @pl.when((step >= lag) & (lax.rem(step, 3) != 1))
                    def _():
                        reducer.step(start + lax.div(2 * (step - 1), 3))
                else:
                    @pl.when((step < limit) | (step == steps - 1))
                    def _():
                        reducer.step(start + jnp.minimum(step, limit))

                put_tiles(stage1, mm(norm_t[:], du[:, :FF_COLS]))
                put_tiles(stage1, mm(norm_t[:], du[:, FF_COLS:]), 80)
                d_w2 = mm_tn(z[:], grad_bf[:])
                for tile in range(width // LANES):
                    stage2[:, tile * 32:(tile + 1) * 32] = d_w2[:, lanes(tile)].reshape(8, 32, LANES)
                copy1(step).start()
                for number in range(8):
                    copy2(step, number).start()

            column = pl.BlockSpec((width, FF_COLS), lambda step: (0, step))
            kept = ff_block(count)
            pipeline(
                body, grid=(steps,),
                in_specs=[column, pl.BlockSpec((width, FF_COLS), lambda step: (0, step + steps)),
                          pl.BlockSpec((FF_COLS, width), lambda step: (step, 0)), kept, kept, kept],
            )(w1_all, w1_all, w2_all, src['fa'], src['fg'], src['z'])

            def finish(at):
                d_res, d_gain, d_shift = norm_back(hidden[at], acc[at], line(rows, 4))
                grad_ref[at] += d_res
                add_line(d_rows, 4, d_gain)
                add_line(d_rows, 5, d_shift)

            each_piece(finish)
            wait(steps - 1)

        pl.run_scoped(scoped, pltpu.VMEM((width, count), BF16), pltpu.VMEM((count, width), BF16),
                      pltpu.VMEM((count, 2 * FF_COLS), BF16), pltpu.VMEM((width, 2 * FF_COLS), BF16),
                      pltpu.VMEM((count, width), F32), pltpu.VMEM((*CUBE, 160, LANES), F32),
                      pltpu.VMEM((8, 160, LANES), F32), pltpu.SemaphoreType.DMA, pltpu.SemaphoreType.DMA((8,)))

    def attention_phase(layer, index, first, cross):
        hidden = hidden_ref.at[index % 2]
        rows = rows_ref.at[layer]
        d_rows = d_rows_ref.at[layer]
        src = saved[layer]
        packed = src['w_b' if cross else 'w_a']
        inner = packed.shape[1] - width
        steps = count // PAIR_ROWS
        per_step = PAIR_ROWS // tokens
        start, in_samples, in_tails = first
        gain, shift, bias = CROSS_ROWS if cross else SELF_ROWS
        samples = count // tokens
        pad = context_ref.shape[0] // samples
        kv_rows_all = context_ref.shape[0] if cross else count

        def scoped(d_mix, d_q, d_kv, norm_t, d_wq, d_wout, stage, stage_out, sem, sem_out, w_in, w_out, in_sems_, context, kv, ctx_sems):
            if cross:
                loads = [pltpu.make_async_copy(context_ref, context, ctx_sems.at[0]),
                         pltpu.make_async_copy(src['kv'], kv, ctx_sems.at[1])]
                for copy in loads:
                    copy.start()
                d_wq[:] = jnp.zeros_like(d_wq)
                for copy in loads:
                    copy.wait()
            d_wout[:] = jnp.zeros_like(d_wout)
            for copy in [load(packed.at[:, pl.ds(0, inner)], w_in, in_sems_.at[0]),
                         load(packed.at[:, pl.ds(inner, width)], w_out, in_sems_.at[1])]:
                copy.wait()

            def body(idx, qkv, mixed):
                step = idx.index[0]
                at_rows = span(step, PAIR_ROWS)
                grad_bf = grad_ref[at_rows].astype(BF16)
                add_line(d_rows, bias, row_sum(grad_ref[at_rows]))
                d_wout[:] += mm_tn(mixed[:], grad_bf)
                d_mix[:] = mm_nt(grad_bf, w_out[:]).astype(BF16)

                def sample(number, carry):
                    at = span(number, tokens)
                    sample_index = step * per_step + number
                    if cross:
                        kv_at, d_q_at, k_ref, d_k_ref, k_first, limit = span(sample_index, pad), at, kv, d_kv, 0, ctx_len
                    else:
                        kv_at, d_q_at = at, span(sample_index, tokens)
                        k_ref, d_k_ref, k_first, limit = qkv, d_q, width, tokens
                    d_k_at = kv_at if cross else d_q_at

                    def operands(pair):
                        k_cols, v_cols = (lanes(pair + (k_first + more) // LANES) for more in (0, width))
                        return qkv[at, lanes(pair)], k_ref[kv_at, k_cols], k_ref[kv_at, v_cols], d_mix[at, lanes(pair)]

                    def scores(pair):
                        return pair_backward_scores(*operands(pair))

                    def rest(pair, ready):
                        query, keys, values, d_out = operands(pair)
                        d_query, d_keys, d_values = pair_backward(*ready, query, keys, d_out, limit)
                        d_q[d_q_at, lanes(pair)] = d_query
                        d_k_ref[d_k_at, lanes(pair + k_first // LANES)] = d_keys
                        d_k_ref[d_k_at, lanes(pair + (k_first + width) // LANES)] = d_values

                    ahead(heads // 2, scores, rest)

                    @pl.when(sample_index < in_samples)
                    def _():
                        reducer.step(start + sample_index)

                    return carry

                lax.fori_loop(0, per_step, sample, 0)
                here_all = pieces_of(0, chunk)
                at_all = pieces_of(step * chunk, chunk)
                for at, here in zip(at_all, here_all):
                    hat, unused = normalize(hidden[at])
                    norm = (hat * line(rows, gain) + line(rows, shift)).astype(BF16)
                    if cross:
                        d_mix[here] = norm
                    else:
                        norm_t[:, at] = norm.T
                if cross:
                    d_wq[:] += mm_tn(d_mix[:], d_q[:])
                    d_norm = mm_nt(d_q[:], w_in[:])
                else:
                    d_norm = mm_nt(d_q[at_rows], w_in[:])
                for piece, at in enumerate(at_all):
                    d_res, d_gain, d_shift = norm_back(hidden[at], d_norm[piece * LN_ROWS:(piece + 1) * LN_ROWS], line(rows, gain))
                    grad_ref[at] += d_res
                    add_line(d_rows, gain, d_gain)
                    add_line(d_rows, shift, d_shift)

            block = lambda ref: pl.BlockSpec((PAIR_ROWS, ref.shape[1]), lambda step: (step, 0))
            operands = [src['q' if cross else 'qkv'], src['out2' if cross else 'out1']]
            pipeline(
                body, grid=(steps,), in_specs=[block(operands[0]), block(operands[1])],
            )(*operands)
            where = base(layer) + (layout.out2 if cross else layout.out)
            size = width // SHARDS * (width // LANES)
            if cross:
                put_tiles(stage_out, d_wq[:])
                put_tiles(stage_out, d_wout[:], size)
                copy_out = pltpu.make_async_copy(stage_out, region(base(layer) + layout.q2, 2 * size), sem_out)
            else:
                put_tiles(stage_out, d_wout[:])
                copy_out = pltpu.make_async_copy(stage_out, region(where, size), sem_out)
            copy_out.start()
            rows_each = stage.shape[4]
            cols_each = stage.shape[4] // ((context_ref.shape[1] if cross else width) // SHARDS) * LANES
            tails = (2 if cross else 3) * width // cols_each
            first_row = base(layer) + (layout.kv2 if cross else layout.qkv)

            def copy_tail(step):
                return pltpu.make_async_copy(stage, region(first_row + step * rows_each, rows_each), sem)

            def tail(step, carry):
                cols = span(step, cols_each)
                result = mm_tn(context[:], d_kv[:, cols]) if cross else mm(norm_t[:], d_q[:, cols])

                @pl.when(step > 0)
                def _():
                    copy_tail(step - 1).wait()

                put_tiles(stage, result)
                copy_tail(step).start()
                if in_tails:
                    @pl.when(step < in_tails)
                    def _():
                        reducer.step(start + in_samples + step)

                return carry

            lax.fori_loop(0, tails, tail, 0)
            copy_tail(tails - 1).wait()
            copy_out.wait()

        small = pltpu.VMEM((SUB, LANES), BF16)
        w_scratch = [pltpu.VMEM((width, inner), BF16), pltpu.VMEM((width, width), BF16), pltpu.SemaphoreType.DMA((2,))]
        size = width // SHARDS * (width // LANES)
        if cross:
            ctx_width = context_ref.shape[1]
            pl.run_scoped(scoped, pltpu.VMEM((PAIR_ROWS, width), BF16), pltpu.VMEM((PAIR_ROWS, width), BF16),
                          pltpu.VMEM((kv_rows_all, 2 * width), BF16), small, pltpu.VMEM((width, width), F32),
                          pltpu.VMEM((width, width), F32), pltpu.VMEM((*CUBE, ctx_width // SHARDS * 2, LANES), F32),
                          pltpu.VMEM((*CUBE, 2 * size, LANES), F32), pltpu.SemaphoreType.DMA,
                          pltpu.SemaphoreType.DMA, *w_scratch, pltpu.VMEM(context_ref.shape, BF16),
                          pltpu.VMEM(src['kv'].shape, BF16), pltpu.SemaphoreType.DMA((2,)))
        else:
            pl.run_scoped(scoped, pltpu.VMEM((PAIR_ROWS, width), BF16), pltpu.VMEM((count, 3 * width), BF16), small,
                          pltpu.VMEM((width, count), BF16), small, pltpu.VMEM((width, width), F32),
                          pltpu.VMEM((*CUBE, width // SHARDS * 3, LANES), F32),
                          pltpu.VMEM((*CUBE, size, LANES), F32), pltpu.SemaphoreType.DMA,
                          pltpu.SemaphoreType.DMA, *w_scratch, small, small, pltpu.SemaphoreType.DMA((2,)))

    place.entry_barrier()
    hidden_copy(0).start()
    for layer in range(blocks):
        rows_copy(layer).start()
    d_rows_ref[:] = jnp.zeros_like(d_rows_ref)
    vec_ref[:] = jnp.zeros_like(vec_ref)

    def load_cot(cot, sem):
        copy = pltpu.make_async_copy(cot_ref, cot, sem)
        copy.start()
        copy.wait()
        each_piece(lambda at: grad_ref.__setitem__(at, cot[at].astype(F32)))

    pl.run_scoped(load_cot, pltpu.VMEM(cot_ref.shape, BF16), pltpu.SemaphoreType.DMA)
    for layer in range(blocks):
        rows_copy(layer).wait()
    for index, (layer, kind) in enumerate(phases):
        hidden_copy(index).wait()
        if index + 1 < len(phases):
            hidden_copy(index + 1).start()
        if kind == 'h2':
            ff_phase(layer, index, plan[index])
        else:
            attention_phase(layer, index, plan[index], kind == 'h1')

    def finish(stage, sem, image, sem_image):
        def cast(at):
            image[at] = grad_ref[at].astype(BF16)

        each_piece(cast)
        copy_image = pltpu.make_async_copy(image, gx_ref, sem_image)
        copy_image.start()
        per_device = 17 * width // SHARDS
        stage[:] = jnp.zeros_like(stage)
        for layer in range(blocks):
            vec = vec_ref.at[layer]
            for row in range(9):
                for tile in range(width // LANES):
                    at = row * (width // LANES) + tile
                    vec[at:at + 1] = d_rows_ref[layer, row:row + 1, lanes(tile)]
            lane = lax.broadcasted_iota(jnp.int32, (SUB, LANES), 1)
            for shard in range(SHARDS):
                row, off = divmod(shard * per_device, LANES)
                here, after = vec[pl.ds(row, SUB)], vec[pl.ds(row + 1, SUB)]
                if off:
                    here = jnp.where(lane < LANES - off, pltpu.roll(here, LANES - off, 1), pltpu.roll(after, LANES - off, 1))
                bits = [shard // weight % 2 for weight in WEIGHT]
                stage[(*bits, pl.ds(layer * layout.vec_rows, layout.vec_rows))] = here
        copy = pltpu.make_async_copy(stage, region(layout.vec, stage.shape[4]), sem)
        copy.start()
        copy.wait()
        repeat(layout.macros + STREAMS * STAGES - plan[-1], lambda index: reducer.step(plan[-1] + index))
        load(out_ref, sum_ref, sem).wait()
        copy_image.wait()

    pl.run_scoped(finish, pltpu.VMEM((*CUBE, blocks * layout.vec_rows + layout.pad, LANES), F32),
                  pltpu.SemaphoreType.DMA, pltpu.VMEM(cot_ref.shape, BF16), pltpu.SemaphoreType.DMA)


def backward(cot, context, saved, tokens, ctx_len, total):
    count, width = cot.shape
    blocks = len(saved)
    layout = Layout(width, context.shape[1], blocks)
    cfg = (tokens, ctx_len, width, blocks, layout, total, PLAN)
    operands = [cot, context]
    for block in saved:
        operands += [block[name] for name in NAMES]
    shape = saved[0]['rows'].shape
    outs = pl.pallas_call(
        functools.partial(backward_kernel, cfg),
        in_specs=any_specs(len(operands)), out_specs=any_specs(3),
        out_shape=[jax.ShapeDtypeStruct((count, width), BF16),
                   jax.ShapeDtypeStruct((*CUBE, layout.rows, LANES), F32),
                   jax.ShapeDtypeStruct((layout.rows, LANES), F32)],
        scratch_shapes=[pltpu.VMEM((count, width), F32), pltpu.VMEM((2, count, width), F32),
                        pltpu.VMEM((blocks,) + shape, F32), pltpu.VMEM((blocks,) + shape, F32),
                        pltpu.VMEM((blocks, 96, LANES), F32), pltpu.VMEM((layout.rows, LANES), F32),
                        pltpu.SemaphoreType.DMA((2 + blocks,))] + Reducer.scratch(),
        name='backward', **settings(0),
    )(*operands)
    return outs[0], outs[2], layout


PLAN = [(0, 2, 0), (6, 4, 0), (10, 6, 1), (17, 0, SUB), (26, 4, 0), (30, 6, 1), 37]


def deliver_kernel(cfg, sum_ref, gx_ref, tokens_ref, *out_refs):
    width, ctx_width, blocks, layout = cfg
    out_refs[-2][:] = gx_ref[:]
    out_refs[-1][:] = tokens_ref[:]
    tiles = width // LANES
    for layer in range(blocks):
        for name, target in zip(MATS, out_refs):
            first = (blocks - 1 - layer) * layout.block + getattr(layout, name)
            total = target.shape[0] // blocks
            part = {'kv2': ctx_width, 'ff2': 4 * width}.get(name, width) // SHARDS
            many = total // part

            def put(tile, size, stride, row):
                target[pl.ds(tile * blocks + layer, size, stride=stride * blocks)] = sum_ref[row:row + size]

            for index in range(many):
                if name == 'ff1':
                    half, at = divmod(index, many // 2)
                    step, tile = divmod(at, 2)
                    put(index, part, many, first + step * 160 + half * 80 + tile * part)
                elif name == 'ff2':
                    for block in range(part // 32):
                        put(block * 160 + index, 32, tiles, first + block * 160 + index * 32)
                else:
                    put(index, part, many, first + index * part)
        per_device = 17 * width // SHARDS
        for row in range(-(-per_device // LANES)):
            size = min(LANES, per_device - row * LANES)
            out_refs[len(MATS)][layer:layer + 1, row * LANES:row * LANES + size] = line(
                sum_ref, layout.vec + layer * layout.vec_rows + row)[:, :size]


def deliver(sums, grad_x, tokens, shapes, cfg):
    in_vmem = pl.BlockSpec(memory_space=pltpu.VMEM)
    out_shape = [jax.ShapeDtypeStruct(shape, F32) for shape in shapes] + [
        jax.ShapeDtypeStruct(grad_x.shape, BF16), jax.ShapeDtypeStruct(tokens.shape, BF16)]
    return pl.pallas_call(
        functools.partial(deliver_kernel, cfg), in_specs=[in_vmem] * 3, out_specs=[in_vmem] * len(out_shape),
        out_shape=out_shape, compiler_params=pltpu.CompilerParams(vmem_limit_bytes=VMEM_BYTES), name='deliver',
    )(sums, grad_x, tokens)


def solution(mesh):
    n_dev = mesh.shape[AXIS]

    def local(tokens_x, context, cot_out, *shards):
        samples, tokens, width = tokens_x.shape
        blocks = shards[0].shape[0]
        spare = -shards[-1].shape[1] % LANES
        padded = shards[:-1] + (jnp.pad(shards[-1], ((0, 0), (0, spare))),)
        raws = [shard.reshape(blocks, -1, LANES).swapaxes(0, 1) for shard in padded]
        raws = [raw.reshape(-1, LANES) for raw in raws[:-1]] + raws[-1:]
        saved, ctx_rows, out_tokens = forward(tokens_x, context, raws, blocks)
        grad_x, sums, layout = backward(cot_out.reshape(samples * tokens, width), ctx_rows, saved, tokens,
                                        context.shape[1], samples * n_dev)
        shapes = [raw.shape for raw in raws[:-1]] + [shards[-1].shape]
        *grads, vec, grad_x, out_tokens = deliver(sums, grad_x, out_tokens, shapes,
                                                  (width, context.shape[2], blocks, layout))
        grads = [grad.reshape(-1, blocks, LANES).swapaxes(0, 1).reshape(blocks, -1) for grad in grads] + [vec]
        return (out_tokens.reshape(tokens_x.shape), grad_x.reshape(tokens_x.shape), *grads)

    param_spec = P(None, AXIS)
    in_specs = (P(AXIS), P(AXIS), P(AXIS)) + (param_spec,) * 8
    out_specs = (P(AXIS), P(AXIS)) + (param_spec,) * 8
    return jax.shard_map(local, mesh=mesh, in_specs=in_specs, out_specs=out_specs, check_vma=False)
```

```python
import functools
import math
from typing import Any, NamedTuple
import jax
import jax.numpy as jnp
from jax import lax
from jax.experimental import pallas as pl
from jax.experimental.pallas import tpu as pltpu
from jax.sharding import PartitionSpec as P

AXIS = 'fsdp'
HEAD = 64
EPS = 1e-5
SHARDS = 16
CUBE = (2, 2, 2, 2)
WEIGHT = (8, 4, 2, 1)
CHIP_WEIGHT = WEIGHT[1:]
CHIPS = 8
SUB = 8
FULL = slice(None)
SELF_ROWS, CROSS_ROWS = (0, 1, 6), (2, 3, 7)
F32 = jnp.float32
BF16 = jnp.bfloat16
LANES = 128
VMEM_BYTES = 63 * 2 ** 20
BELL = (2 * math.pi) ** -0.5
LN_ROWS = 128
PAIR_ROWS = 512
FF_ROWS = 256
FF_PART = 160
FF_SUB = 32
FF_COLS = 256

TAIL_C = 3.3
TAIL = (0.398796301085, 1.32638029784, 3.66563581228, 14.7229083576, -17.4165998636, 251.026512347, -660.864693498,
        511.950585826)
HALF_LOG2E = 0.5 * math.log2(math.e)


def mm(lhs, rhs):
    return jnp.dot(lhs, rhs, preferred_element_type=F32)


def mm_nt(lhs, rhs):
    return lax.dot_general(lhs, rhs, (((1,), (1,)), ((), ())), preferred_element_type=F32)


def mm_tn(lhs, rhs):
    return lax.dot_general(lhs, rhs, (((0,), (0,)), ((), ())), preferred_element_type=F32)


pipeline = functools.partial(pltpu.emit_pipeline, _explicit_indices=True)


def lane_mean(x):
    return jnp.mean(x, axis=-1, keepdims=True)


def lane_sum(x):
    return jnp.sum(x, axis=-1, keepdims=True)


def row_sum(x):
    return jnp.sum(x, axis=0, keepdims=True)


def line(ref, index):
    return ref[index:index + 1]


def add_line(ref, index, values):
    ref[index:index + 1] += values


def span(index, size):
    return pl.ds(pl.multiple_of(index * size, size), size)


def pieces_of(first, size):
    return [pl.ds(pl.multiple_of(first + piece * LN_ROWS, LN_ROWS), LN_ROWS) for piece in range(size // LN_ROWS)]


def lanes(tile):
    return slice(tile * LANES, (tile + 1) * LANES)


def repeat(count, body):
    def one(index, carry):
        body(index)
        return carry

    lax.fori_loop(0, count, one, 0)


def normalize(x):
    centered = x - lane_mean(x)
    scale = lax.rsqrt(lane_mean(centered * centered) + EPS)
    return centered * scale, scale


def norm_back(x, d_norm, gain):
    hat, scale = normalize(x)
    d_hat = d_norm * gain
    pulled = d_hat - lane_mean(d_hat) - hat * lane_mean(d_hat * hat)
    return pulled * scale, row_sum(d_norm * hat), row_sum(d_norm)


def low_half(rows):
    return lax.broadcasted_iota(jnp.int32, (rows, LANES), 1) < HEAD


def head_stack(pair, low):
    zero = jnp.zeros_like(pair)
    return jnp.concatenate([jnp.where(low, pair, zero), jnp.where(low, zero, pair)], axis=0)


def head_unstack(stacked, low):
    half = stacked.shape[0] // 2
    return jnp.where(low, stacked[:half], stacked[half:])


def softmax_halves(scores, valid):
    half = scores.shape[0] // 2
    parts = []
    for part in (scores[:half], scores[half:]):
        if valid < half:
            part = jnp.where(lax.broadcasted_iota(jnp.int32, part.shape, 0) < valid, part, -jnp.inf)
        part = jnp.exp(part - jnp.max(part, axis=0, keepdims=True))
        parts.append(part * (1.0 / row_sum(part)))
    return parts


def stack_bf16(parts):
    return jnp.concatenate([part.astype(BF16) for part in parts], axis=0)


def rows_at(number):
    return slice(number * FF_ROWS, (number + 1) * FF_ROWS)


def ahead(count, first, second, third=None):
    ready = first(0)
    for index in range(count):
        now = ready
        if index + 1 < count:
            ready = first(index + 1)
        second(index, now)
        if third and index:
            third(index - 1)
    if third:
        third(count - 1)


def scaled(query):
    return query * BF16(HEAD ** -0.5)


def pair_scores(query, keys):
    return mm_nt(head_stack(keys, low_half(keys.shape[0])), scaled(query))


def pair_forward(scores, values, valid):
    probs = stack_bf16(softmax_halves(scores, valid))
    return mm_tn(head_stack(values, low_half(values.shape[0])), probs).astype(BF16).T


def pair_backward_scores(query, keys, values, d_out):
    low = low_half(keys.shape[0])
    return mm_nt(head_stack(keys, low), scaled(query)), mm_nt(head_stack(values, low), d_out)


def pair_backward(scores, d_probs, query, keys, d_out, valid):
    low = low_half(keys.shape[0])
    half = keys.shape[0]
    parts = softmax_halves(scores, valid)
    d_values = head_unstack(mm(stack_bf16(parts), d_out), low).astype(BF16)
    d_scores = []
    for part, d_part in zip(parts, (d_probs[:half], d_probs[half:])):
        d_scores.append(part * (d_part - row_sum(part * d_part)))
    d_scores = stack_bf16(d_scores)
    d_query = (mm_tn(head_stack(keys, low), d_scores) * HEAD ** -0.5).astype(BF16).T
    return d_query, head_unstack(mm(d_scores, scaled(query)), low).astype(BF16), d_values


def normal_cdf(u):
    inverse = 1.0 / (TAIL_C + jnp.abs(u))
    poly = TAIL[-1]
    for coef in TAIL[-2::-1]:
        poly = poly * inverse + coef
    bell = jnp.exp2(u * u * -HALF_LOG2E)
    tail = bell * (inverse * poly)
    return jnp.where(u >= 0, 1.0 - tail, tail), bell


UNIT = 80
COLORS = 3
MACRO = COLORS * UNIT
SLOTS = 3
STREAMS = 2
STAGES = 4
CORE = 3
ORDERS = ((2, 1, 0), (1, 0, 2), (0, 2, 1))
MESH = pl.DeviceIdType.MESH


def bits_of(device):
    return [lax.rem(lax.div(device, weight), 2) for weight in WEIGHT]


class Place:
    def __init__(self):
        me = lax.axis_index(AXIS)
        self.bits = bits_of(me)
        self.others = [1 - bit for bit in self.bits]
        self.devices = [(me + (other - bit) * weight,) for bit, other, weight in zip(self.bits, self.others, WEIGHT)]

    def rows_of(self, ref, first, rows):
        half = ref.shape[CORE] // 2
        return pl.ds(pl.multiple_of(self.bits[CORE] * half + first, SUB), rows)

    def own(self, ref):
        return ref.at[(*self.bits[:CORE], self.rows_of(ref, 0, ref.shape[CORE] // 2))]

    def entry_barrier(self):
        barrier = pltpu.get_barrier_semaphore()
        for device in self.devices:
            pl.semaphore_signal(barrier, inc=1, device_id=device, device_id_type=MESH)
        pl.semaphore_wait(barrier, 4)


def pick(ref, lead, dim, value):
    return ref.at[(lead,) + (FULL,) * dim + (value,)]


class At(NamedTuple):
    stream: Any
    index: Any
    row: Any


class Reducer:
    def __init__(self, place, macros, scale, grads, out, refs):
        self.place, self.macros, self.scale, self.grads, self.out = place, macros, scale, grads, out
        self.own, self.held = refs[0], refs[1:1 + STAGES]
        self.send, self.recv, self.load = refs[1 + STAGES:]

    @staticmethod
    def scratch():
        held = [pltpu.VMEM((STREAMS * SLOTS * COLORS,) + (2,) * (3 - stage) + (UNIT, LANES), F32) for stage in range(STAGES)]
        sems = [pltpu.SemaphoreType.DMA((STREAMS, COLORS, STAGES)), pltpu.SemaphoreType.DMA((STREAMS * SLOTS * COLORS, STAGES)),
                pltpu.SemaphoreType.DMA((STREAMS, COLORS))]
        return [pltpu.VMEM((STREAMS * COLORS, *CUBE[1:], UNIT, LANES), F32)] + held + sems

    def axis(self, color, stage):
        return CORE if stage == 0 else ORDERS[color][stage - 1]

    def dim(self, color, stage):
        gone = ORDERS[color][:stage - 1]
        return sum(1 for axis in range(ORDERS[color][stage - 1]) if axis not in gone)

    def copy(self, at, color, stage):
        axis = self.axis(color, stage)
        other = self.place.others[axis]
        index = at.index + color
        if stage == 0:
            source = self.grads.at[:, :, :, other, pl.ds(at.row + color * UNIT, UNIT)]
        else:
            source = pick(self.held[stage - 1], index, self.dim(color, stage), other)
        return pltpu.make_async_remote_copy(
            src_ref=source, dst_ref=self.held[stage].at[index], send_sem=self.send.at[at.stream, color, stage],
            recv_sem=self.recv.at[index, stage], device_id=self.place.devices[axis], device_id_type=MESH)

    def own_copy(self, at, color):
        return pltpu.make_async_copy(self.grads.at[:, :, :, self.place.bits[CORE], pl.ds(at.row + color * UNIT, UNIT)],
                                     self.own.at[at.stream * COLORS + color], self.load.at[at.stream, color])

    def add(self, at, color, stage):
        index = at.index + color
        if stage == 0:
            self.held[0][index] += self.own[at.stream * COLORS + color]
            return
        mine = self.held[stage - 1][(index,) + (FULL,) * self.dim(color, stage)
                                    + (self.place.bits[self.axis(color, stage)],)]
        if stage < STAGES - 1:
            self.held[stage][index] += mine
        else:
            self.out[pl.ds(at.row + color * UNIT, UNIT)] = (self.held[stage][index] + mine) * self.scale

    def step(self, t):
        stream, tau = lax.rem(t, STREAMS), lax.div(t, STREAMS)

        def when_live(local, body):
            @pl.when((local >= 0) & (local * STREAMS + stream < self.macros))
            def _():
                body(At(stream, (stream * SLOTS + lax.rem(local, SLOTS)) * COLORS,
                        pl.multiple_of((local * STREAMS + stream) * MACRO, SUB)))

        def take(stage, at):
            for color in range(COLORS):
                copy = self.copy(at, color, stage)
                copy.wait_send()
                copy.wait_recv()
                if stage == 0:
                    self.own_copy(at, color).wait()
            for color in range(COLORS):
                self.add(at, color, stage)

        def give(stage, at):
            for color in range(COLORS):
                self.copy(at, color, stage).start()
                if stage == 0:
                    self.own_copy(at, color).start()

        for stage in reversed(range(STAGES)):
            when_live(tau - 1 - stage, functools.partial(take, stage))
        for stage in range(STAGES):
            when_live(tau - stage, functools.partial(give, stage))

    def beside(self, index, counts, start):
        number, first = 0, start
        for site, digit in enumerate(map(int, counts)):
            if digit:
                number += jnp.where(index == site, digit, 0)
                first += jnp.where(index > site, digit, 0)
        if start < start + sum(map(int, counts)):
            lax.fori_loop(0, number, lambda step, carry: (self.step(first + step), carry)[1], 0)


class Piece(NamedTuple):
    ref: Any
    first: Any
    rows: Any
    cols: Any
    color: int
    number: int


class Gatherer:
    def __init__(self, place, macros, send, recv):
        self.place, self.send, self.recv = place, send, recv
        self.jobs = {}
        number = 0
        for index, macro in enumerate(macros):
            first, gap = (0, 1) if index < 2 else (index - 1, 2)
            pieces = []
            for ref, color, row, rows, cols in macro:
                pieces.append(Piece(ref, row, rows, cols, color, number))
                number += 1
            for stage in range(STAGES + 1):
                self.jobs.setdefault(first + gap * stage, []).append((stage, pieces))

    def copy(self, piece, stage):
        order = ORDERS[piece.color]
        index = [FULL if axis in order[:stage] else self.place.bits[axis] for axis in range(CORE)]
        block = piece.ref.at[(*index, self.place.rows_of(piece.ref, piece.first, piece.rows), piece.cols)]
        axis = order[stage] if stage < CORE else CORE
        return pltpu.make_async_remote_copy(
            src_ref=block, dst_ref=block, send_sem=self.send.at[piece.number, stage],
            recv_sem=self.recv.at[piece.number, stage], device_id=self.place.devices[axis], device_id_type=MESH)

    def step(self, t):
        for stage, pieces in self.jobs[t]:
            if stage:
                for piece in pieces:
                    copy = self.copy(piece, stage - 1)
                    copy.wait_send()
                    copy.wait_recv()
            if stage < STAGES:
                for piece in pieces:
                    self.copy(piece, stage).start()

    def beside(self, index, part, sites, offset=0):
        first, count = sum(FORWARD_STEPS[:part]), FORWARD_STEPS[part]
        for number in range(count):
            site = (number + 1) * sites // count - 1 if count <= sites else number * sites // count

            @pl.when(index == offset + site)
            def _(number=number):
                self.step(first + number)


def thirds(tiles):
    edges = [round(tiles * part / 3) * LANES for part in range(4)]
    return [slice(first, last) for first, last in zip(edges[:-1], edges[1:])]


FORWARD_STEPS = (7, 7, 4, 3, 3, 4, 3, 2, 0)
MATS = ('qkv', 'out', 'q2', 'kv2', 'out2', 'ff1', 'ff2')
WEIGHTS = ('w_a', 'w_b', 'w_kv2', 'w_ff1', 'w_ff2')
KEPT = ('h', 'h1', 'h2', 'qkv', 'out1', 'q', 'kv', 'out2', 'fa', 'fg', 'z', 'rows')


def load(source, target, sem):
    copy = pltpu.make_async_copy(source, target, sem)
    copy.start()
    return copy


def fetch(source, cols, target, sems, into=FULL):
    def copy(shard):
        index = [lax.rem(lax.div(shard, weight), 2) for weight in CHIP_WEIGHT]
        return pltpu.make_async_copy(source.at[(*index, FULL, cols)], target.at[span(shard, source.shape[CORE]), into],
                                     sems.at[shard])

    repeat(CHIPS, lambda shard: copy(shard).start())
    return lambda: repeat(CHIPS, lambda shard: copy(shard).wait())


def macro_list(weights, vec):
    macros = []
    for block in weights:
        high = {name: block[name].shape[CORE] // 2 for name in WEIGHTS}
        def add(name, row, rows, first, cols):
            parts = thirds(cols // LANES)
            macros.append([(block[name], color, row, rows, pl.ds(first + part.start, part.stop - part.start))
                           for color, part in enumerate(parts[len(macros) % COLORS:] + parts[:len(macros) % COLORS])])

        wide = block['w_a'].shape[-1] // 2
        for part in range(2):
            add('w_a', 0, high['w_a'], part * wide, wide)
        quarter = high['w_kv2'] // 4
        for part in range(4):
            add('w_kv2', part * quarter, quarter, 0, wide)
        add('w_b', 0, high['w_b'], 0, wide)
        tenth = high['w_ff2'] // 20
        for part in range(2):
            macros.append([(block['w_ff2'], color, (part * 10 + row) * tenth, rows * tenth, FULL)
                           for color, row, rows in zip(range(COLORS), (0, 3, 7), (3, 4, 3))])
        inner = block['w_ff1'].shape[-1] // 2
        for part in range(2):
            for half in range(2):
                add('w_ff1', 0, high['w_ff1'], half * inner + part * inner // 2, inner // 2)
    macros[0].append((vec, 0, 0, vec.shape[CORE] // 2, FULL))
    return macros


def forward_kernel(cfg, *refs):
    tokens, width, blocks, per_vec = cfg
    heads = width // HEAD
    tiles = width // LANES
    tokens_ref, context_ref = refs[:2]
    raw_refs = refs[2:2 + len(MATS) + 1]
    refs = refs[2 + len(raw_refs):]
    kept = [dict(zip(KEPT, refs[layer * len(KEPT):])) for layer in range(blocks)]
    refs = refs[blocks * len(KEPT):]
    weights = [dict(zip(WEIGHTS, refs[layer * len(WEIGHTS):])) for layer in range(blocks)]
    refs = refs[blocks * len(WEIGHTS):]
    vec_all_ref, ctx_out_ref, tokens_out_ref, hidden, context, rows_ref, vec_ref, sems, send, recv = refs
    samples, ctx_len = context_ref.shape[:2]
    pad = context.shape[0] // samples
    count = tokens_ref.shape[0]
    chunk = PAIR_ROWS
    per_step = chunk // tokens
    place = Place()
    gatherer = Gatherer(place, macro_list(weights, vec_all_ref), send, recv)

    def each_piece(body):
        repeat(count // chunk, lambda index: [body(at) for at in pieces_of(index * chunk, chunk)])

    def startup(image, wide, flat, vec_piece, raws, pieces, raw_sems, own_sems):
        first = [load(tokens_ref, image, sems.at[0]), load(context_ref, wide, sems.at[1])]
        loads = [load(source, target, raw_sems.at[index])
                 for index, (source, target) in enumerate(zip(raw_refs, raws))]

        def tile(layer, name, target, first_col):
            raw = raws[MATS.index(name)]
            flat[:raw.shape[0]] = raw[:].astype(F32)
            rows = target.shape[0]
            stride = raw.shape[0] // rows
            for index in range(stride // blocks):
                at = first_col + index * LANES
                target[:, at:at + LANES] = flat[pl.ds(index * blocks + layer, rows, stride=stride)].astype(BF16)

        def own(layer, name):
            number = layer * len(WEIGHTS) + WEIGHTS.index(name)
            return load(pieces[number], place.own(weights[layer][name]), own_sems.at[number])

        def prepare(layer, name):
            target = pieces[layer * len(WEIGHTS) + WEIGHTS.index(name)]
            if name == 'w_a':
                tile(layer, 'qkv', target, 0)
                tile(layer, 'out', target, 3 * width)
            elif name == 'w_b':
                tile(layer, 'q2', target, 0)
                tile(layer, 'out2', target, width)
            else:
                tile(layer, name[2:], target, 0)
            return own(layer, name)

        for copy in loads:
            copy.wait()
        vec_piece[:] = jnp.zeros_like(vec_piece)
        for layer in range(blocks):
            flat[:per_vec] = raws[-1][:, layer].astype(F32)
            vec_piece[layer * SUB:layer * SUB + per_vec] = flat[:per_vec].astype(BF16)
        pending = [prepare(0, 'w_a'), load(vec_piece, place.own(vec_all_ref), sems.at[2])]
        place.entry_barrier()
        later = [[(0, 'w_kv2')], [(0, 'w_b'), (0, 'w_ff2')], [(0, 'w_ff1')], [(1, name) for name in WEIGHTS[:CORE]],
                 [(1, name) for name in WEIGHTS[CORE:]]]
        for t, jobs in enumerate(later):
            for copy in pending:
                copy.wait()
            gatherer.step(t)
            pending = [prepare(layer, name) for layer, name in jobs if layer < blocks]
        for copy in first:
            copy.wait()
        each_piece(lambda at: hidden.at[0].__setitem__(at, image[at].astype(F32)))
        context[:] = jnp.zeros_like(context)
        for sample in range(samples):
            context[sample * pad:sample * pad + ctx_len] = wide[sample]
        for copy in pending:
            copy.wait()
        for t in range(len(later), FORWARD_STEPS[0]):
            gatherer.step(t)

    def raw_shape(index):
        return pltpu.VMEM(raw_refs[index].shape, BF16)

    pl.run_scoped(startup, pltpu.VMEM(tokens_ref.shape, BF16), pltpu.VMEM(context_ref.shape, BF16),
                  pltpu.VMEM((max(ref.shape[0] for ref in raw_refs), LANES), F32), pltpu.VMEM((blocks * SUB, LANES), BF16),
                  [raw_shape(index) for index in range(len(raw_refs))],
                  [pltpu.VMEM((block[name].shape[CORE] // 2, block[name].shape[-1]), BF16)
                   for block in weights for name in WEIGHTS],
                  pltpu.SemaphoreType.DMA((len(raw_refs),)), pltpu.SemaphoreType.DMA((blocks * len(WEIGHTS),)))
    ctx_copy = load(context, ctx_out_ref, sems.at[3])

    def unpack(parts, sem):
        load(vec_all_ref, parts, sem).wait()
        vec_ref[:] = jnp.zeros_like(vec_ref)
        rows_ref[:] = jnp.zeros_like(rows_ref)
        lane = lax.broadcasted_iota(jnp.int32, (SUB, LANES), 1)
        per_device = 17 * width // SHARDS
        for layer in range(blocks):
            vec = vec_ref.at[layer]
            for shard in range(SHARDS):
                chip, core = divmod(shard, 2)
                bits = [chip // weight % 2 for weight in CHIP_WEIGHT]
                part = parts[(*bits, pl.ds((core * blocks + layer) * SUB, SUB))].astype(F32)
                row, off = divmod(shard * per_device, LANES)
                if off:
                    part = pltpu.roll(part, off, 1)
                    vec[pl.ds(row + 1, SUB)] += jnp.where(lane < off, part, 0.0)
                vec[pl.ds(row, SUB)] += jnp.where(lane >= off, part, 0.0)
            for row in range(9):
                for tile in range(tiles):
                    rows_ref[layer, row:row + 1, lanes(tile)] = line(vec, row * tiles + tile)

    pl.run_scoped(unpack, pltpu.VMEM(vec_all_ref.shape, BF16), pltpu.SemaphoreType.DMA)
    rows_copies = [load(rows_ref.at[layer], kept[layer]['rows'], sems.at[4 + layer]) for layer in range(blocks)]

    def attention(layer, source, target, cross, part):
        rows = rows_ref.at[layer]
        packed = weights[layer]['w_b' if cross else 'w_a']
        inner = packed.shape[-1] - width
        gain, shift, bias = CROSS_ROWS if cross else SELF_ROWS

        def scoped(norm, w_in, w_out, w_kv, kv, in_sems):
            waits = [fetch(packed, pl.ds(0, inner), w_in, in_sems.at[0]), fetch(packed, pl.ds(inner, width), w_out, in_sems.at[1])]
            if cross:
                fetch(weights[layer]['w_kv2'], FULL, w_kv, in_sems.at[2])()
                kv[:] = mm(context[:], w_kv[:]).astype(BF16)
                kv_copy = load(kv, kept[layer]['kv'], in_sems.at[2, 0])
            for wait in waits:
                wait()

            def body(idx, qkv, mixed):
                step = idx.index[0]
                at_rows = span(step, chunk)
                for at, here in zip(pieces_of(step * chunk, chunk), pieces_of(0, chunk)):
                    hat, unused = normalize(source[at])
                    norm[here] = (hat * line(rows, gain) + line(rows, shift)).astype(BF16)
                qkv[:] = mm(norm[:], w_in[:]).astype(BF16)

                def sample(number):
                    at = span(number, tokens)
                    index = step * per_step + number
                    kv_at = span(index, pad) if cross else at
                    k_ref, k_first, limit = (kv, 0, ctx_len) if cross else (qkv, width, tokens)

                    def scores(pair):
                        return pair_scores(qkv[at, lanes(pair)], k_ref[kv_at, lanes(pair + k_first // LANES)])

                    def rest(pair, ready):
                        values = k_ref[kv_at, lanes(pair + (k_first + width) // LANES)]
                        mixed[at, lanes(pair)] = pair_forward(ready, values, limit)

                    ahead(heads // 2, scores, rest)
                    gatherer.beside(index, part, samples)

                repeat(per_step, sample)
                target[at_rows] = source[at_rows] + mm(mixed[:], w_out[:]) + line(rows, bias)

            block = lambda cols: pl.BlockSpec((chunk, cols), lambda step: (step, 0))
            pipeline(body, grid=(count // chunk,), out_specs=[block(inner), block(width)])(
                kept[layer]['q' if cross else 'qkv'], kept[layer]['out2' if cross else 'out1'])
            if cross:
                kv_copy.wait()

        small = pltpu.VMEM((SUB, LANES), BF16)
        pl.run_scoped(scoped, pltpu.VMEM((chunk, width), BF16), pltpu.VMEM((width, inner), BF16),
                      pltpu.VMEM((width, width), BF16), pltpu.VMEM((context_ref.shape[2], 2 * width), BF16) if cross else small,
                      pltpu.VMEM((samples * pad, 2 * width), BF16) if cross else small, pltpu.SemaphoreType.DMA((3, CHIPS)))

    def feed_forward(layer, source, target, part):
        rows = rows_ref.at[layer]
        vec = vec_ref.at[layer]
        inner = weights[layer]['w_ff1'].shape[-1] // 2
        steps = inner // FF_COLS
        wide = FF_COLS // LANES

        def scoped(norm, w1, w2, w_sems):
            def fetch_half(part):
                both = [pl.ds(half * inner + part * inner // 2, inner // 2) for half in range(2)]
                return [fetch(weights[layer]['w_ff1'], cols, w1, w_sems.at[half], cols) for half, cols in enumerate(both)]

            waits = fetch_half(0) + [fetch(weights[layer]['w_ff2'], FULL, w2, w_sems.at[2])]

            def begin(at):
                hat, unused = normalize(source[at])
                norm[at] = (hat * line(rows, 4) + line(rows, 5)).astype(BF16)
                target[at] = source[at] + line(rows, SUB)

            each_piece(begin)
            for wait in waits:
                wait()

            def body(idx, fa, fg, z):
                step = idx.index[0]
                cols, gate_cols = span(step, FF_COLS), span(step + steps, FF_COLS)

                @pl.when(step == steps // 2)
                def _():
                    for wait in fetch_half(1):
                        wait()

                def bias(half):
                    first = 9 * tiles + (half * steps + step) * wide
                    return jnp.concatenate([vec[pl.ds(first + index, 1)] for index in range(wide)], axis=1)

                bias_a, bias_g = bias(0), bias(1)

                def hidden_of(number):
                    normed = norm[rows_at(number)]
                    return mm(normed, w1[:, gate_cols]) + bias_g, mm(normed, w1[:, cols]) + bias_a

                def rest(number, ready):
                    at = rows_at(number)
                    gate, value = ready
                    cdf, bell = normal_cdf(gate)
                    factor = gate * cdf
                    z[at] = (value * factor).astype(BF16)
                    fa[at] = factor
                    fg[at] = value * (cdf + gate * bell * BELL)

                def project(number):
                    target[rows_at(number)] += mm(z[rows_at(number)], w2[cols])

                ahead(count // FF_ROWS, hidden_of, rest, project)
                for half in range(2):
                    gatherer.beside(step, part + half, steps // 2, half * steps // 2)

            block = ff_block(count)
            pipeline(body, grid=(steps,), out_specs=[block, block, block])(
                kept[layer]['fa'], kept[layer]['fg'], kept[layer]['z'])

        pl.run_scoped(scoped, pltpu.VMEM((count, width), BF16), pltpu.VMEM((width, 2 * inner), BF16),
                      pltpu.VMEM((inner, width), BF16), pltpu.SemaphoreType.DMA((3, CHIPS)))

    phases = 3 * blocks
    saves = [load(hidden.at[0], kept[0]['h'], sems.at[6]), None]
    for phase in range(phases):
        layer, kind = divmod(phase, 3)
        source, target = hidden.at[phase % 2], hidden.at[(phase + 1) % 2]
        other = (phase + 1) % 2
        if saves[other] is not None:
            saves[other].wait()
        if kind < 2:
            attention(layer, source, target, kind == 1, 1 + 4 * layer + kind)
        else:
            feed_forward(layer, source, target, 1 + 4 * layer + kind)
        following = divmod(phase + 1, 3)
        saves[other] = None
        if phase + 1 < phases:
            saves[other] = load(target, kept[following[0]][KEPT[following[1]]], sems.at[6 + other])

    def finish(image):
        each_piece(lambda at: image.__setitem__(at, hidden[phases % 2, at].astype(BF16)))
        load(image, tokens_out_ref, sems.at[0]).wait()

    pl.run_scoped(finish, pltpu.VMEM(tokens_ref.shape, BF16))
    for copy in [copy for copy in saves if copy is not None] + [ctx_copy] + rows_copies:
        copy.wait()


def settings(number):
    return dict(compiler_params=pltpu.CompilerParams(collective_id=number, has_side_effects=True,
                                                     vmem_limit_bytes=VMEM_BYTES),
                cost_estimate=pl.CostEstimate(flops=10 ** 11, bytes_accessed=10 ** 8, transcendentals=0))


def ff_block(count):
    return pl.BlockSpec((None, count, FF_COLS), lambda step: (step, 0, 0))


def any_specs(count):
    return [pl.BlockSpec(memory_space=pl.ANY)] * count


def forward(tokens_x, context, raws, blocks):
    samples, tokens, width = tokens_x.shape
    ctx_width = context.shape[2]
    count, inner = samples * tokens, 4 * width
    pad = -(-context.shape[1] // SHARDS) * SHARDS
    steps = inner // FF_COLS
    plain = jax.ShapeDtypeStruct((count, width), F32)
    half = jax.ShapeDtypeStruct((count, width), BF16)
    wide = jax.ShapeDtypeStruct((steps, count, FF_COLS), F32)
    kept = [plain, plain, plain, jax.ShapeDtypeStruct((count, 3 * width), BF16), half, half,
            jax.ShapeDtypeStruct((samples * pad, 2 * width), BF16), half, wide, wide,
            jax.ShapeDtypeStruct(wide.shape, BF16), jax.ShapeDtypeStruct((SHARDS, width), F32)]
    whole_of = lambda rows, cols: jax.ShapeDtypeStruct((*CUBE[:CORE], rows // CHIPS, cols), BF16)
    weights = [whole_of(width, 4 * width), whole_of(width, 2 * width), whole_of(ctx_width, 2 * width),
               whole_of(width, 2 * inner), whole_of(inner, width)]
    extra = [whole_of(SHARDS * blocks * SUB, LANES), jax.ShapeDtypeStruct((samples * pad, ctx_width), BF16), half]
    shapes = kept * blocks + weights * blocks + extra
    pieces = 1 + COLORS * 13 * blocks
    outs = pl.pallas_call(
        functools.partial(forward_kernel, (tokens, width, blocks, raws[-1].shape[0])),
        in_specs=any_specs(2 + len(raws)), out_specs=any_specs(len(shapes)), out_shape=shapes,
        scratch_shapes=[pltpu.VMEM((2, count, width), F32), pltpu.VMEM((samples * pad, ctx_width), BF16),
                        pltpu.VMEM((blocks, SHARDS, width), F32), pltpu.VMEM((blocks, 96, LANES), F32),
                        pltpu.SemaphoreType.DMA((8,)), pltpu.SemaphoreType.DMA((pieces, STAGES)),
                        pltpu.SemaphoreType.DMA((pieces, STAGES))],
        name='forward', **settings(1),
    )(tokens_x.reshape(count, width), context, *raws)
    kept_of = [outs[layer * len(kept):(layer + 1) * len(kept)] for layer in range(blocks)]
    outs = outs[blocks * len(kept):]
    weights_of = [[whole.reshape(-1, whole.shape[-1]) for whole in outs[layer * len(weights):(layer + 1) * len(weights)]]
                  for layer in range(blocks)]
    saved = [dict(zip(KEPT + WEIGHTS, list(one) + list(two))) for one, two in zip(kept_of, weights_of)]
    return saved, outs[-2], outs[-1]


def view(values, *lead):
    return values.reshape(CUBE + lead + (LANES,))


def put_tiles(stage, values, first=0):
    rows = values.shape[0] // SHARDS
    for tile in range(values.shape[1] // LANES):
        at = first + tile * rows
        stage[:, :, :, :, at:at + rows] = view(values[:, lanes(tile)], rows)


class Layout:
    def __init__(self, width, ctx_width, blocks):
        unit = width // SHARDS * (width // LANES)
        self.ff1, self.ff2 = 0, 8 * unit
        self.q2 = 12 * unit
        self.out2 = self.q2 + unit
        self.kv2 = self.out2 + unit
        self.out = self.kv2 + ctx_width // SHARDS * (2 * width // LANES)
        self.qkv = self.out + unit
        self.block = self.qkv + 3 * unit
        self.vec = blocks * self.block
        self.vec_rows = -(-17 * width // SHARDS // LANES // SUB) * SUB
        used = self.vec + blocks * self.vec_rows
        self.macros = -(-used // MACRO)
        self.pad = self.macros * MACRO - used
        self.rows = self.macros * MACRO


NAMES = KEPT + WEIGHTS


def backward_kernel(cfg, *refs):
    tokens, ctx_len, width, blocks, layout, total, plan = cfg
    heads = width // HEAD
    cot_ref, context_ref = refs[:2]
    saved = [dict(zip(NAMES, refs[2 + layer * len(NAMES):])) for layer in range(blocks)]
    refs = refs[2 + blocks * len(NAMES):]
    gx_ref, grads_ref, sum_ref = refs[:3]
    refs = refs[3:]
    grad_ref, hidden_ref, rows_ref, d_rows_ref, vec_ref, out_ref, in_sems = refs[:7]
    place = Place()
    reducer = Reducer(place, layout.macros, 1.0 / total, grads_ref, out_ref, refs[7:])
    count = grad_ref.shape[0]
    chunk = PAIR_ROWS
    chunks = count // chunk
    phases = [(layer, kind) for layer in reversed(range(blocks)) for kind in ('h2', 'h1', 'h')]

    def hidden_copy(index):
        layer, kind = phases[index]
        return pltpu.make_async_copy(saved[layer][kind], hidden_ref.at[index % 2], in_sems.at[index % 2])

    def rows_copy(layer):
        return pltpu.make_async_copy(saved[layer]['rows'], rows_ref.at[layer], in_sems.at[2 + layer])

    def base(layer):
        return (blocks - 1 - layer) * layout.block

    def region(row, size):
        return grads_ref.at[:, :, :, :, pl.ds(pl.multiple_of(row, SUB), size)]

    def each_piece(body):
        repeat(chunks, lambda index: [body(at) for at in pieces_of(index * chunk, chunk)])

    def ff_phase(layer, index, first):
        hidden = hidden_ref.at[index % 2]
        rows = rows_ref.at[layer]
        d_rows = d_rows_ref.at[layer]
        vec = vec_ref.at[layer]
        src = saved[layer]
        w1_all, w2_all = src['w_ff1'], src['w_ff2']
        inner = w2_all.shape[0]
        steps = inner // FF_COLS
        start, counts = first

        def scoped(norm_t, grad_bf, du, w1, acc, stage1, stage2, sem1, sem2):
            def begin(at):
                hat, unused = normalize(hidden[at])
                norm_t[:, at] = (hat * line(rows, 4) + line(rows, 5)).astype(BF16).T
                grad_bf[at] = grad_ref[at].astype(BF16)
                add_line(d_rows, 8, row_sum(grad_ref[at]))
                acc[at] = jnp.zeros((LN_ROWS, width), F32)

            each_piece(begin)

            def copy1(step):
                return pltpu.make_async_copy(stage1, region(base(layer) + layout.ff1 + step * FF_PART, FF_PART), sem1)

            def copy2(step, part):
                block = step * 8 + part
                shard = lax.div(block, 5)
                row = pl.multiple_of(base(layer) + layout.ff2 + lax.rem(block, 5) * FF_PART, SUB)
                bits = bits_of(shard)
                return pltpu.make_async_copy(stage2.at[part], grads_ref.at[(*bits, pl.ds(row, FF_PART))], sem2.at[part])

            def wait(step):
                copy1(step).wait()
                for part in range(8):
                    copy2(step, part).wait()

            def body(idx, w1a, w1g, w2, fa, fg, z):
                step = idx.index[0]
                w1[:, :FF_COLS] = w1a[:]
                w1[:, FF_COLS:] = w1g[:]

                sums = [jnp.zeros((1, FF_COLS), F32)] * 2

                def d_gated(number):
                    return mm_nt(grad_bf[rows_at(number)], w2[:]).astype(BF16).astype(F32)

                def rest(number, dz):
                    at = rows_at(number)
                    for half, factor in enumerate((fa, fg)):
                        part = dz * factor[at]
                        du[at, half * FF_COLS:(half + 1) * FF_COLS] = part.astype(BF16)
                        sums[half] += row_sum(part)

                def project(number):
                    acc[rows_at(number)] += mm_nt(du[rows_at(number)], w1[:])

                ahead(count // FF_ROWS, d_gated, rest, project)
                for half in range(2):
                    for tile in range(2):
                        row = 9 * width // LANES + half * (inner // LANES) + 2 * step + tile
                        vec[pl.ds(row, 1)] = sums[half][:, lanes(tile)]

                @pl.when(step > 0)
                def _():
                    wait(step - 1)

                reducer.beside(step, counts, start)
                put_tiles(stage1, mm(norm_t[:], du[:, :FF_COLS]))
                put_tiles(stage1, mm(norm_t[:], du[:, FF_COLS:]), 80)
                d_w2 = mm_tn(z[:], grad_bf[:])
                for tile in range(width // LANES):
                    stage2[:, tile * FF_SUB:(tile + 1) * FF_SUB] = d_w2[:, lanes(tile)].reshape(8, FF_SUB, LANES)
                copy1(step).start()
                for number in range(8):
                    copy2(step, number).start()

            column = pl.BlockSpec((width, FF_COLS), lambda step: (0, step))
            kept = ff_block(count)
            pipeline(
                body, grid=(steps,),
                in_specs=[column, pl.BlockSpec((width, FF_COLS), lambda step: (0, step + steps)),
                          pl.BlockSpec((FF_COLS, width), lambda step: (step, 0)), kept, kept, kept],
            )(w1_all, w1_all, w2_all, src['fa'], src['fg'], src['z'])

            def finish(at):
                d_res, d_gain, d_shift = norm_back(hidden[at], acc[at], line(rows, 4))
                grad_ref[at] += d_res
                add_line(d_rows, 4, d_gain)
                add_line(d_rows, 5, d_shift)

            each_piece(finish)
            wait(steps - 1)

        pl.run_scoped(scoped, pltpu.VMEM((width, count), BF16), pltpu.VMEM((count, width), BF16),
                      pltpu.VMEM((count, 2 * FF_COLS), BF16), pltpu.VMEM((width, 2 * FF_COLS), BF16),
                      pltpu.VMEM((count, width), F32), pltpu.VMEM((*CUBE, FF_PART, LANES), F32),
                      pltpu.VMEM((8, FF_PART, LANES), F32), pltpu.SemaphoreType.DMA, pltpu.SemaphoreType.DMA((8,)))

    def attention_phase(layer, index, first, cross):
        hidden = hidden_ref.at[index % 2]
        rows = rows_ref.at[layer]
        d_rows = d_rows_ref.at[layer]
        src = saved[layer]
        packed = src['w_b' if cross else 'w_a']
        inner = packed.shape[1] - width
        steps = count // PAIR_ROWS
        per_step = PAIR_ROWS // tokens
        start, counts = first
        gain, shift, bias = CROSS_ROWS if cross else SELF_ROWS
        samples = count // tokens
        pad = context_ref.shape[0] // samples
        kv_rows_all = context_ref.shape[0] if cross else count

        def scoped(d_mix, d_q, d_kv, norm_t, d_wq, d_wout, stage, stage_out, sem, sem_out, w_in, w_out, in_sems_, context, kv, ctx_sems):
            if cross:
                loads = [pltpu.make_async_copy(context_ref, context, ctx_sems.at[0]),
                         pltpu.make_async_copy(src['kv'], kv, ctx_sems.at[1])]
                for copy in loads:
                    copy.start()
                d_wq[:] = jnp.zeros_like(d_wq)
                for copy in loads:
                    copy.wait()
            d_wout[:] = jnp.zeros_like(d_wout)
            for copy in [load(packed.at[:, pl.ds(0, inner)], w_in, in_sems_.at[0]),
                         load(packed.at[:, pl.ds(inner, width)], w_out, in_sems_.at[1])]:
                copy.wait()

            def body(idx, qkv, mixed):
                step = idx.index[0]
                at_rows = span(step, PAIR_ROWS)
                grad_bf = grad_ref[at_rows].astype(BF16)
                add_line(d_rows, bias, row_sum(grad_ref[at_rows]))
                d_wout[:] += mm_tn(mixed[:], grad_bf)
                d_mix[:] = mm_nt(grad_bf, w_out[:]).astype(BF16)

                def sample(number, carry):
                    at = span(number, tokens)
                    sample_index = step * per_step + number
                    if cross:
                        kv_at, d_q_at, k_ref, d_k_ref, k_first, limit = span(sample_index, pad), at, kv, d_kv, 0, ctx_len
                    else:
                        kv_at, d_q_at = at, span(sample_index, tokens)
                        k_ref, d_k_ref, k_first, limit = qkv, d_q, width, tokens
                    d_k_at = kv_at if cross else d_q_at

                    def operands(pair):
                        k_cols, v_cols = (lanes(pair + (k_first + more) // LANES) for more in (0, width))
                        return qkv[at, lanes(pair)], k_ref[kv_at, k_cols], k_ref[kv_at, v_cols], d_mix[at, lanes(pair)]

                    def scores(pair):
                        return pair_backward_scores(*operands(pair))

                    def rest(pair, ready):
                        query, keys, values, d_out = operands(pair)
                        d_query, d_keys, d_values = pair_backward(*ready, query, keys, d_out, limit)
                        d_q[d_q_at, lanes(pair)] = d_query
                        d_k_ref[d_k_at, lanes(pair + k_first // LANES)] = d_keys
                        d_k_ref[d_k_at, lanes(pair + (k_first + width) // LANES)] = d_values

                    ahead(heads // 2, scores, rest)

                    reducer.beside(sample_index, counts[:samples], start)
                    return carry

                lax.fori_loop(0, per_step, sample, 0)
                here_all = pieces_of(0, chunk)
                at_all = pieces_of(step * chunk, chunk)
                for at, here in zip(at_all, here_all):
                    hat, unused = normalize(hidden[at])
                    norm = (hat * line(rows, gain) + line(rows, shift)).astype(BF16)
                    if cross:
                        d_mix[here] = norm
                    else:
                        norm_t[:, at] = norm.T
                if cross:
                    d_wq[:] += mm_tn(d_mix[:], d_q[:])
                    d_norm = mm_nt(d_q[:], w_in[:])
                else:
                    d_norm = mm_nt(d_q[at_rows], w_in[:])
                for piece, at in enumerate(at_all):
                    d_res, d_gain, d_shift = norm_back(hidden[at], d_norm[piece * LN_ROWS:(piece + 1) * LN_ROWS], line(rows, gain))
                    grad_ref[at] += d_res
                    add_line(d_rows, gain, d_gain)
                    add_line(d_rows, shift, d_shift)

            block = lambda ref: pl.BlockSpec((PAIR_ROWS, ref.shape[1]), lambda step: (step, 0))
            operands = [src['q' if cross else 'qkv'], src['out2' if cross else 'out1']]
            pipeline(
                body, grid=(steps,), in_specs=[block(operands[0]), block(operands[1])],
            )(*operands)
            where = base(layer) + (layout.out2 if cross else layout.out)
            size = width // SHARDS * (width // LANES)
            if cross:
                put_tiles(stage_out, d_wq[:])
                put_tiles(stage_out, d_wout[:], size)
                copy_out = pltpu.make_async_copy(stage_out, region(base(layer) + layout.q2, 2 * size), sem_out)
            else:
                put_tiles(stage_out, d_wout[:])
                copy_out = pltpu.make_async_copy(stage_out, region(where, size), sem_out)
            copy_out.start()
            rows_each = stage.shape[4]
            cols_each = stage.shape[4] // ((context_ref.shape[1] if cross else width) // SHARDS) * LANES
            tails = (2 if cross else 3) * width // cols_each
            first_row = base(layer) + (layout.kv2 if cross else layout.qkv)

            def copy_tail(step):
                return pltpu.make_async_copy(stage, region(first_row + step * rows_each, rows_each), sem)

            def tail(step, carry):
                cols = span(step, cols_each)
                result = mm_tn(context[:], d_kv[:, cols]) if cross else mm(norm_t[:], d_q[:, cols])

                @pl.when(step > 0)
                def _():
                    copy_tail(step - 1).wait()

                @pl.when(step == 1)
                def _():
                    copy_out.wait()

                put_tiles(stage, result)
                copy_tail(step).start()
                reducer.beside(step, counts[samples:], start + sum(map(int, counts[:samples])))
                return carry

            lax.fori_loop(0, tails, tail, 0)
            copy_tail(tails - 1).wait()

        small = pltpu.VMEM((SUB, LANES), BF16)
        w_scratch = [pltpu.VMEM((width, inner), BF16), pltpu.VMEM((width, width), BF16), pltpu.SemaphoreType.DMA((2,))]
        size = width // SHARDS * (width // LANES)
        if cross:
            ctx_width = context_ref.shape[1]
            pl.run_scoped(scoped, pltpu.VMEM((PAIR_ROWS, width), BF16), pltpu.VMEM((PAIR_ROWS, width), BF16),
                          pltpu.VMEM((kv_rows_all, 2 * width), BF16), small, pltpu.VMEM((width, width), F32),
                          pltpu.VMEM((width, width), F32), pltpu.VMEM((*CUBE, ctx_width // SHARDS * 2, LANES), F32),
                          pltpu.VMEM((*CUBE, 2 * size, LANES), F32), pltpu.SemaphoreType.DMA,
                          pltpu.SemaphoreType.DMA, *w_scratch, pltpu.VMEM(context_ref.shape, BF16),
                          pltpu.VMEM(src['kv'].shape, BF16), pltpu.SemaphoreType.DMA((2,)))
        else:
            pl.run_scoped(scoped, pltpu.VMEM((PAIR_ROWS, width), BF16), pltpu.VMEM((count, 3 * width), BF16), small,
                          pltpu.VMEM((width, count), BF16), small, pltpu.VMEM((width, width), F32),
                          pltpu.VMEM((*CUBE, width // SHARDS * 3, LANES), F32),
                          pltpu.VMEM((*CUBE, size, LANES), F32), pltpu.SemaphoreType.DMA,
                          pltpu.SemaphoreType.DMA, *w_scratch, small, small, pltpu.SemaphoreType.DMA((2,)))

    place.entry_barrier()
    hidden_copy(0).start()
    for layer in range(blocks):
        rows_copy(layer).start()
    d_rows_ref[:] = jnp.zeros_like(d_rows_ref)
    vec_ref[:] = jnp.zeros_like(vec_ref)

    def load_cot(cot, sem):
        copy = pltpu.make_async_copy(cot_ref, cot, sem)
        copy.start()
        copy.wait()
        each_piece(lambda at: grad_ref.__setitem__(at, cot[at].astype(F32)))

    pl.run_scoped(load_cot, pltpu.VMEM(cot_ref.shape, BF16), pltpu.SemaphoreType.DMA)
    for layer in range(blocks):
        rows_copy(layer).wait()
    for index, (layer, kind) in enumerate(phases):
        hidden_copy(index).wait()
        if index + 1 < len(phases):
            hidden_copy(index + 1).start()
        if kind == 'h2':
            ff_phase(layer, index, plan[index])
        else:
            attention_phase(layer, index, plan[index], kind == 'h1')

    def finish(stage, sem, image, sem_image):
        def cast(at):
            image[at] = grad_ref[at].astype(BF16)

        each_piece(cast)
        copy_image = pltpu.make_async_copy(image, gx_ref, sem_image)
        copy_image.start()
        per_device = 17 * width // SHARDS
        stage[:] = jnp.zeros_like(stage)
        for layer in range(blocks):
            vec = vec_ref.at[layer]
            for row in range(9):
                for tile in range(width // LANES):
                    at = row * (width // LANES) + tile
                    vec[at:at + 1] = d_rows_ref[layer, row:row + 1, lanes(tile)]
            lane = lax.broadcasted_iota(jnp.int32, (SUB, LANES), 1)
            for shard in range(SHARDS):
                row, off = divmod(shard * per_device, LANES)
                here, after = vec[pl.ds(row, SUB)], vec[pl.ds(row + 1, SUB)]
                if off:
                    here = jnp.where(lane < LANES - off, pltpu.roll(here, LANES - off, 1), pltpu.roll(after, LANES - off, 1))
                bits = [shard // weight % 2 for weight in WEIGHT]
                stage[(*bits, pl.ds(layer * layout.vec_rows, layout.vec_rows))] = here
        copy = pltpu.make_async_copy(stage, region(layout.vec, stage.shape[4]), sem)
        copy.start()
        copy.wait()
        repeat(layout.macros + STREAMS * STAGES - plan[-1], lambda index: reducer.step(plan[-1] + index))
        load(out_ref, sum_ref, sem).wait()
        copy_image.wait()

    pl.run_scoped(finish, pltpu.VMEM((*CUBE, blocks * layout.vec_rows + layout.pad, LANES), F32),
                  pltpu.SemaphoreType.DMA, pltpu.VMEM(cot_ref.shape, BF16), pltpu.SemaphoreType.DMA)


def backward(cot, context, saved, tokens, ctx_len, total):
    count, width = cot.shape
    blocks = len(saved)
    layout = Layout(width, context.shape[1], blocks)
    starts = [sum(map(int, ''.join(PLAN[:phase]))) for phase in range(len(PLAN) + 1)]
    cfg = (tokens, ctx_len, width, blocks, layout, total, [*zip(starts, PLAN), starts[-1]])
    operands = [cot, context]
    for block in saved:
        operands += [block[name] for name in NAMES]
    shape = saved[0]['rows'].shape
    outs = pl.pallas_call(
        functools.partial(backward_kernel, cfg),
        in_specs=any_specs(len(operands)), out_specs=any_specs(3),
        out_shape=[jax.ShapeDtypeStruct((count, width), BF16),
                   jax.ShapeDtypeStruct((*CUBE, layout.rows, LANES), F32),
                   jax.ShapeDtypeStruct((layout.rows, LANES), F32)],
        scratch_shapes=[pltpu.VMEM((count, width), F32), pltpu.VMEM((2, count, width), F32),
                        pltpu.VMEM((blocks,) + shape, F32), pltpu.VMEM((blocks,) + shape, F32),
                        pltpu.VMEM((blocks, 96, LANES), F32), pltpu.VMEM((layout.rows, LANES), F32),
                        pltpu.SemaphoreType.DMA((2 + blocks,))] + Reducer.scratch(),
        name='backward', **settings(0),
    )(*operands)
    return outs[0], outs[2], layout


PLAN = ('0011002011', '11101000100', '11100101001', '1021011012', '11002001000', '21010111100')


def deliver_kernel(cfg, sum_ref, gx_ref, tokens_ref, *out_refs):
    width, ctx_width, blocks, layout = cfg
    out_refs[-2][:] = gx_ref[:]
    out_refs[-1][:] = tokens_ref[:]
    tiles = width // LANES
    for layer in range(blocks):
        for name, target in zip(MATS, out_refs):
            first = (blocks - 1 - layer) * layout.block + getattr(layout, name)
            total = target.shape[0] // blocks
            part = {'kv2': ctx_width, 'ff2': 4 * width}.get(name, width) // SHARDS
            many = total // part

            def put(tile, size, stride, row):
                target[pl.ds(tile * blocks + layer, size, stride=stride * blocks)] = sum_ref[row:row + size]

            for index in range(many):
                if name == 'ff1':
                    half, at = divmod(index, many // 2)
                    step, tile = divmod(at, 2)
                    put(index, part, many, first + step * FF_PART + half * 80 + tile * part)
                elif name == 'ff2':
                    for block in range(part // FF_SUB):
                        put(block * FF_PART + index, FF_SUB, tiles, first + block * FF_PART + index * FF_SUB)
                else:
                    put(index, part, many, first + index * part)
        per_device = 17 * width // SHARDS
        for row in range(-(-per_device // LANES)):
            size = min(LANES, per_device - row * LANES)
            out_refs[len(MATS)][layer:layer + 1, row * LANES:row * LANES + size] = line(
                sum_ref, layout.vec + layer * layout.vec_rows + row)[:, :size]


def deliver(sums, grad_x, tokens, shapes, cfg):
    in_vmem = pl.BlockSpec(memory_space=pltpu.VMEM)
    out_shape = [jax.ShapeDtypeStruct(shape, F32) for shape in shapes] + [
        jax.ShapeDtypeStruct(grad_x.shape, BF16), jax.ShapeDtypeStruct(tokens.shape, BF16)]
    return pl.pallas_call(
        functools.partial(deliver_kernel, cfg), in_specs=[in_vmem] * 3, out_specs=[in_vmem] * len(out_shape),
        out_shape=out_shape, compiler_params=pltpu.CompilerParams(vmem_limit_bytes=VMEM_BYTES), name='deliver',
    )(sums, grad_x, tokens)


def solution(mesh):
    n_dev = mesh.shape[AXIS]

    def local(tokens_x, context, cot_out, *shards):
        samples, tokens, width = tokens_x.shape
        blocks = shards[0].shape[0]
        spare = -shards[-1].shape[1] % LANES
        padded = shards[:-1] + (jnp.pad(shards[-1], ((0, 0), (0, spare))),)
        raws = [shard.reshape(blocks, -1, LANES).swapaxes(0, 1) for shard in padded]
        raws = [raw.reshape(-1, LANES) for raw in raws[:-1]] + raws[-1:]
        saved, ctx_rows, out_tokens = forward(tokens_x, context, raws, blocks)
        grad_x, sums, layout = backward(cot_out.reshape(samples * tokens, width), ctx_rows, saved, tokens,
                                        context.shape[1], samples * n_dev)
        shapes = [raw.shape for raw in raws[:-1]] + [shards[-1].shape]
        *grads, vec, grad_x, out_tokens = deliver(sums, grad_x, out_tokens, shapes,
                                                  (width, context.shape[2], blocks, layout))
        grads = [grad.reshape(-1, blocks, LANES).swapaxes(0, 1).reshape(blocks, -1) for grad in grads] + [vec]
        return (out_tokens.reshape(tokens_x.shape), grad_x.reshape(tokens_x.shape), *grads)

    param_spec = P(None, AXIS)
    in_specs = (P(AXIS), P(AXIS), P(AXIS)) + (param_spec,) * 8
    out_specs = (P(AXIS), P(AXIS)) + (param_spec,) * 8
    return jax.shard_map(local, mesh=mesh, in_specs=in_specs, out_specs=out_specs, check_vma=False)
```

```python
import functools
import math
from typing import Any, NamedTuple
import jax
import jax.numpy as jnp
from jax import lax
from jax.experimental import pallas as pl
from jax.experimental.pallas import tpu as pltpu
from jax.sharding import PartitionSpec as P

AXIS = 'fsdp'
HEAD = 64
EPS = 1e-5
SHARDS = 16
CUBE = (2, 2, 2, 2)
WEIGHT = (8, 4, 2, 1)
CHIP_WEIGHT = WEIGHT[1:]
CHIPS = 8
SUB = 8
FULL = slice(None)
SELF_ROWS, CROSS_ROWS = (0, 1, 6), (2, 3, 7)
F32 = jnp.float32
BF16 = jnp.bfloat16
LANES = 128
VMEM_BYTES = 63 * 2 ** 20
BELL = (2 * math.pi) ** -0.5
LN_ROWS = 128
PAIR_ROWS = 512
FF_ROWS = 256
FF_PART = 160
FF_SUB = 32
FF_COLS = 256

TAIL_C = 3.3
TAIL = (0.398796301085, 1.32638029784, 3.66563581228, 14.7229083576, -17.4165998636, 251.026512347, -660.864693498,
        511.950585826)
HALF_LOG2E = 0.5 * math.log2(math.e)


def mm(lhs, rhs):
    return jnp.dot(lhs, rhs, preferred_element_type=F32)


def mm_nt(lhs, rhs):
    return lax.dot_general(lhs, rhs, (((1,), (1,)), ((), ())), preferred_element_type=F32)


def mm_tn(lhs, rhs):
    return lax.dot_general(lhs, rhs, (((0,), (0,)), ((), ())), preferred_element_type=F32)


pipeline = functools.partial(pltpu.emit_pipeline, _explicit_indices=True)


def lane_mean(x):
    return jnp.mean(x, axis=-1, keepdims=True)


def lane_sum(x):
    return jnp.sum(x, axis=-1, keepdims=True)


def row_sum(x):
    return jnp.sum(x, axis=0, keepdims=True)


def line(ref, index):
    return ref[index:index + 1]


def add_line(ref, index, values):
    ref[index:index + 1] += values


def span(index, size):
    return pl.ds(pl.multiple_of(index * size, size), size)


def pieces_of(first, size):
    return [pl.ds(pl.multiple_of(first + piece * LN_ROWS, LN_ROWS), LN_ROWS) for piece in range(size // LN_ROWS)]


def lanes(tile):
    return slice(tile * LANES, (tile + 1) * LANES)


def repeat(count, body):
    def one(index, carry):
        body(index)
        return carry

    lax.fori_loop(0, count, one, 0)


def normalize(x):
    centered = x - lane_mean(x)
    scale = lax.rsqrt(lane_mean(centered * centered) + EPS)
    return centered * scale, scale


def norm_back(x, d_norm, gain):
    hat, scale = normalize(x)
    d_hat = d_norm * gain
    pulled = d_hat - lane_mean(d_hat) - hat * lane_mean(d_hat * hat)
    return pulled * scale, row_sum(d_norm * hat), row_sum(d_norm)


def low_half(rows):
    return lax.broadcasted_iota(jnp.int32, (rows, LANES), 1) < HEAD


def head_stack(pair, low):
    zero = jnp.zeros_like(pair)
    return jnp.concatenate([jnp.where(low, pair, zero), jnp.where(low, zero, pair)], axis=0)


def head_unstack(stacked, low):
    half = stacked.shape[0] // 2
    return jnp.where(low, stacked[:half], stacked[half:])


def softmax_halves(scores, valid):
    half = scores.shape[0] // 2
    parts = []
    for part in (scores[:half], scores[half:]):
        if valid < half:
            part = jnp.where(lax.broadcasted_iota(jnp.int32, part.shape, 0) < valid, part, -jnp.inf)
        part = jnp.exp(part - jnp.max(part, axis=0, keepdims=True))
        parts.append(part * (1.0 / row_sum(part)))
    return parts


def stack_bf16(parts):
    return jnp.concatenate([part.astype(BF16) for part in parts], axis=0)


def rows_at(number):
    return slice(number * FF_ROWS, (number + 1) * FF_ROWS)


def ahead(count, first, second, third=None):
    ready = first(0)
    for index in range(count):
        now = ready
        if index + 1 < count:
            ready = first(index + 1)
        second(index, now)
        if third and index:
            third(index - 1)
    if third:
        third(count - 1)


def scaled(query):
    return query * BF16(HEAD ** -0.5)


def pair_scores(query, keys):
    return mm_nt(head_stack(keys, low_half(keys.shape[0])), scaled(query))


def pair_forward(scores, values, valid):
    probs = stack_bf16(softmax_halves(scores, valid))
    return mm_tn(head_stack(values, low_half(values.shape[0])), probs).astype(BF16).T


def pair_backward_scores(query, keys, values, d_out):
    low = low_half(keys.shape[0])
    return mm_nt(head_stack(keys, low), scaled(query)), mm_nt(head_stack(values, low), d_out)


def pair_backward(scores, d_probs, query, keys, d_out, valid):
    low = low_half(keys.shape[0])
    half = keys.shape[0]
    parts = softmax_halves(scores, valid)
    d_values = head_unstack(mm(stack_bf16(parts), d_out), low).astype(BF16)
    d_scores = []
    for part, d_part in zip(parts, (d_probs[:half], d_probs[half:])):
        d_scores.append(part * (d_part - row_sum(part * d_part)))
    d_scores = stack_bf16(d_scores)
    d_query = (mm_tn(head_stack(keys, low), d_scores) * HEAD ** -0.5).astype(BF16).T
    return d_query, head_unstack(mm(d_scores, scaled(query)), low).astype(BF16), d_values


def normal_cdf(u):
    inverse = 1.0 / (TAIL_C + jnp.abs(u))
    poly = TAIL[-1]
    for coef in TAIL[-2::-1]:
        poly = poly * inverse + coef
    bell = jnp.exp2(u * u * -HALF_LOG2E)
    tail = bell * (inverse * poly)
    return jnp.where(u >= 0, 1.0 - tail, tail), bell


UNIT = 80
COLORS = 3
MACRO = COLORS * UNIT
SLOTS = 3
STREAMS = 2
STAGES = 4
CORE = 3
ORDERS = ((2, 1, 0), (1, 0, 2), (0, 2, 1))
MESH = pl.DeviceIdType.MESH


def bits_of(device):
    return [lax.rem(lax.div(device, weight), 2) for weight in WEIGHT]


class Place:
    def __init__(self):
        me = lax.axis_index(AXIS)
        self.bits = bits_of(me)
        self.others = [1 - bit for bit in self.bits]
        self.devices = [(me + (other - bit) * weight,) for bit, other, weight in zip(self.bits, self.others, WEIGHT)]

    def rows_of(self, ref, first, rows):
        half = ref.shape[CORE] // 2
        return pl.ds(pl.multiple_of(self.bits[CORE] * half + first, SUB), rows)

    def own(self, ref):
        return ref.at[(*self.bits[:CORE], self.rows_of(ref, 0, ref.shape[CORE] // 2))]

    def entry_barrier(self):
        barrier = pltpu.get_barrier_semaphore()
        for device in self.devices:
            pl.semaphore_signal(barrier, inc=1, device_id=device, device_id_type=MESH)
        pl.semaphore_wait(barrier, 4)


def pick(ref, lead, dim, value):
    return ref.at[(lead,) + (FULL,) * dim + (value,)]


class At(NamedTuple):
    stream: Any
    index: Any
    row: Any


class Reducer:
    def __init__(self, place, macros, scale, grads, out, refs):
        self.place, self.macros, self.scale, self.grads, self.out = place, macros, scale, grads, out
        self.own, self.held = refs[0], refs[1:1 + STAGES]
        self.send, self.recv, self.load = refs[1 + STAGES:]

    @staticmethod
    def scratch():
        held = [pltpu.VMEM((STREAMS * SLOTS * COLORS,) + (2,) * (3 - stage) + (UNIT, LANES), F32) for stage in range(STAGES)]
        sems = [pltpu.SemaphoreType.DMA((STREAMS, COLORS, STAGES)), pltpu.SemaphoreType.DMA((STREAMS * SLOTS * COLORS, STAGES)),
                pltpu.SemaphoreType.DMA((STREAMS, COLORS))]
        return [pltpu.VMEM((STREAMS * COLORS, *CUBE[1:], UNIT, LANES), F32)] + held + sems

    def axis(self, color, stage):
        return CORE if stage == 0 else ORDERS[color][stage - 1]

    def dim(self, color, stage):
        gone = ORDERS[color][:stage - 1]
        return sum(1 for axis in range(ORDERS[color][stage - 1]) if axis not in gone)

    def copy(self, at, color, stage):
        axis = self.axis(color, stage)
        other = self.place.others[axis]
        index = at.index + color
        if stage == 0:
            source = self.grads.at[:, :, :, other, pl.ds(at.row + color * UNIT, UNIT)]
        else:
            source = pick(self.held[stage - 1], index, self.dim(color, stage), other)
        return pltpu.make_async_remote_copy(
            src_ref=source, dst_ref=self.held[stage].at[index], send_sem=self.send.at[at.stream, color, stage],
            recv_sem=self.recv.at[index, stage], device_id=self.place.devices[axis], device_id_type=MESH)

    def own_copy(self, at, color):
        return pltpu.make_async_copy(self.grads.at[:, :, :, self.place.bits[CORE], pl.ds(at.row + color * UNIT, UNIT)],
                                     self.own.at[at.stream * COLORS + color], self.load.at[at.stream, color])

    def add(self, at, color, stage):
        index = at.index + color
        if stage == 0:
            self.held[0][index] += self.own[at.stream * COLORS + color]
            return
        mine = self.held[stage - 1][(index,) + (FULL,) * self.dim(color, stage)
                                    + (self.place.bits[self.axis(color, stage)],)]
        if stage < STAGES - 1:
            self.held[stage][index] += mine
        else:
            self.out[pl.ds(at.row + color * UNIT, UNIT)] = (self.held[stage][index] + mine) * self.scale

    def step(self, t):
        stream, tau = lax.rem(t, STREAMS), lax.div(t, STREAMS)

        def when_live(local, body):
            @pl.when((local >= 0) & (local * STREAMS + stream < self.macros))
            def _():
                body(At(stream, (stream * SLOTS + lax.rem(local, SLOTS)) * COLORS,
                        pl.multiple_of((local * STREAMS + stream) * MACRO, SUB)))

        def take(stage, at):
            for color in range(COLORS):
                copy = self.copy(at, color, stage)
                copy.wait_send()
                copy.wait_recv()
                if stage == 0:
                    self.own_copy(at, color).wait()
            for color in range(COLORS):
                self.add(at, color, stage)

        def give(stage, at):
            for color in range(COLORS):
                self.copy(at, color, stage).start()
                if stage == 0:
                    self.own_copy(at, color).start()

        for stage in reversed(range(STAGES)):
            when_live(tau - 1 - stage, functools.partial(take, stage))
        for stage in range(STAGES):
            when_live(tau - stage, functools.partial(give, stage))

    def beside(self, index, counts, start):
        number, first = 0, start
        for site, digit in enumerate(map(int, counts)):
            if digit:
                number += jnp.where(index == site, digit, 0)
                first += jnp.where(index > site, digit, 0)
        if start < start + sum(map(int, counts)):
            lax.fori_loop(0, number, lambda step, carry: (self.step(first + step), carry)[1], 0)


class Piece(NamedTuple):
    ref: Any
    first: Any
    rows: Any
    cols: Any
    color: int
    number: int


class Gatherer:
    def __init__(self, place, macros, send, recv):
        self.place, self.send, self.recv = place, send, recv
        self.jobs = {}
        number = 0
        for index, macro in enumerate(macros):
            first, gap = (0, 1) if index < 2 else (index - 1, 2)
            pieces = []
            for ref, color, row, rows, cols in macro:
                pieces.append(Piece(ref, row, rows, cols, color, number))
                number += 1
            for stage in range(STAGES + 1):
                self.jobs.setdefault(first + gap * stage, []).append((stage, pieces))

    def copy(self, piece, stage):
        order = ORDERS[piece.color]
        index = [FULL if axis in order[:stage] else self.place.bits[axis] for axis in range(CORE)]
        block = piece.ref.at[(*index, self.place.rows_of(piece.ref, piece.first, piece.rows), piece.cols)]
        axis = order[stage] if stage < CORE else CORE
        return pltpu.make_async_remote_copy(
            src_ref=block, dst_ref=block, send_sem=self.send.at[piece.number, stage],
            recv_sem=self.recv.at[piece.number, stage], device_id=self.place.devices[axis], device_id_type=MESH)

    def step(self, t):
        for stage, pieces in self.jobs[t]:
            if stage:
                for piece in pieces:
                    copy = self.copy(piece, stage - 1)
                    copy.wait_send()
                    copy.wait_recv()
            if stage < STAGES:
                for piece in pieces:
                    self.copy(piece, stage).start()

    def beside(self, index, part, sites, offset=0):
        first, count = sum(FORWARD_STEPS[:part]), FORWARD_STEPS[part]
        for number in range(count):
            site = (number + 1) * sites // count - 1 if count <= sites else number * sites // count

            @pl.when(index == offset + site)
            def _(number=number):
                self.step(first + number)


FORWARD_STEPS = (6, 8, 4, 3, 3, 3, 4, 2, 0)
MATS = ('qkv', 'out', 'q2', 'kv2', 'out2', 'ff1', 'ff2')
WEIGHTS = ('w_a', 'w_b', 'w_kv2', 'w_ff1', 'w_ff2')
KEPT = ('h', 'h1', 'h2', 'qkv', 'out1', 'q', 'kv', 'out2', 'fa', 'fg', 'z', 'rows')


def load(source, target, sem):
    copy = pltpu.make_async_copy(source, target, sem)
    copy.start()
    return copy


def fetch(source, cols, target, sems, into=FULL):
    def copy(shard):
        index = [lax.rem(lax.div(shard, weight), 2) for weight in CHIP_WEIGHT]
        return pltpu.make_async_copy(source.at[(*index, FULL, cols)], target.at[span(shard, source.shape[CORE]), into],
                                     sems.at[shard])

    repeat(CHIPS, lambda shard: copy(shard).start())
    return lambda: repeat(CHIPS, lambda shard: copy(shard).wait())


def macro_list(weights, vec):
    macros = []
    for block in weights:
        high = {name: block[name].shape[CORE] // 2 for name in WEIGHTS}

        def add(name, row, rows, first, cols):
            edges = [round(rows // SUB * part / COLORS) * SUB for part in range(COLORS + 1)]
            macros.append([(block[name], (part + len(macros)) % COLORS, row + edges[part], edges[part + 1] - edges[part],
                            pl.ds(first, cols)) for part in range(COLORS)])

        wide = block['w_a'].shape[-1] // 2
        for part in range(2):
            add('w_a', 0, high['w_a'], part * wide, wide)
        quarter = high['w_kv2'] // 4
        for part in range(4):
            add('w_kv2', part * quarter, quarter, 0, wide)
        add('w_b', 0, high['w_b'], 0, wide)
        half = high['w_ff2'] // 2
        for part in range(2):
            add('w_ff2', part * half, half, 0, wide // 2)
        inner = block['w_ff1'].shape[-1] // 2
        for part in range(2):
            for half in range(2):
                add('w_ff1', 0, high['w_ff1'], half * inner + part * inner // 2, inner // 2)
    macros[0].append((vec, 0, 0, vec.shape[CORE] // 2, FULL))
    return macros


def forward_kernel(cfg, *refs):
    tokens, width, blocks, per_vec = cfg
    heads = width // HEAD
    tiles = width // LANES
    tokens_ref, context_ref = refs[:2]
    raw_refs = refs[2:2 + len(MATS) + 1]
    refs = refs[2 + len(raw_refs):]
    kept = [dict(zip(KEPT, refs[layer * len(KEPT):])) for layer in range(blocks)]
    refs = refs[blocks * len(KEPT):]
    weights = [dict(zip(WEIGHTS, refs[layer * len(WEIGHTS):])) for layer in range(blocks)]
    refs = refs[blocks * len(WEIGHTS):]
    vec_all_ref, ctx_out_ref, tokens_out_ref, hidden, context, rows_ref, vec_ref, sems, send, recv = refs
    samples, ctx_len = context_ref.shape[:2]
    pad = context.shape[0] // samples
    count = tokens_ref.shape[0]
    chunk = PAIR_ROWS
    per_step = chunk // tokens
    place = Place()
    gatherer = Gatherer(place, macro_list(weights, vec_all_ref), send, recv)

    def each_piece(body):
        repeat(count // chunk, lambda index: [body(at) for at in pieces_of(index * chunk, chunk)])

    def startup(image, wide, flat, vec_piece, raws, pieces, raw_sems, own_sems):
        first = [load(tokens_ref, image, sems.at[0]), load(context_ref, wide, sems.at[1])]
        loads = [load(source, target, raw_sems.at[index])
                 for index, (source, target) in enumerate(zip(raw_refs, raws))]

        def tile(layer, name, target, first_col):
            raw = raws[MATS.index(name)]
            flat[:raw.shape[0]] = raw[:].astype(F32)
            rows = target.shape[0]
            stride = raw.shape[0] // rows
            for index in range(stride // blocks):
                at = first_col + index * LANES
                target[:, at:at + LANES] = flat[pl.ds(index * blocks + layer, rows, stride=stride)].astype(BF16)

        def own(layer, name):
            number = layer * len(WEIGHTS) + WEIGHTS.index(name)
            return load(pieces[number], place.own(weights[layer][name]), own_sems.at[number])

        def prepare(layer, name):
            target = pieces[layer * len(WEIGHTS) + WEIGHTS.index(name)]
            if name == 'w_a':
                tile(layer, 'qkv', target, 0)
                tile(layer, 'out', target, 3 * width)
            elif name == 'w_b':
                tile(layer, 'q2', target, 0)
                tile(layer, 'out2', target, width)
            else:
                tile(layer, name[2:], target, 0)
            return own(layer, name)

        for copy in loads:
            copy.wait()
        vec_piece[:] = jnp.zeros_like(vec_piece)
        for layer in range(blocks):
            flat[:per_vec] = raws[-1][:, layer].astype(F32)
            vec_piece[layer * SUB:layer * SUB + per_vec] = flat[:per_vec].astype(BF16)
        pending = [prepare(0, 'w_a'), load(vec_piece, place.own(vec_all_ref), sems.at[2])]
        place.entry_barrier()
        later = [[(0, 'w_kv2')], [(0, 'w_b'), (0, 'w_ff2')], [(0, 'w_ff1')], [(1, name) for name in WEIGHTS[:CORE]],
                 [(1, name) for name in WEIGHTS[CORE:]]]
        for t, jobs in enumerate(later):
            for copy in pending:
                copy.wait()
            gatherer.step(t)
            pending = [prepare(layer, name) for layer, name in jobs if layer < blocks]
        for copy in first:
            copy.wait()
        each_piece(lambda at: hidden.at[0].__setitem__(at, image[at].astype(F32)))
        context[:] = jnp.zeros_like(context)
        for sample in range(samples):
            context[sample * pad:sample * pad + ctx_len] = wide[sample]
        for copy in pending:
            copy.wait()
        for t in range(len(later), FORWARD_STEPS[0]):
            gatherer.step(t)

    def raw_shape(index):
        return pltpu.VMEM(raw_refs[index].shape, BF16)

    pl.run_scoped(startup, pltpu.VMEM(tokens_ref.shape, BF16), pltpu.VMEM(context_ref.shape, BF16),
                  pltpu.VMEM((max(ref.shape[0] for ref in raw_refs), LANES), F32), pltpu.VMEM((blocks * SUB, LANES), BF16),
                  [raw_shape(index) for index in range(len(raw_refs))],
                  [pltpu.VMEM((block[name].shape[CORE] // 2, block[name].shape[-1]), BF16)
                   for block in weights for name in WEIGHTS],
                  pltpu.SemaphoreType.DMA((len(raw_refs),)), pltpu.SemaphoreType.DMA((blocks * len(WEIGHTS),)))
    ctx_copy = load(context, ctx_out_ref, sems.at[3])

    def unpack(parts, sem):
        load(vec_all_ref, parts, sem).wait()
        vec_ref[:] = jnp.zeros_like(vec_ref)
        rows_ref[:] = jnp.zeros_like(rows_ref)
        lane = lax.broadcasted_iota(jnp.int32, (SUB, LANES), 1)
        per_device = 17 * width // SHARDS
        for layer in range(blocks):
            vec = vec_ref.at[layer]
            for shard in range(SHARDS):
                chip, core = divmod(shard, 2)
                bits = [chip // weight % 2 for weight in CHIP_WEIGHT]
                part = parts[(*bits, pl.ds((core * blocks + layer) * SUB, SUB))].astype(F32)
                row, off = divmod(shard * per_device, LANES)
                if off:
                    part = pltpu.roll(part, off, 1)
                    vec[pl.ds(row + 1, SUB)] += jnp.where(lane < off, part, 0.0)
                vec[pl.ds(row, SUB)] += jnp.where(lane >= off, part, 0.0)
            for row in range(9):
                for tile in range(tiles):
                    rows_ref[layer, row:row + 1, lanes(tile)] = line(vec, row * tiles + tile)

    pl.run_scoped(unpack, pltpu.VMEM(vec_all_ref.shape, BF16), pltpu.SemaphoreType.DMA)
    rows_copies = [load(rows_ref.at[layer], kept[layer]['rows'], sems.at[4 + layer]) for layer in range(blocks)]

    def attention(layer, source, target, cross, part):
        rows = rows_ref.at[layer]
        packed = weights[layer]['w_b' if cross else 'w_a']
        inner = packed.shape[-1] - width
        gain, shift, bias = CROSS_ROWS if cross else SELF_ROWS

        def scoped(norm, w_in, w_out, w_kv, kv, in_sems):
            waits = [fetch(packed, pl.ds(0, inner), w_in, in_sems.at[0]), fetch(packed, pl.ds(inner, width), w_out, in_sems.at[1])]
            if cross:
                fetch(weights[layer]['w_kv2'], FULL, w_kv, in_sems.at[2])()
                kv[:] = mm(context[:], w_kv[:]).astype(BF16)
                kv_copy = load(kv, kept[layer]['kv'], in_sems.at[2, 0])
            for wait in waits:
                wait()

            def body(idx, qkv, mixed):
                step = idx.index[0]
                at_rows = span(step, chunk)
                for at, here in zip(pieces_of(step * chunk, chunk), pieces_of(0, chunk)):
                    hat, unused = normalize(source[at])
                    norm[here] = (hat * line(rows, gain) + line(rows, shift)).astype(BF16)
                qkv[:] = mm(norm[:], w_in[:]).astype(BF16)

                def sample(number):
                    at = span(number, tokens)
                    index = step * per_step + number
                    kv_at = span(index, pad) if cross else at
                    k_ref, k_first, limit = (kv, 0, ctx_len) if cross else (qkv, width, tokens)

                    def scores(pair):
                        return pair_scores(qkv[at, lanes(pair)], k_ref[kv_at, lanes(pair + k_first // LANES)])

                    def rest(pair, ready):
                        values = k_ref[kv_at, lanes(pair + (k_first + width) // LANES)]
                        mixed[at, lanes(pair)] = pair_forward(ready, values, limit)

                    ahead(heads // 2, scores, rest)
                    gatherer.beside(index, part, samples)

                repeat(per_step, sample)
                target[at_rows] = source[at_rows] + mm(mixed[:], w_out[:]) + line(rows, bias)

            block = lambda cols: pl.BlockSpec((chunk, cols), lambda step: (step, 0))
            pipeline(body, grid=(count // chunk,), out_specs=[block(inner), block(width)])(
                kept[layer]['q' if cross else 'qkv'], kept[layer]['out2' if cross else 'out1'])
            if cross:
                kv_copy.wait()

        small = pltpu.VMEM((SUB, LANES), BF16)
        pl.run_scoped(scoped, pltpu.VMEM((chunk, width), BF16), pltpu.VMEM((width, inner), BF16),
                      pltpu.VMEM((width, width), BF16), pltpu.VMEM((context_ref.shape[2], 2 * width), BF16) if cross else small,
                      pltpu.VMEM((samples * pad, 2 * width), BF16) if cross else small, pltpu.SemaphoreType.DMA((3, CHIPS)))

    def feed_forward(layer, source, target, part):
        rows = rows_ref.at[layer]
        vec = vec_ref.at[layer]
        inner = weights[layer]['w_ff1'].shape[-1] // 2
        steps = inner // FF_COLS
        wide = FF_COLS // LANES

        def scoped(norm, w1, w2, w_sems):
            def fetch_half(part):
                both = [pl.ds(half * inner + part * inner // 2, inner // 2) for half in range(2)]
                return [fetch(weights[layer]['w_ff1'], cols, w1, w_sems.at[half], cols) for half, cols in enumerate(both)]

            waits = fetch_half(0) + [fetch(weights[layer]['w_ff2'], FULL, w2, w_sems.at[2])]

            def begin(at):
                hat, unused = normalize(source[at])
                norm[at] = (hat * line(rows, 4) + line(rows, 5)).astype(BF16)
                target[at] = source[at] + line(rows, SUB)

            each_piece(begin)
            for wait in waits:
                wait()

            def body(idx, fa, fg, z):
                step = idx.index[0]
                cols, gate_cols = span(step, FF_COLS), span(step + steps, FF_COLS)

                @pl.when(step == steps // 2)
                def _():
                    for wait in fetch_half(1):
                        wait()

                def bias(half):
                    first = 9 * tiles + (half * steps + step) * wide
                    return jnp.concatenate([vec[pl.ds(first + index, 1)] for index in range(wide)], axis=1)

                bias_a, bias_g = bias(0), bias(1)

                def hidden_of(number):
                    normed = norm[rows_at(number)]
                    return mm(normed, w1[:, gate_cols]) + bias_g, mm(normed, w1[:, cols]) + bias_a

                def rest(number, ready):
                    at = rows_at(number)
                    gate, value = ready
                    cdf, bell = normal_cdf(gate)
                    factor = gate * cdf
                    z[at] = (value * factor).astype(BF16)
                    fa[at] = factor
                    fg[at] = value * (cdf + gate * bell * BELL)

                def project(number):
                    target[rows_at(number)] += mm(z[rows_at(number)], w2[cols])

                ahead(count // FF_ROWS, hidden_of, rest, project)
                for half in range(2):
                    gatherer.beside(step, part + half, steps // 2, half * steps // 2)

            block = ff_block(count)
            pipeline(body, grid=(steps,), out_specs=[block, block, block])(
                kept[layer]['fa'], kept[layer]['fg'], kept[layer]['z'])

        pl.run_scoped(scoped, pltpu.VMEM((count, width), BF16), pltpu.VMEM((width, 2 * inner), BF16),
                      pltpu.VMEM((inner, width), BF16), pltpu.SemaphoreType.DMA((3, CHIPS)))

    phases = 3 * blocks
    saves = [load(hidden.at[0], kept[0]['h'], sems.at[6]), None]
    for phase in range(phases):
        layer, kind = divmod(phase, 3)
        source, target = hidden.at[phase % 2], hidden.at[(phase + 1) % 2]
        other = (phase + 1) % 2
        if saves[other] is not None:
            saves[other].wait()
        if kind < 2:
            attention(layer, source, target, kind == 1, 1 + 4 * layer + kind)
        else:
            feed_forward(layer, source, target, 1 + 4 * layer + kind)
        following = divmod(phase + 1, 3)
        saves[other] = None
        if phase + 1 < phases:
            saves[other] = load(target, kept[following[0]][KEPT[following[1]]], sems.at[6 + other])

    def finish(image):
        each_piece(lambda at: image.__setitem__(at, hidden[phases % 2, at].astype(BF16)))
        load(image, tokens_out_ref, sems.at[0]).wait()

    pl.run_scoped(finish, pltpu.VMEM(tokens_ref.shape, BF16))
    for copy in [copy for copy in saves if copy is not None] + [ctx_copy] + rows_copies:
        copy.wait()


def settings(number):
    return dict(compiler_params=pltpu.CompilerParams(collective_id=number, has_side_effects=True,
                                                     vmem_limit_bytes=VMEM_BYTES),
                cost_estimate=pl.CostEstimate(flops=10 ** 11, bytes_accessed=10 ** 8, transcendentals=0))


def ff_block(count):
    return pl.BlockSpec((None, count, FF_COLS), lambda step: (step, 0, 0))


def any_specs(count):
    return [pl.BlockSpec(memory_space=pl.ANY)] * count


def forward(tokens_x, context, raws, blocks):
    samples, tokens, width = tokens_x.shape
    ctx_width = context.shape[2]
    count, inner = samples * tokens, 4 * width
    pad = -(-context.shape[1] // SHARDS) * SHARDS
    steps = inner // FF_COLS
    plain = jax.ShapeDtypeStruct((count, width), F32)
    half = jax.ShapeDtypeStruct((count, width), BF16)
    wide = jax.ShapeDtypeStruct((steps, count, FF_COLS), F32)
    kept = [plain, plain, plain, jax.ShapeDtypeStruct((count, 3 * width), BF16), half, half,
            jax.ShapeDtypeStruct((samples * pad, 2 * width), BF16), half, wide, wide,
            jax.ShapeDtypeStruct(wide.shape, BF16), jax.ShapeDtypeStruct((SHARDS, width), F32)]
    whole_of = lambda rows, cols: jax.ShapeDtypeStruct((*CUBE[:CORE], rows // CHIPS, cols), BF16)
    weights = [whole_of(width, 4 * width), whole_of(width, 2 * width), whole_of(ctx_width, 2 * width),
               whole_of(width, 2 * inner), whole_of(inner, width)]
    extra = [whole_of(SHARDS * blocks * SUB, LANES), jax.ShapeDtypeStruct((samples * pad, ctx_width), BF16), half]
    shapes = kept * blocks + weights * blocks + extra
    pieces = 1 + COLORS * 13 * blocks
    outs = pl.pallas_call(
        functools.partial(forward_kernel, (tokens, width, blocks, raws[-1].shape[0])),
        in_specs=any_specs(2 + len(raws)), out_specs=any_specs(len(shapes)), out_shape=shapes,
        scratch_shapes=[pltpu.VMEM((2, count, width), F32), pltpu.VMEM((samples * pad, ctx_width), BF16),
                        pltpu.VMEM((blocks, SHARDS, width), F32), pltpu.VMEM((blocks, 96, LANES), F32),
                        pltpu.SemaphoreType.DMA((8,)), pltpu.SemaphoreType.DMA((pieces, STAGES)),
                        pltpu.SemaphoreType.DMA((pieces, STAGES))],
        name='forward', **settings(1),
    )(tokens_x.reshape(count, width), context, *raws)
    kept_of = [outs[layer * len(kept):(layer + 1) * len(kept)] for layer in range(blocks)]
    outs = outs[blocks * len(kept):]
    weights_of = [[whole.reshape(-1, whole.shape[-1]) for whole in outs[layer * len(weights):(layer + 1) * len(weights)]]
                  for layer in range(blocks)]
    saved = [dict(zip(KEPT + WEIGHTS, list(one) + list(two))) for one, two in zip(kept_of, weights_of)]
    return saved, outs[-2], outs[-1]


def view(values, *lead):
    return values.reshape(CUBE + lead + (LANES,))


def put_tiles(stage, values, first=0):
    rows = values.shape[0] // SHARDS
    for tile in range(values.shape[1] // LANES):
        at = first + tile * rows
        stage[:, :, :, :, at:at + rows] = view(values[:, lanes(tile)], rows)


class Layout:
    def __init__(self, width, ctx_width, blocks):
        unit = width // SHARDS * (width // LANES)
        self.ff1, self.ff2 = 0, 8 * unit
        self.q2 = 12 * unit
        self.out2 = self.q2 + unit
        self.kv2 = self.out2 + unit
        self.out = self.kv2 + ctx_width // SHARDS * (2 * width // LANES)
        self.qkv = self.out + unit
        self.block = self.qkv + 3 * unit
        self.vec = blocks * self.block
        self.vec_rows = -(-17 * width // SHARDS // LANES // SUB) * SUB
        used = self.vec + blocks * self.vec_rows
        self.macros = -(-used // MACRO)
        self.pad = self.macros * MACRO - used
        self.rows = self.macros * MACRO


NAMES = KEPT + WEIGHTS


def backward_kernel(cfg, *refs):
    tokens, ctx_len, width, blocks, layout, total, plan = cfg
    heads = width // HEAD
    cot_ref, context_ref = refs[:2]
    saved = [dict(zip(NAMES, refs[2 + layer * len(NAMES):])) for layer in range(blocks)]
    refs = refs[2 + blocks * len(NAMES):]
    gx_ref, grads_ref, sum_ref = refs[:3]
    refs = refs[3:]
    grad_ref, hidden_ref, rows_ref, d_rows_ref, vec_ref, out_ref, in_sems = refs[:7]
    place = Place()
    reducer = Reducer(place, layout.macros, 1.0 / total, grads_ref, out_ref, refs[7:])
    count = grad_ref.shape[0]
    chunk = PAIR_ROWS
    chunks = count // chunk
    phases = [(layer, kind) for layer in reversed(range(blocks)) for kind in ('h2', 'h1', 'h')]

    def hidden_copy(index):
        layer, kind = phases[index]
        return pltpu.make_async_copy(saved[layer][kind], hidden_ref.at[index % 2], in_sems.at[index % 2])

    def rows_copy(layer):
        return pltpu.make_async_copy(saved[layer]['rows'], rows_ref.at[layer], in_sems.at[2 + layer])

    def base(layer):
        return (blocks - 1 - layer) * layout.block

    def region(row, size):
        return grads_ref.at[:, :, :, :, pl.ds(pl.multiple_of(row, SUB), size)]

    def each_piece(body):
        repeat(chunks, lambda index: [body(at) for at in pieces_of(index * chunk, chunk)])

    def ff_phase(layer, index, first):
        hidden = hidden_ref.at[index % 2]
        rows = rows_ref.at[layer]
        d_rows = d_rows_ref.at[layer]
        vec = vec_ref.at[layer]
        src = saved[layer]
        w1_all, w2_all = src['w_ff1'], src['w_ff2']
        inner = w2_all.shape[0]
        steps = inner // FF_COLS
        start, counts = first

        def scoped(norm_t, grad_bf, du, w1, acc, stage1, stage2, sem1, sem2):
            def begin(at):
                hat, unused = normalize(hidden[at])
                norm_t[:, at] = (hat * line(rows, 4) + line(rows, 5)).astype(BF16).T
                grad_bf[at] = grad_ref[at].astype(BF16)
                add_line(d_rows, 8, row_sum(grad_ref[at]))
                acc[at] = jnp.zeros((LN_ROWS, width), F32)

            each_piece(begin)

            def copy1(step):
                return pltpu.make_async_copy(stage1, region(base(layer) + layout.ff1 + step * FF_PART, FF_PART), sem1)

            def copy2(step, part):
                block = step * 8 + part
                shard = lax.div(block, 5)
                row = pl.multiple_of(base(layer) + layout.ff2 + lax.rem(block, 5) * FF_PART, SUB)
                bits = bits_of(shard)
                return pltpu.make_async_copy(stage2.at[part], grads_ref.at[(*bits, pl.ds(row, FF_PART))], sem2.at[part])

            def wait(step):
                copy1(step).wait()
                for part in range(8):
                    copy2(step, part).wait()

            def body(idx, w1a, w1g, w2, fa, fg, z):
                step = idx.index[0]
                w1[:, :FF_COLS] = w1a[:]
                w1[:, FF_COLS:] = w1g[:]

                sums = [jnp.zeros((1, FF_COLS), F32)] * 2

                def d_gated(number):
                    return mm_nt(grad_bf[rows_at(number)], w2[:]).astype(BF16).astype(F32)

                def rest(number, dz):
                    at = rows_at(number)
                    for half, factor in enumerate((fa, fg)):
                        part = dz * factor[at]
                        du[at, half * FF_COLS:(half + 1) * FF_COLS] = part.astype(BF16)
                        sums[half] += row_sum(part)

                def project(number):
                    acc[rows_at(number)] += mm_nt(du[rows_at(number)], w1[:])

                ahead(count // FF_ROWS, d_gated, rest, project)
                for half in range(2):
                    for tile in range(2):
                        row = 9 * width // LANES + half * (inner // LANES) + 2 * step + tile
                        vec[pl.ds(row, 1)] = sums[half][:, lanes(tile)]

                @pl.when(step > 0)
                def _():
                    wait(step - 1)

                reducer.beside(step, counts, start)
                put_tiles(stage1, mm(norm_t[:], du[:, :FF_COLS]))
                put_tiles(stage1, mm(norm_t[:], du[:, FF_COLS:]), 80)
                d_w2 = mm_tn(z[:], grad_bf[:])
                for tile in range(width // LANES):
                    stage2[:, tile * FF_SUB:(tile + 1) * FF_SUB] = d_w2[:, lanes(tile)].reshape(8, FF_SUB, LANES)
                copy1(step).start()
                for number in range(8):
                    copy2(step, number).start()

            column = pl.BlockSpec((width, FF_COLS), lambda step: (0, step))
            kept = ff_block(count)
            pipeline(
                body, grid=(steps,),
                in_specs=[column, pl.BlockSpec((width, FF_COLS), lambda step: (0, step + steps)),
                          pl.BlockSpec((FF_COLS, width), lambda step: (step, 0)), kept, kept, kept],
            )(w1_all, w1_all, w2_all, src['fa'], src['fg'], src['z'])

            def finish(at):
                d_res, d_gain, d_shift = norm_back(hidden[at], acc[at], line(rows, 4))
                grad_ref[at] += d_res
                add_line(d_rows, 4, d_gain)
                add_line(d_rows, 5, d_shift)

            each_piece(finish)
            wait(steps - 1)

        pl.run_scoped(scoped, pltpu.VMEM((width, count), BF16), pltpu.VMEM((count, width), BF16),
                      pltpu.VMEM((count, 2 * FF_COLS), BF16), pltpu.VMEM((width, 2 * FF_COLS), BF16),
                      pltpu.VMEM((count, width), F32), pltpu.VMEM((*CUBE, FF_PART, LANES), F32),
                      pltpu.VMEM((8, FF_PART, LANES), F32), pltpu.SemaphoreType.DMA, pltpu.SemaphoreType.DMA((8,)))

    def attention_phase(layer, index, first, cross):
        hidden = hidden_ref.at[index % 2]
        rows = rows_ref.at[layer]
        d_rows = d_rows_ref.at[layer]
        src = saved[layer]
        packed = src['w_b' if cross else 'w_a']
        inner = packed.shape[1] - width
        steps = count // PAIR_ROWS
        per_step = PAIR_ROWS // tokens
        start, counts = first
        gain, shift, bias = CROSS_ROWS if cross else SELF_ROWS
        samples = count // tokens
        pad = context_ref.shape[0] // samples
        kv_rows_all = context_ref.shape[0] if cross else count

        def scoped(d_mix, d_q, d_kv, norm_t, d_wq, d_wout, stage, stage_out, sem, sem_out, w_in, w_out, in_sems_, context, kv, ctx_sems):
            if cross:
                loads = [pltpu.make_async_copy(context_ref, context, ctx_sems.at[0]),
                         pltpu.make_async_copy(src['kv'], kv, ctx_sems.at[1])]
                for copy in loads:
                    copy.start()
                d_wq[:] = jnp.zeros_like(d_wq)
                for copy in loads:
                    copy.wait()
            d_wout[:] = jnp.zeros_like(d_wout)
            for copy in [load(packed.at[:, pl.ds(0, inner)], w_in, in_sems_.at[0]),
                         load(packed.at[:, pl.ds(inner, width)], w_out, in_sems_.at[1])]:
                copy.wait()

            def body(idx, qkv, mixed):
                step = idx.index[0]
                at_rows = span(step, PAIR_ROWS)
                grad_bf = grad_ref[at_rows].astype(BF16)
                add_line(d_rows, bias, row_sum(grad_ref[at_rows]))
                d_wout[:] += mm_tn(mixed[:], grad_bf)
                d_mix[:] = mm_nt(grad_bf, w_out[:]).astype(BF16)

                def sample(number, carry):
                    at = span(number, tokens)
                    sample_index = step * per_step + number
                    if cross:
                        kv_at, d_q_at, k_ref, d_k_ref, k_first, limit = span(sample_index, pad), at, kv, d_kv, 0, ctx_len
                    else:
                        kv_at, d_q_at = at, span(sample_index, tokens)
                        k_ref, d_k_ref, k_first, limit = qkv, d_q, width, tokens
                    d_k_at = kv_at if cross else d_q_at

                    def operands(pair):
                        k_cols, v_cols = (lanes(pair + (k_first + more) // LANES) for more in (0, width))
                        return qkv[at, lanes(pair)], k_ref[kv_at, k_cols], k_ref[kv_at, v_cols], d_mix[at, lanes(pair)]

                    def scores(pair):
                        return pair_backward_scores(*operands(pair))

                    def rest(pair, ready):
                        query, keys, values, d_out = operands(pair)
                        d_query, d_keys, d_values = pair_backward(*ready, query, keys, d_out, limit)
                        d_q[d_q_at, lanes(pair)] = d_query
                        d_k_ref[d_k_at, lanes(pair + k_first // LANES)] = d_keys
                        d_k_ref[d_k_at, lanes(pair + (k_first + width) // LANES)] = d_values

                    ahead(heads // 2, scores, rest)

                    reducer.beside(sample_index, counts[:samples], start)
                    return carry

                lax.fori_loop(0, per_step, sample, 0)
                here_all = pieces_of(0, chunk)
                at_all = pieces_of(step * chunk, chunk)
                for at, here in zip(at_all, here_all):
                    hat, unused = normalize(hidden[at])
                    norm = (hat * line(rows, gain) + line(rows, shift)).astype(BF16)
                    if cross:
                        d_mix[here] = norm
                    else:
                        norm_t[:, at] = norm.T
                if cross:
                    d_wq[:] += mm_tn(d_mix[:], d_q[:])
                    d_norm = mm_nt(d_q[:], w_in[:])
                else:
                    d_norm = mm_nt(d_q[at_rows], w_in[:])
                for piece, at in enumerate(at_all):
                    d_res, d_gain, d_shift = norm_back(hidden[at], d_norm[piece * LN_ROWS:(piece + 1) * LN_ROWS], line(rows, gain))
                    grad_ref[at] += d_res
                    add_line(d_rows, gain, d_gain)
                    add_line(d_rows, shift, d_shift)

            block = lambda ref: pl.BlockSpec((PAIR_ROWS, ref.shape[1]), lambda step: (step, 0))
            operands = [src['q' if cross else 'qkv'], src['out2' if cross else 'out1']]
            pipeline(
                body, grid=(steps,), in_specs=[block(operands[0]), block(operands[1])],
            )(*operands)
            where = base(layer) + (layout.out2 if cross else layout.out)
            size = width // SHARDS * (width // LANES)
            if cross:
                put_tiles(stage_out, d_wq[:])
                put_tiles(stage_out, d_wout[:], size)
                copy_out = pltpu.make_async_copy(stage_out, region(base(layer) + layout.q2, 2 * size), sem_out)
            else:
                put_tiles(stage_out, d_wout[:])
                copy_out = pltpu.make_async_copy(stage_out, region(where, size), sem_out)
            copy_out.start()
            rows_each = stage.shape[4]
            cols_each = stage.shape[4] // ((context_ref.shape[1] if cross else width) // SHARDS) * LANES
            tails = (2 if cross else 3) * width // cols_each
            first_row = base(layer) + (layout.kv2 if cross else layout.qkv)

            def copy_tail(step):
                return pltpu.make_async_copy(stage, region(first_row + step * rows_each, rows_each), sem)

            def tail(step, carry):
                cols = span(step, cols_each)
                result = mm_tn(context[:], d_kv[:, cols]) if cross else mm(norm_t[:], d_q[:, cols])

                @pl.when(step > 0)
                def _():
                    copy_tail(step - 1).wait()

                @pl.when(step == 1)
                def _():
                    copy_out.wait()

                put_tiles(stage, result)
                copy_tail(step).start()
                reducer.beside(step, counts[samples:], start + sum(map(int, counts[:samples])))
                return carry

            lax.fori_loop(0, tails, tail, 0)
            copy_tail(tails - 1).wait()

        small = pltpu.VMEM((SUB, LANES), BF16)
        w_scratch = [pltpu.VMEM((width, inner), BF16), pltpu.VMEM((width, width), BF16), pltpu.SemaphoreType.DMA((2,))]
        size = width // SHARDS * (width // LANES)
        if cross:
            ctx_width = context_ref.shape[1]
            pl.run_scoped(scoped, pltpu.VMEM((PAIR_ROWS, width), BF16), pltpu.VMEM((PAIR_ROWS, width), BF16),
                          pltpu.VMEM((kv_rows_all, 2 * width), BF16), small, pltpu.VMEM((width, width), F32),
                          pltpu.VMEM((width, width), F32), pltpu.VMEM((*CUBE, ctx_width // SHARDS * 2, LANES), F32),
                          pltpu.VMEM((*CUBE, 2 * size, LANES), F32), pltpu.SemaphoreType.DMA,
                          pltpu.SemaphoreType.DMA, *w_scratch, pltpu.VMEM(context_ref.shape, BF16),
                          pltpu.VMEM(src['kv'].shape, BF16), pltpu.SemaphoreType.DMA((2,)))
        else:
            pl.run_scoped(scoped, pltpu.VMEM((PAIR_ROWS, width), BF16), pltpu.VMEM((count, 3 * width), BF16), small,
                          pltpu.VMEM((width, count), BF16), small, pltpu.VMEM((width, width), F32),
                          pltpu.VMEM((*CUBE, width // SHARDS * 3, LANES), F32),
                          pltpu.VMEM((*CUBE, size, LANES), F32), pltpu.SemaphoreType.DMA,
                          pltpu.SemaphoreType.DMA, *w_scratch, small, small, pltpu.SemaphoreType.DMA((2,)))

    place.entry_barrier()
    hidden_copy(0).start()
    for layer in range(blocks):
        rows_copy(layer).start()
    d_rows_ref[:] = jnp.zeros_like(d_rows_ref)
    vec_ref[:] = jnp.zeros_like(vec_ref)

    def load_cot(cot, sem):
        copy = pltpu.make_async_copy(cot_ref, cot, sem)
        copy.start()
        copy.wait()
        each_piece(lambda at: grad_ref.__setitem__(at, cot[at].astype(F32)))

    pl.run_scoped(load_cot, pltpu.VMEM(cot_ref.shape, BF16), pltpu.SemaphoreType.DMA)
    for layer in range(blocks):
        rows_copy(layer).wait()
    for index, (layer, kind) in enumerate(phases):
        hidden_copy(index).wait()
        if index + 1 < len(phases):
            hidden_copy(index + 1).start()
        if kind == 'h2':
            ff_phase(layer, index, plan[index])
        else:
            attention_phase(layer, index, plan[index], kind == 'h1')

    def finish(stage, sem, image, sem_image):
        def cast(at):
            image[at] = grad_ref[at].astype(BF16)

        each_piece(cast)
        copy_image = pltpu.make_async_copy(image, gx_ref, sem_image)
        copy_image.start()
        per_device = 17 * width // SHARDS
        stage[:] = jnp.zeros_like(stage)
        for layer in range(blocks):
            vec = vec_ref.at[layer]
            for row in range(9):
                for tile in range(width // LANES):
                    at = row * (width // LANES) + tile
                    vec[at:at + 1] = d_rows_ref[layer, row:row + 1, lanes(tile)]
            lane = lax.broadcasted_iota(jnp.int32, (SUB, LANES), 1)
            for shard in range(SHARDS):
                row, off = divmod(shard * per_device, LANES)
                here, after = vec[pl.ds(row, SUB)], vec[pl.ds(row + 1, SUB)]
                if off:
                    here = jnp.where(lane < LANES - off, pltpu.roll(here, LANES - off, 1), pltpu.roll(after, LANES - off, 1))
                bits = [shard // weight % 2 for weight in WEIGHT]
                stage[(*bits, pl.ds(layer * layout.vec_rows, layout.vec_rows))] = here
        copy = pltpu.make_async_copy(stage, region(layout.vec, stage.shape[4]), sem)
        copy.start()
        copy.wait()
        repeat(layout.macros + STREAMS * STAGES - plan[-1], lambda index: reducer.step(plan[-1] + index))
        load(out_ref, sum_ref, sem).wait()
        copy_image.wait()

    pl.run_scoped(finish, pltpu.VMEM((*CUBE, blocks * layout.vec_rows + layout.pad, LANES), F32),
                  pltpu.SemaphoreType.DMA, pltpu.VMEM(cot_ref.shape, BF16), pltpu.SemaphoreType.DMA)


def backward(cot, context, saved, tokens, ctx_len, total):
    count, width = cot.shape
    blocks = len(saved)
    layout = Layout(width, context.shape[1], blocks)
    starts = [sum(map(int, ''.join(PLAN[:phase]))) for phase in range(len(PLAN) + 1)]
    cfg = (tokens, ctx_len, width, blocks, layout, total, [*zip(starts, PLAN), starts[-1]])
    operands = [cot, context]
    for block in saved:
        operands += [block[name] for name in NAMES]
    shape = saved[0]['rows'].shape
    outs = pl.pallas_call(
        functools.partial(backward_kernel, cfg),
        in_specs=any_specs(len(operands)), out_specs=any_specs(3),
        out_shape=[jax.ShapeDtypeStruct((count, width), BF16),
                   jax.ShapeDtypeStruct((*CUBE, layout.rows, LANES), F32),
                   jax.ShapeDtypeStruct((layout.rows, LANES), F32)],
        scratch_shapes=[pltpu.VMEM((count, width), F32), pltpu.VMEM((2, count, width), F32),
                        pltpu.VMEM((blocks,) + shape, F32), pltpu.VMEM((blocks,) + shape, F32),
                        pltpu.VMEM((blocks, 96, LANES), F32), pltpu.VMEM((layout.rows, LANES), F32),
                        pltpu.SemaphoreType.DMA((2 + blocks,))] + Reducer.scratch(),
        name='backward', **settings(0),
    )(*operands)
    return outs[0], outs[2], layout


PLAN = ('0011002011', '11101000100', '11100101001', '1021011012', '11002001000', '21010111100')


def deliver_kernel(cfg, sum_ref, gx_ref, tokens_ref, *out_refs):
    width, ctx_width, blocks, layout = cfg
    out_refs[-2][:] = gx_ref[:]
    out_refs[-1][:] = tokens_ref[:]
    tiles = width // LANES
    for layer in range(blocks):
        for name, target in zip(MATS, out_refs):
            first = (blocks - 1 - layer) * layout.block + getattr(layout, name)
            total = target.shape[0] // blocks
            part = {'kv2': ctx_width, 'ff2': 4 * width}.get(name, width) // SHARDS
            many = total // part

            def put(tile, size, stride, row):
                target[pl.ds(tile * blocks + layer, size, stride=stride * blocks)] = sum_ref[row:row + size]

            for index in range(many):
                if name == 'ff1':
                    half, at = divmod(index, many // 2)
                    step, tile = divmod(at, 2)
                    put(index, part, many, first + step * FF_PART + half * 80 + tile * part)
                elif name == 'ff2':
                    for block in range(part // FF_SUB):
                        put(block * FF_PART + index, FF_SUB, tiles, first + block * FF_PART + index * FF_SUB)
                else:
                    put(index, part, many, first + index * part)
        per_device = 17 * width // SHARDS
        for row in range(-(-per_device // LANES)):
            size = min(LANES, per_device - row * LANES)
            out_refs[len(MATS)][layer:layer + 1, row * LANES:row * LANES + size] = line(
                sum_ref, layout.vec + layer * layout.vec_rows + row)[:, :size]


def deliver(sums, grad_x, tokens, shapes, cfg):
    in_vmem = pl.BlockSpec(memory_space=pltpu.VMEM)
    out_shape = [jax.ShapeDtypeStruct(shape, F32) for shape in shapes] + [
        jax.ShapeDtypeStruct(grad_x.shape, BF16), jax.ShapeDtypeStruct(tokens.shape, BF16)]
    return pl.pallas_call(
        functools.partial(deliver_kernel, cfg), in_specs=[in_vmem] * 3, out_specs=[in_vmem] * len(out_shape),
        out_shape=out_shape, compiler_params=pltpu.CompilerParams(vmem_limit_bytes=VMEM_BYTES), name='deliver',
    )(sums, grad_x, tokens)


def solution(mesh):
    n_dev = mesh.shape[AXIS]

    def local(tokens_x, context, cot_out, *shards):
        samples, tokens, width = tokens_x.shape
        blocks = shards[0].shape[0]
        spare = -shards[-1].shape[1] % LANES
        padded = shards[:-1] + (jnp.pad(shards[-1], ((0, 0), (0, spare))),)
        raws = [shard.reshape(blocks, -1, LANES).swapaxes(0, 1) for shard in padded]
        raws = [raw.reshape(-1, LANES) for raw in raws[:-1]] + raws[-1:]
        saved, ctx_rows, out_tokens = forward(tokens_x, context, raws, blocks)
        grad_x, sums, layout = backward(cot_out.reshape(samples * tokens, width), ctx_rows, saved, tokens,
                                        context.shape[1], samples * n_dev)
        shapes = [raw.shape for raw in raws[:-1]] + [shards[-1].shape]
        *grads, vec, grad_x, out_tokens = deliver(sums, grad_x, out_tokens, shapes,
                                                  (width, context.shape[2], blocks, layout))
        grads = [grad.reshape(-1, blocks, LANES).swapaxes(0, 1).reshape(blocks, -1) for grad in grads] + [vec]
        return (out_tokens.reshape(tokens_x.shape), grad_x.reshape(tokens_x.shape), *grads)

    param_spec = P(None, AXIS)
    in_specs = (P(AXIS), P(AXIS), P(AXIS)) + (param_spec,) * 8
    out_specs = (P(AXIS), P(AXIS)) + (param_spec,) * 8
    return jax.shard_map(local, mesh=mesh, in_specs=in_specs, out_specs=out_specs, check_vma=False)
```
